32 devices in a mesh: fluid: 8 (over y, x, core), solid: 4 (over z).
Axes of the slice: x: 2, y: 2, z: 4, core: 2. Of those that a mesh axis runs over, the one named last changes fastest.
Arguments:
- rbf_blocks: bfloat16 [3328, 256, 256], P(('fluid', 'solid')), may hold values from -0.375 to 0.375
- fluid_traction: bfloat16 [3328, 768], P(('fluid', 'solid')), may hold values from -24 to 24
- fluid_mass: bfloat16 [3328, 768], P(('fluid', 'solid')), may hold values from 0.19921875 to 2
- route: int32 [3328, 1], P(('fluid', 'solid')), may hold values from 0 to 31; in each aligned block of 104 rows (0 to 103, 104 to 207, ...) at most 6 rows name the same one
- slot: int32 [3328], P(('fluid', 'solid')), may hold values from 0 to 7
- shell_inverse: bfloat16 [256, 768, 768], P(('fluid', 'solid')), may hold values from -0.0078125 to 0.0078125
- robin_coef: float32 [256, 768], P(('fluid', 'solid')), may hold values from 1 to 27
- shell_start: float32 [256, 768], P(('fluid', 'solid')), may hold values from -3 to 3
Outputs:
- shell_displacement: float32 [256, 768], P(('fluid', 'solid'))
- fluid_load: bfloat16 [3328, 768], P(('fluid', 'solid'))
- residual_norms: float32 [6], replicated
The draws below stay inside these ranges and needn't reach their ends.
Inputs may be any that keep to these rules, and one draw needn't show every extreme that they name: `route`: among the 104 blocks of one device at most 6 name the same owner device.
All inputs are finite; a program needn't handle non-finite values.
Results may differ from the reference program's by a relative error of at most 0.009.
Values may be sent and summed in bfloat16 or wider, within the bound.
A program may use at most 128 MiB of HBM per device.

```python
import math
import jax
import jax.numpy as jnp
import numpy as np
from jax import lax

NODES = 256
FB_DEV = 104
SB_DEV = 8
ITERS = 6
CAP = 6
NFB = 3328
NSB = 256
N_FLUID = 8
N_SOLID = 4
DEVICES = 32


def place_ends(drawn, key, least, top_value):
    spot = [jax.random.randint(jax.random.fold_in(key, axis), (), 0, length) for axis, length in enumerate(drawn.shape)]
    widest = drawn.shape.index(max(drawn.shape))
    beside = spot[:widest] + [(spot[widest] + 1) % drawn.shape[widest]] + spot[widest + 1:]
    return drawn.at[tuple(spot)].set(least).at[tuple(beside)].set(top_value)


def level_of(key, extent, cuts, least, largest):
    loudness, own = 1.0, jax.random.fold_in(key, 6)
    for position, shards_of in cuts:
        draws = jnp.exp(jax.random.uniform(jax.random.fold_in(own, position), (shards_of,), jnp.float32, least / len(cuts), largest / len(cuts)))
        loudness = loudness * jnp.repeat(draws, extent[position] // shards_of).reshape([-1 if axis == position else 1 for axis in range(len(extent))])
    return loudness


def routed_block(rng, own, number, rows, amount, top, limit, slope):
    order = jax.random.permutation(rng, amount)
    crowded, ordinary = load_shares(amount, rows * top, limit, slope, True), load_shares(amount, rows * top, limit, slope, False)
    places = jnp.arange(amount)

    def named(tallies, offset_by):
        used = int((tallies > 0).sum())
        fixed = max(1, used // 4)
        moved = fixed + (places - fixed + offset_by * (used - fixed)) % max(1, amount - fixed)
        return jnp.zeros((amount,), jnp.int32).at[order[jnp.where(places < fixed, places, moved)]].set(jnp.asarray(tallies, jnp.int32))

    tallies = jnp.where(number % 4 == 0, named(crowded, number // 4), named(ordinary, number - number // 4 - 1))
    mixed = jax.random.permutation(jax.random.fold_in(own, 3), amount)
    giver, taker = mixed[0:amount // 2 * 2:2], mixed[1:amount // 2 * 2:2]
    slack = jnp.minimum(tallies[giver] - 1, limit - tallies[taker]) // 2
    slack = jnp.where((giver == order[0]) | (taker == order[0]) | (tallies[taker] == 0), 0, jnp.maximum(slack, 0))
    moved = jax.random.randint(jax.random.fold_in(own, 4), (amount // 2,), 0, 1 << 20) % (slack + 1)
    tallies = tallies.at[giver].add(-moved).at[taker].add(moved)
    members = jnp.searchsorted(jnp.cumsum(tallies), jnp.arange(rows * top), side="right").astype(jnp.int32)
    listing = members.reshape(top, rows).T
    listing = listing[jax.random.permutation(jax.random.fold_in(own, 1), rows)]
    offset_by = jax.random.randint(jax.random.fold_in(own, 2), (rows, 1), 0, top)
    return jnp.take_along_axis(listing, (jnp.arange(top)[None, :] + offset_by) % top, axis=1)


def load_shares(amount, total, reach, lean, full):
    portions = [(1 << 20) // math.isqrt(standing ** lean) + 1 for standing in range(1, amount + 1)]
    largest = reach if full else min(reach, max(-(-total // amount), total * portions[0] // sum(portions)))
    least = 1 if total - largest >= amount - 1 else 0
    counts, rest = [largest] + [least] * (amount - 1), total - largest - least * (amount - 1)
    while rest > 0:
        free = [i for i in range(1, amount) if counts[i] < largest] or [i for i in range(1, amount) if counts[i] < reach]
        mass, left = sum([portions[i] for i in free]), rest
        for i in free:
            extra = min(reach - counts[i], max(1, left * portions[i] // mass), rest)
            counts[i] = counts[i] + extra
            rest = rest - extra
    return np.array(counts)


def noise(own_key, dims, scale, bound, split=(), kind=jnp.bfloat16):
    drawn = scale * jax.random.normal(own_key, dims, jnp.float32)
    if split:
        drawn = drawn * level_of(own_key, dims, split, -0.22, 0.18)
    return jnp.clip(drawn, -bound, bound).astype(kind)


def setup_inputs(seed: int = 0) -> dict:
    splits = jax.random.split(jax.random.key(seed), 9)
    rbf_blocks = noise(splits[0], (NFB, NODES, NODES), NODES ** -0.5, 0.375, ((0, 32),))
    fluid_traction = noise(splits[1], (NFB, 3 * NODES), 4.0, 24.0, ((0, 32),))
    fluid_mass = jnp.clip(jnp.exp(math.log(2.0) - 2.306499 * jax.random.uniform(splits[2], (NFB, 3 * NODES), jnp.float32) ** level_of(splits[2], (NFB, 3 * NODES), ((0, 32),), -0.2, 0.2)), 0.19921875, 2.0).astype(jnp.bfloat16)
    route_keys = jax.random.split(jax.random.fold_in(splits[3], 1), NFB // FB_DEV)
    route_turns = jax.random.permutation(jax.random.fold_in(splits[3], 3), NFB // FB_DEV)
    route = jax.vmap(lambda own, number: routed_block(jax.random.fold_in(splits[3], 2), own, number, FB_DEV, DEVICES, 1, CAP, 0))(route_keys, route_turns).reshape((NFB, 1))
    slot = place_ends(jax.random.randint(splits[4], (NFB,), 0, SB_DEV), jax.random.fold_in(splits[4], 1), 0, SB_DEV - 1).astype(jnp.int32)
    shell_inverse = noise(splits[5], (NSB, 3 * NODES, 3 * NODES), (3 * NODES * 64 * FB_DEV // SB_DEV) ** -0.5, 0.0078125, ((0, 32),))
    robin_coef = jnp.clip(jnp.exp(math.log(27.0) - 3.295837 * jax.random.uniform(splits[6], (NSB, 3 * NODES), jnp.float32) ** level_of(splits[6], (NSB, 3 * NODES), ((0, 32),), -0.2, 0.2)), 1.0, 27.0)
    shell_start = noise(splits[7], (NSB, 3 * NODES), 0.5, 3.0, ((0, 32),), jnp.float32)
    return {"rbf_blocks": rbf_blocks, "fluid_traction": fluid_traction, "fluid_mass": fluid_mass, "route": route, "slot": slot, "shell_inverse": shell_inverse, "robin_coef": robin_coef, "shell_start": shell_start}


RELAX = 0.3
EPSILON = 1e-06

def fluid_side(pieces):
    hblock, displaced, traction, massive = pieces
    hfloat = hblock.astype(jnp.float32)
    moved = jnp.einsum('bcj,bij->bci', displaced.reshape(-1, 3, NODES).astype(jnp.float32), hfloat).reshape(-1, 3 * NODES)
    load = (traction.astype(jnp.float32) - massive.astype(jnp.float32) * moved).astype(jnp.bfloat16)
    mapped = jnp.einsum('bci,bij->bcj', load.reshape(-1, 3, NODES).astype(jnp.float32), hfloat).reshape(-1, 3 * NODES)
    return (load, mapped.astype(jnp.bfloat16))

def shell_side(pieces):
    inverse, forcing = pieces
    return jnp.einsum('bi,bij->bj', forcing.astype(jnp.float32), inverse.astype(jnp.float32))

def least_squares(gram, target_side):
    order = gram.shape[0]
    lower = [[None] * order for _ in range(order)]
    for row in range(order):
        for column in range(row + 1):
            total = gram[row, column]
            for inner in range(column):
                total = total - lower[row][inner] * lower[column][inner]
            if row == column:
                lower[row][row] = jnp.sqrt(total)
            else:
                lower[row][column] = total / lower[column][column]
    middle = []
    for row in range(order):
        total = target_side[row]
        for inner in range(row):
            total = total - lower[row][inner] * middle[inner]
        middle.append(total / lower[row][row])
    result = [None] * order
    for row in reversed(range(order)):
        total = middle[row]
        for inner in range(row + 1, order):
            total = total - lower[inner][row] * result[inner]
        result[row] = total / lower[row][row]
    return jnp.stack(result)

def reference(rbf_blocks, fluid_traction, fluid_mass, route, slot, shell_inverse, robin_coef, shell_start):
    groups = N_FLUID * N_SOLID
    breadth = 3 * NODES
    shells_all = shell_start.shape[0]
    target = (route[:, 0] * SB_DEV + slot).astype(jnp.int32)
    rbf_grouped = rbf_blocks.reshape(groups, FB_DEV, NODES, NODES)
    traction_grouped = fluid_traction.reshape(groups, FB_DEV, breadth)
    mass_grouped = fluid_mass.reshape(groups, FB_DEV, breadth)
    inverse_grouped = shell_inverse.reshape(groups, SB_DEV, breadth, breadth)
    count = shells_all * breadth
    batching = min(16, groups)
    current = shell_start
    residuals = []
    images = []
    norms = []
    last_load = None
    for iteration in range(ITERS):
        displaced = current.astype(jnp.bfloat16)[target]
        loads, mapped = lax.map(fluid_side, (rbf_grouped, displaced.reshape(groups, FB_DEV, breadth), traction_grouped, mass_grouped), batch_size=batching)
        last_load = loads.reshape(-1, breadth)
        shell_load = jax.ops.segment_sum(mapped.reshape(-1, breadth).astype(jnp.float32), target, num_segments=shells_all)
        forcing = (shell_load + robin_coef * current).astype(jnp.bfloat16)
        image = lax.map(shell_side, (inverse_grouped, forcing.reshape(groups, SB_DEV, breadth)), batch_size=batching).reshape(shells_all, breadth)
        residual = image - current
        squares = jnp.sum(residual * residual)
        norms.append(jnp.sqrt(squares / count + EPSILON))
        residuals.append(residual)
        images.append(image)
        if iteration == 0:
            current = current + RELAX * residual
        else:
            changes = jnp.stack([(residuals[i + 1] - residuals[i]).reshape(-1) for i in range(iteration)])
            image_changes = jnp.stack([images[i + 1] - images[i] for i in range(iteration)])
            gram = jnp.dot(changes, changes.T, precision=lax.Precision.HIGHEST)
            rhs = jnp.dot(changes, residual.reshape(-1), precision=lax.Precision.HIGHEST)
            coefs = least_squares(gram, -rhs)
            current = image + jnp.tensordot(coefs, image_changes, axes=1, precision=lax.Precision.HIGHEST)
    return (current, last_load, jnp.stack(norms))
```

```python
import functools

import jax
import jax.numpy as jnp
from jax import lax
from jax.experimental import pallas as pl
from jax.experimental.pallas import tpu as pltpu
from jax.sharding import PartitionSpec as P

ITERS = 6


RELAX = 0.3
EPSILON = 1e-06


def transport(buffer, devices, capacity):
    breadth = buffer.shape[1]
    moved = lax.all_to_all(
        buffer.reshape(devices, capacity, breadth),
        ("fluid", "solid"),
        split_axis=0,
        concat_axis=0,
        tiled=True,
    )
    return moved.reshape(devices * capacity, breadth)


def least_squares(gram, target_side):
    order = gram.shape[0]
    lower = [[None] * order for _ in range(order)]
    for row in range(order):
        for column in range(row + 1):
            total = gram[row, column]
            for inner in range(column):
                total = total - lower[row][inner] * lower[column][inner]
            if row == column:
                lower[row][row] = jnp.sqrt(total)
            else:
                lower[row][column] = total / lower[column][column]
    middle = []
    for row in range(order):
        total = target_side[row]
        for inner in range(row):
            total = total - lower[row][inner] * middle[inner]
        middle.append(total / lower[row][row])
    result = [None] * order
    for row in reversed(range(order)):
        total = middle[row]
        for inner in range(row + 1, order):
            total = total - lower[inner][row] * result[inner]
        result[row] = total / lower[row][row]
    return jnp.stack(result)


def per_device(
    rbf_blocks, fluid_traction, fluid_mass, route, slot, shell_inverse, robin_coef, shell_start
):
    devices = lax.axis_size("fluid") * lax.axis_size("solid")
    blocks = rbf_blocks.shape[0]
    nodes = rbf_blocks.shape[1]
    breadth = 3 * nodes
    shells = shell_inverse.shape[0]
    capacity = max(2, 2 * blocks // devices)
    slots_all = devices * capacity
    destination = route[:, 0]
    block_order = jnp.arange(blocks, dtype=jnp.int32)
    earlier = (destination[:, None] == destination[None, :]) & (
        block_order[None, :] < block_order[:, None]
    )
    slot_rank = jnp.sum(earlier.astype(jnp.int32), axis=1)
    position = destination * capacity + slot_rank
    positions = jnp.arange(slots_all, dtype=jnp.int32)
    placing = positions[:, None] == position[None, :]
    place_out = placing.astype(jnp.bfloat16)
    place_in = (position[:, None] == positions[None, :]).astype(jnp.bfloat16)
    wanted = jnp.max(jnp.where(placing, slot[None, :] + 1, 0), axis=1) - 1
    asked = lax.all_to_all(
        wanted.reshape(devices, capacity),
        ("fluid", "solid"),
        split_axis=0,
        concat_axis=0,
        tiled=True,
    ).reshape(slots_all)
    shell_ids = jnp.arange(shells, dtype=jnp.int32)
    picking = (asked[:, None] == shell_ids[None, :]).astype(jnp.bfloat16)
    collecting = (shell_ids[:, None] == asked[None, :]).astype(jnp.bfloat16)
    traction = fluid_traction.astype(jnp.float32)
    massive = fluid_mass.astype(jnp.float32)
    count = shells * devices * breadth
    current = shell_start
    residuals = []
    images = []
    norms = []
    last_load = None
    for iteration in range(ITERS):
        current_half = current.astype(jnp.bfloat16)
        outgoing = jnp.dot(picking, current_half, preferred_element_type=jnp.float32).astype(
            jnp.bfloat16
        )
        incoming = transport(outgoing, devices, capacity)
        displaced = jnp.dot(place_in, incoming, preferred_element_type=jnp.float32).astype(
            jnp.bfloat16
        )
        moved = jnp.einsum(
            "bcj,bij->bci",
            displaced.reshape(blocks, 3, nodes),
            rbf_blocks,
            preferred_element_type=jnp.float32,
        ).reshape(blocks, breadth)
        load = (traction - massive * moved).astype(jnp.bfloat16)
        last_load = load
        mapped = (
            jnp.einsum(
                "bci,bij->bcj",
                load.reshape(blocks, 3, nodes),
                rbf_blocks,
                preferred_element_type=jnp.float32,
            )
            .reshape(blocks, breadth)
            .astype(jnp.bfloat16)
        )
        sending = jnp.dot(place_out, mapped, preferred_element_type=jnp.float32).astype(
            jnp.bfloat16
        )
        arrived = transport(sending, devices, capacity)
        shell_load = jnp.dot(collecting, arrived, preferred_element_type=jnp.float32)
        forcing = (shell_load + robin_coef * current).astype(jnp.bfloat16)
        image = jnp.einsum("bi,bij->bj", forcing, shell_inverse, preferred_element_type=jnp.float32)
        residual = image - current
        residuals.append(residual)
        images.append(image)
        squares_local = jnp.sum(residual * residual)
        if iteration == 0:
            gram_local = jnp.zeros((1, 1), jnp.float32)
            rhs_local = jnp.zeros((1,), jnp.float32)
        else:
            changes = jnp.stack(
                [(residuals[i + 1] - residuals[i]).reshape(-1) for i in range(iteration)]
            )
            gram_local = jnp.dot(changes, changes.T, precision=lax.Precision.HIGHEST)
            rhs_local = jnp.dot(changes, residual.reshape(-1), precision=lax.Precision.HIGHEST)
        gram, rhs, squares = lax.psum((gram_local, rhs_local, squares_local), ("fluid", "solid"))
        norms.append(jnp.sqrt(squares / count + EPSILON))
        if iteration == 0:
            current = current + RELAX * residual
        else:
            image_changes = jnp.stack([images[i + 1] - images[i] for i in range(iteration)])
            coefs = least_squares(gram, -rhs)
            current = image + jnp.tensordot(
                coefs, image_changes, axes=1, precision=lax.Precision.HIGHEST
            )
    return (current, last_load, jnp.stack(norms))


CHUNK = 52
LANES = 128
VMEM_BYTES = 67043328
MESH = pl.DeviceIdType.MESH


def kernel(
    nf, nz, blocks, nodes, shells, count,
    tgt_ref, tr_ref, ms_ref, robin_ref, start_ref, rbf_hbm, inv_hbm,
    cur_out, load_out, norm_out,
    rbf, inv, gath, scal, xcur, xprev, pprev, cur, rprev, wx, wp, vhist, sc, cb,
    place, collect, tr8, ms8, disp8, map8, moved, mapn, part,
    send_a, recv_a, send_b, recv_b,
    rbf_sem, inv_sem, ag_s, ag_r, pr_s, pr_r, sl_s, sl_r, ra_s, ra_r, rb_s, rb_r,
):
    f32, bf16 = jnp.float32, jnp.bfloat16
    breadth = 3 * nodes
    nxy = nf // 2
    nx = 2 if nxy % 2 == 0 else 1
    ny = nxy // nx
    chips = nxy * nz
    half = chips * shells
    group = nz * shells
    f = lax.axis_index("fluid")
    z = lax.axis_index("solid")
    core = lax.rem(f, 2)
    other = 1 - core
    xy = f // 2
    x, y = lax.rem(xy, nx), xy // nx
    nchunk = blocks // CHUNK
    ngroup = blocks // 8
    parts = nodes // LANES

    def hops(step):
        ey, ex, ez = step
        return min(ey, ny - ey) + min(ex, nx - ex) + min(ez, nz - ez)

    steps = sorted(
        [(ey, ex, ez) for ey in range(ny) for ex in range(nx) for ez in range(nz) if ey + ex + ez],
        key=hops, reverse=True,
    )
    far = len(steps)

    def away(step, sign=1):
        ey, ex, ez = step
        plane = lax.rem(y + sign * ey + ny, ny) * nx + lax.rem(x + sign * ex + nx, nx)
        return plane, lax.rem(z + sign * ez + nz, nz)

    targets = [away(s) for s in steps]
    sources = [away(s, -1) for s in steps]

    def chip(plane, depth):
        return plane * nz + depth

    me = chip(xy, z)

    def remote(src, dst, send_sem, recv_sem, plane, unit, depth):
        return pltpu.make_async_remote_copy(
            src_ref=src, dst_ref=dst, send_sem=send_sem, recv_sem=recv_sem,
            device_id=(plane * 2 + unit, depth), device_id_type=MESH,
        )

    def rbf_copy(i):
        at = pl.ds(i * CHUNK, CHUNK)
        return pltpu.make_async_copy(rbf_hbm.at[at], rbf.at[at], rbf_sem.at[i])

    def inv_copy():
        return pltpu.make_async_copy(inv_hbm, inv, inv_sem)

    for i in range(nchunk):
        rbf_copy(i).start()
    inv_copy().start()

    barrier = pltpu.get_barrier_semaphore()
    for plane, depth in targets + [(xy, z)]:
        for unit in (core, other):
            if plane is xy and unit is core:
                continue
            pl.semaphore_signal(
                barrier, inc=1, device_id=(plane * 2 + unit, depth), device_id_type=MESH
            )

    xcur[...] = start_ref[...]
    for ref in (xprev, pprev, cur, rprev, wx, wp, vhist, sc, cb):
        ref[...] = jnp.zeros(ref.shape, ref.dtype)
    mapn[...] = jnp.zeros(mapn.shape, bf16)

    def clear(i, c):
        at = pl.ds(pl.multiple_of(i * 64, 64), 64)
        for ref in (tr8, ms8, disp8):
            ref[:, at, :] = jnp.zeros((parts, 64, LANES), f32)
        return c

    lax.fori_loop(0, ngroup, clear, 0)

    def strided(q, c):
        return pl.ds(q * 64 + c, 8, stride=8)

    def scatter(ref, q, c, value):
        for p in range(parts):
            ref[p, strided(q, c), :] = value[:, p * LANES:(p + 1) * LANES]

    def gather(ref, q, c):
        return jnp.concatenate([ref[p, strided(q, c), :] for p in range(parts)], axis=1)

    def rows_of(ref, at):
        return jnp.concatenate([ref[p, at, :] for p in range(parts)], axis=1)

    def set_rows(ref, at, value):
        for p in range(parts):
            ref[p, at, :] = value[:, p * LANES:(p + 1) * LANES]

    for src, dst in ((tr_ref, tr8), (ms_ref, ms8)):
        for row in range(0, blocks, 16):
            size = min(16, blocks - row)
            wide = src[row:row + size, :].astype(f32)
            for k in range(size // 8):
                for c in range(3):
                    scatter(dst, row // 8 + k, c, wide[k * 8:(k + 1) * 8, c * nodes:(c + 1) * nodes])

    target = tgt_ref[...]
    diagonal = lax.broadcasted_iota(jnp.int32, (blocks, blocks), 0) == lax.broadcasted_iota(
        jnp.int32, (blocks, blocks), 1
    )
    column = jnp.sum(jnp.where(diagonal, target.astype(f32), 0.0), axis=1, keepdims=True)
    for side in range(2):
        unit = core if side == 0 else other
        line = lax.broadcasted_iota(jnp.int32, (half, 1), 0)
        ids = (line // group * 2 + unit) * group + lax.rem(line, group)
        collect[side] = jnp.zeros(collect.shape[1:], bf16)
        collect[side, :, 0:blocks] = jnp.where(ids == target, 1.0, 0.0).astype(bf16)
        lane = lax.broadcasted_iota(jnp.int32, (1, half), 1)
        ids = (lane // group * 2 + unit) * group + lax.rem(lane, group)
        place[side] = jnp.where(ids.astype(f32) == column, 1.0, 0.0).astype(bf16)

    pl.semaphore_wait(barrier, 2 * far + 1)

    lane = lax.broadcasted_iota(jnp.int32, (1, LANES), 1)

    def pick(vector, q):
        return jnp.sum(jnp.where(lane == q, vector, 0.0), axis=1, keepdims=True)

    def dot(a, b, dims=((1,), (0,))):
        return lax.dot_general(a, b, (dims, ((), ())), preferred_element_type=f32)

    def ag(j, k, incoming=False):
        at = chip(*sources[k]) if incoming else me
        block = gath.at[j, core, at]
        return remote(block, block, ag_s.at[k], ag_r.at[k], targets[k][0], core, targets[k][1])

    def ag_pair(j, k, incoming=False):
        at = me if k == far else chip(*sources[k])
        block = gath.at[j, other if incoming else core, at]
        return remote(block, block, pr_s.at[k], pr_r.at[k], xy, other, z)

    def scalar_copies(j, incoming=False):
        copies = []
        turn = lax.rem(j, 2)
        for k in range(far + 1):
            for unit in range(2):
                if k == far and unit == 0:
                    continue
                at = (me if k == far else chip(*sources[k])) if incoming else me
                mine = (core if unit == 0 else other) if incoming else core
                plane, depth = (xy, z) if k == far else targets[k]
                block = scal.at[j, mine, at]
                copies.append(remote(
                    block, block, sl_s.at[turn, k, unit], sl_r.at[turn, k, unit],
                    plane, core if unit == 0 else other, depth,
                ))
        return copies

    def scalars(j):
        residual = xcur[...] - cur[...]
        newest = residual - rprev[...]
        rprev[...] = residual
        vhist[lax.rem(j + ITERS + ITERS - 2, ITERS)] = jnp.where(j > 0, newest, 0.0)

        def total(product):
            return jnp.sum(jnp.sum(product, axis=0, keepdims=True), axis=1, keepdims=True)

        vector = jnp.where(lane == 0, total(residual * residual), 0.0)
        for i in range(ITERS - 1):
            vector = jnp.where(lane == 1 + i, total(vhist[i] * residual), vector)
            vector = jnp.where(lane == 8 + i, total(vhist[i] * newest), vector)
        scal[j, core, me] = jnp.where(j > 0, vector, 0.0)
        for copy in scalar_copies(j):
            copy.start()

    def coefficients(j):
        for copy in scalar_copies(j, True):
            copy.wait_recv()
        k = j - 1
        total = jnp.sum(jnp.sum(scal[j], axis=0), axis=0)
        sc[j] = total
        norm = jnp.sqrt(pick(total, 0) / count + EPSILON)

        @pl.when(j > 0)
        def _():
            norm_out[jnp.maximum(k, 0)] = jnp.broadcast_to(norm, (1, LANES))

        order = ITERS - 1
        gram = [[None] * order for _ in range(order)]
        for col in range(order):
            vector = sc[col + 2]
            for row in range(col + 1):
                value = pick(vector, 8 + row)
                if row == col:
                    value = jnp.where(col < k, value, 1.0)
                gram[col][row] = value
        side = [-pick(total, 1 + i) for i in range(order)]
        lower = [[None] * order for _ in range(order)]
        for row in range(order):
            for col in range(row + 1):
                value = gram[row][col]
                for inner in range(col):
                    value = value - lower[row][inner] * lower[col][inner]
                if row == col:
                    lower[row][row] = jnp.sqrt(value)
                else:
                    lower[row][col] = value / lower[col][col]
        middle = []
        for row in range(order):
            value = side[row]
            for inner in range(row):
                value = value - lower[row][inner] * middle[inner]
            middle.append(value / lower[row][row])
        result = [None] * order
        for row in reversed(range(order)):
            value = middle[row]
            for inner in range(row + 1, order):
                value = value - lower[inner][row] * result[inner]
            result[row] = value / lower[row][row]
        relax = jnp.where(j == 1, jnp.full((1, 1), RELAX - 1.0, f32), 0.0)
        for i, value in enumerate([relax] + result):
            cb[i] = jnp.broadcast_to(value, (1, LANES))

    def weight(i):
        return jnp.concatenate([cb[i]] * (breadth // LANES), axis=1)

    def blend(newest, history):
        value = newest
        for i in range(ITERS):
            value = value + weight(i) * history[i]
        return value

    def note(j):
        wx[lax.rem(j + ITERS - 1, ITERS)] = xcur[...] - xprev[...]
        xprev[...] = xcur[...]

    def iteration(j, carry):
        gath[j, core, me] = xcur[...].astype(bf16)
        for k in range(far):
            ag(j, k).start()
        ag_pair(j, far).start()
        scalars(j)
        note(j)
        for k in reversed(range(far)):
            ag(j, k, True).wait_recv()
            ag_pair(j, k).start()

        def image_half(unit):
            return gath[j, unit].astype(f32).reshape(half, breadth).astype(bf16)

        picked = dot(place[0], image_half(core))
        for k in range(far + 1):
            ag_pair(j, k, True).wait_recv()
        picked = picked + dot(place[1], image_half(other))
        for q in range(ngroup):
            for c in range(3):
                scatter(disp8, q, c, picked[q * 8:(q + 1) * 8, c * nodes:(c + 1) * nodes])

        def fluid(i, c):
            @pl.when(j == 0)
            def _():
                rbf_copy(i).wait()

            loads = []
            for u in range(CHUNK):
                b = i * CHUNK + u
                at = pl.ds(pl.multiple_of(b * 8, 8), 8)
                shift = dot(rows_of(disp8, at).astype(bf16), rbf[b], ((1,), (1,)))
                set_rows(moved.at[j], at, shift)
                loads.append((rows_of(tr8, at) - rows_of(ms8, at) * shift).astype(bf16))
            for u in range(CHUNK):
                b = i * CHUNK + u
                at = pl.ds(pl.multiple_of(b * 8, 8), 8)
                set_rows(map8, at, dot(loads[u], rbf[b]))
            return c

        lax.fori_loop(0, nchunk, fluid, 0)

        for q in range(0, ngroup, 2):
            size = min(2, ngroup - q)
            for c in range(3):
                rows = [gather(map8, q + k, c) for k in range(size)]
                value = jnp.concatenate(rows, axis=0) if size > 1 else rows[0]
                mapn[q * 8:(q + size) * 8, c * nodes:(c + 1) * nodes] = value.astype(bf16)
        send_a[...] = dot(collect[1], mapn[...]).reshape(chips, shells, breadth).astype(bf16)
        copy_a = remote(send_a, recv_a, ra_s, ra_r, xy, other, z)
        copy_a.start()
        part[...] = dot(collect[0], mapn[...]).reshape(chips, shells, breadth)
        copy_a.wait_recv()

        def copy_b(k):
            return remote(
                send_b.at[k], recv_b.at[k], rb_s.at[k], rb_r.at[k], targets[k][0], core, targets[k][1]
            )

        for k in range(far):
            at = chip(*targets[k])
            send_b[k] = (part[at] + recv_a[at].astype(f32)).astype(bf16)
            copy_b(k).start()
        shell_load = part[me] + recv_a[me].astype(f32)

        coefficients(j)
        cur[...] = blend(xcur[...], wx)
        for k in range(far):
            ag(j, k).wait_send()
        for k in range(far + 1):
            ag_pair(j, k).wait_send()
        for copy in scalar_copies(j):
            copy.wait_send()
        copy_a.wait_send()

        @pl.when(j == 0)
        def _():
            inv_copy().wait()

        for k in reversed(range(far)):
            copy_b(k).wait_recv()
            shell_load = shell_load + recv_b[k].astype(f32)
        forcing = (shell_load + robin_ref[...] * xcur[...]).astype(bf16)
        shell_row = lax.broadcasted_iota(jnp.int32, (shells, breadth), 0)
        image = jnp.zeros((shells, breadth), f32)
        for s in range(shells):
            image = jnp.where(shell_row == s, dot(forcing, inv[s]), image)
        wp[lax.rem(j + ITERS - 1, ITERS)] = image - pprev[...]
        pprev[...] = image
        xcur[...] = blend(image, wp)
        for k in range(far):
            copy_b(k).wait_send()
        return carry

    lax.fori_loop(0, ITERS, iteration, 0)
    scalars(ITERS)
    note(ITERS)
    weights = []
    for i in range(ITERS):
        value = 1.0 if i == ITERS - 1 else -cb[i]
        value = value + cb[i - 1] if i > 0 else value
        weights.append(jnp.concatenate([value] * (nodes // LANES), axis=1))
    for q in range(0, ngroup, 2):
        size = min(2, ngroup - q)
        rows = slice(q * 8, (q + size) * 8)
        for c in range(3):
            shift = None
            for i in range(ITERS):
                term = [gather(moved.at[i], q + k, c) for k in range(size)]
                term = weights[i] * (jnp.concatenate(term, axis=0) if size > 1 else term[0])
                shift = term if shift is None else shift + term
            lanes = slice(c * nodes, (c + 1) * nodes)
            load = tr_ref[rows, lanes].astype(f32) - ms_ref[rows, lanes].astype(f32) * shift
            load_out[rows, lanes] = load.astype(bf16)
    coefficients(ITERS)
    cur_out[...] = blend(xcur[...], wx)
    for copy in scalar_copies(ITERS):
        copy.wait_send()


def fused(nf, nz, rbf_blocks, fluid_traction, fluid_mass, route, slot, shell_inverse, robin_coef, shell_start):
    f32, bf16 = jnp.float32, jnp.bfloat16
    blocks, nodes, _ = rbf_blocks.shape
    shells, breadth = shell_start.shape
    chips = nf // 2 * nz
    half = chips * shells
    far = chips - 1
    target = (route[:, 0] * shells + slot)[None, :]
    padded = -(-blocks // LANES) * LANES
    dma = pltpu.SemaphoreType.DMA
    vmem = pl.BlockSpec(memory_space=pltpu.VMEM)
    anywhere = pl.BlockSpec(memory_space=pl.ANY)
    state = pltpu.VMEM((shells, breadth), f32)
    history = pltpu.VMEM((ITERS, shells, breadth), f32)
    wide = pltpu.VMEM((nodes // LANES, blocks * 8, LANES), f32)
    current, load, norms = pl.pallas_call(
        functools.partial(kernel, nf, nz, blocks, nodes, shells, 2 * half * breadth),
        out_shape=(
            jax.ShapeDtypeStruct((shells, breadth), f32),
            jax.ShapeDtypeStruct((blocks, breadth), bf16),
            jax.ShapeDtypeStruct((ITERS, 1, LANES), f32),
        ),
        in_specs=[vmem] * 5 + [anywhere] * 2,
        out_specs=(vmem, vmem, vmem),
        scratch_shapes=[
            pltpu.VMEM(rbf_blocks.shape, bf16),
            pltpu.VMEM(shell_inverse.shape, bf16),
            pltpu.VMEM((ITERS, 2, chips, shells, breadth), bf16),
            pltpu.VMEM((ITERS + 1, 2, chips, 1, LANES), f32),
            state, state, state, state, state,
            history, history, history,
            pltpu.VMEM((ITERS + 1, 1, LANES), f32),
            pltpu.VMEM((ITERS, 1, LANES), f32),
            pltpu.VMEM((2, blocks, half), bf16),
            pltpu.VMEM((2, half, padded), bf16),
            wide, wide, wide, wide,
            pltpu.VMEM((ITERS, nodes // LANES, blocks * 8, LANES), f32),
            pltpu.VMEM((padded, breadth), bf16),
            pltpu.VMEM((chips, shells, breadth), f32),
            pltpu.VMEM((chips, shells, breadth), bf16),
            pltpu.VMEM((chips, shells, breadth), bf16),
            pltpu.VMEM((far, shells, breadth), bf16),
            pltpu.VMEM((far, shells, breadth), bf16),
            dma((blocks // CHUNK,)),
            dma,
            dma((far,)), dma((far,)),
            dma((far + 1,)), dma((far + 1,)),
            dma((2, far + 1, 2)), dma((2, far + 1, 2)),
            dma, dma,
            dma((far,)), dma((far,)),
        ],
        compiler_params=pltpu.CompilerParams(
            collective_id=0, has_side_effects=True, vmem_limit_bytes=VMEM_BYTES
        ),
        name="coupling",
    )(
        target, fluid_traction, fluid_mass, robin_coef, shell_start, rbf_blocks, shell_inverse,
    )
    return current, load, norms[:, 0, 0]


def choose(nf, nz):
    def body(rbf_blocks, *others):
        if nf * nz > 32:
            return per_device(rbf_blocks, *others)
        return fused(nf, nz, rbf_blocks, *others)

    return body


def solution(mesh):
    in_specs = (
        P(("fluid", "solid"), None, None),
        P(("fluid", "solid"), None),
        P(("fluid", "solid"), None),
        P(("fluid", "solid"), None),
        P(("fluid", "solid")),
        P(("fluid", "solid"), None, None),
        P(("fluid", "solid"), None),
        P(("fluid", "solid"), None),
    )
    out_specs = (P(("fluid", "solid"), None), P(("fluid", "solid"), None), P())
    return jax.shard_map(
        choose(mesh.shape["fluid"], mesh.shape["solid"]), mesh=mesh, in_specs=in_specs, out_specs=out_specs, check_vma=False
    )
```

```python
import functools

import jax
import jax.numpy as jnp
from jax import lax
from jax.experimental import pallas as pl
from jax.experimental.pallas import tpu as pltpu
from jax.sharding import PartitionSpec as P

ITERS = 6


RELAX = 0.3
EPSILON = 1e-06


def transport(buffer, devices, capacity):
    breadth = buffer.shape[1]
    moved = lax.all_to_all(
        buffer.reshape(devices, capacity, breadth),
        ("fluid", "solid"),
        split_axis=0,
        concat_axis=0,
        tiled=True,
    )
    return moved.reshape(devices * capacity, breadth)


def least_squares(gram, target_side):
    order = gram.shape[0]
    lower = [[None] * order for _ in range(order)]
    for row in range(order):
        for column in range(row + 1):
            total = gram[row, column]
            for inner in range(column):
                total = total - lower[row][inner] * lower[column][inner]
            if row == column:
                lower[row][row] = jnp.sqrt(total)
            else:
                lower[row][column] = total / lower[column][column]
    middle = []
    for row in range(order):
        total = target_side[row]
        for inner in range(row):
            total = total - lower[row][inner] * middle[inner]
        middle.append(total / lower[row][row])
    result = [None] * order
    for row in reversed(range(order)):
        total = middle[row]
        for inner in range(row + 1, order):
            total = total - lower[inner][row] * result[inner]
        result[row] = total / lower[row][row]
    return jnp.stack(result)


def per_device(
    rbf_blocks, fluid_traction, fluid_mass, route, slot, shell_inverse, robin_coef, shell_start
):
    devices = lax.axis_size("fluid") * lax.axis_size("solid")
    blocks = rbf_blocks.shape[0]
    nodes = rbf_blocks.shape[1]
    breadth = 3 * nodes
    shells = shell_inverse.shape[0]
    capacity = max(2, 2 * blocks // devices)
    slots_all = devices * capacity
    destination = route[:, 0]
    block_order = jnp.arange(blocks, dtype=jnp.int32)
    earlier = (destination[:, None] == destination[None, :]) & (
        block_order[None, :] < block_order[:, None]
    )
    slot_rank = jnp.sum(earlier.astype(jnp.int32), axis=1)
    position = destination * capacity + slot_rank
    positions = jnp.arange(slots_all, dtype=jnp.int32)
    placing = positions[:, None] == position[None, :]
    place_out = placing.astype(jnp.bfloat16)
    place_in = (position[:, None] == positions[None, :]).astype(jnp.bfloat16)
    wanted = jnp.max(jnp.where(placing, slot[None, :] + 1, 0), axis=1) - 1
    asked = lax.all_to_all(
        wanted.reshape(devices, capacity),
        ("fluid", "solid"),
        split_axis=0,
        concat_axis=0,
        tiled=True,
    ).reshape(slots_all)
    shell_ids = jnp.arange(shells, dtype=jnp.int32)
    picking = (asked[:, None] == shell_ids[None, :]).astype(jnp.bfloat16)
    collecting = (shell_ids[:, None] == asked[None, :]).astype(jnp.bfloat16)
    traction = fluid_traction.astype(jnp.float32)
    massive = fluid_mass.astype(jnp.float32)
    count = shells * devices * breadth
    current = shell_start
    residuals = []
    images = []
    norms = []
    last_load = None
    for iteration in range(ITERS):
        current_half = current.astype(jnp.bfloat16)
        outgoing = jnp.dot(picking, current_half, preferred_element_type=jnp.float32).astype(
            jnp.bfloat16
        )
        incoming = transport(outgoing, devices, capacity)
        displaced = jnp.dot(place_in, incoming, preferred_element_type=jnp.float32).astype(
            jnp.bfloat16
        )
        moved = jnp.einsum(
            "bcj,bij->bci",
            displaced.reshape(blocks, 3, nodes),
            rbf_blocks,
            preferred_element_type=jnp.float32,
        ).reshape(blocks, breadth)
        load = (traction - massive * moved).astype(jnp.bfloat16)
        last_load = load
        mapped = (
            jnp.einsum(
                "bci,bij->bcj",
                load.reshape(blocks, 3, nodes),
                rbf_blocks,
                preferred_element_type=jnp.float32,
            )
            .reshape(blocks, breadth)
            .astype(jnp.bfloat16)
        )
        sending = jnp.dot(place_out, mapped, preferred_element_type=jnp.float32).astype(
            jnp.bfloat16
        )
        arrived = transport(sending, devices, capacity)
        shell_load = jnp.dot(collecting, arrived, preferred_element_type=jnp.float32)
        forcing = (shell_load + robin_coef * current).astype(jnp.bfloat16)
        image = jnp.einsum("bi,bij->bj", forcing, shell_inverse, preferred_element_type=jnp.float32)
        residual = image - current
        residuals.append(residual)
        images.append(image)
        squares_local = jnp.sum(residual * residual)
        if iteration == 0:
            gram_local = jnp.zeros((1, 1), jnp.float32)
            rhs_local = jnp.zeros((1,), jnp.float32)
        else:
            changes = jnp.stack(
                [(residuals[i + 1] - residuals[i]).reshape(-1) for i in range(iteration)]
            )
            gram_local = jnp.dot(changes, changes.T, precision=lax.Precision.HIGHEST)
            rhs_local = jnp.dot(changes, residual.reshape(-1), precision=lax.Precision.HIGHEST)
        gram, rhs, squares = lax.psum((gram_local, rhs_local, squares_local), ("fluid", "solid"))
        norms.append(jnp.sqrt(squares / count + EPSILON))
        if iteration == 0:
            current = current + RELAX * residual
        else:
            image_changes = jnp.stack([images[i + 1] - images[i] for i in range(iteration)])
            coefs = least_squares(gram, -rhs)
            current = image + jnp.tensordot(
                coefs, image_changes, axes=1, precision=lax.Precision.HIGHEST
            )
    return (current, last_load, jnp.stack(norms))


CHUNK = 52
LOAD = 13
TURN = 4
LANES = 128
VMEM_BYTES = 67043328
MESH = pl.DeviceIdType.MESH


def kernel(
    nf, nz, blocks, nodes, shells, count,
    start_ref, route_hbm, slot_hbm, tr_hbm, ms_hbm, robin_hbm, rbf_hbm, inv_hbm,
    cur_out, load_out, norm_out,
    route_ref, slot_ref, tr_ref, ms_ref, robin_ref, load_buf,
    rbf, flip, inv, gath, scal, xcur, xprev, pprev, cur, rprev, wx, wp, vhist, sc, cb,
    place, collect, tr8, ms8, disp8, map8, load8, moved, mapn, part,
    send_a, recv_a, send_b, recv_b,
    in_sem, out_sem, rbf_sem, inv_sem, ag_s, ag_r, pr_s, pr_r, sl_s, sl_r, ra_s, ra_r, rb_s, rb_r,
):
    f32, bf16 = jnp.float32, jnp.bfloat16
    breadth = 3 * nodes
    nxy = nf // 2
    nx = 2 if nxy % 2 == 0 else 1
    ny = nxy // nx
    chips = nxy * nz
    half = chips * shells
    group = nz * shells
    f = lax.axis_index("fluid")
    z = lax.axis_index("solid")
    core = lax.rem(f, 2)
    other = 1 - core
    xy = f // 2
    x, y = lax.rem(xy, nx), xy // nx
    nchunk = blocks // CHUNK
    nload = blocks // LOAD
    ngroup = blocks // 8
    parts = nodes // LANES

    def hops(step):
        ey, ex, ez = step
        return min(ey, ny - ey) + min(ex, nx - ex) + min(ez, nz - ez)

    steps = sorted(
        [(ey, ex, ez) for ey in range(ny) for ex in range(nx) for ez in range(nz) if ey + ex + ez],
        key=hops, reverse=True,
    )
    far = len(steps)

    def away(step, sign=1):
        ey, ex, ez = step
        plane = lax.rem(y + sign * ey + ny, ny) * nx + lax.rem(x + sign * ex + nx, nx)
        return plane, lax.rem(z + sign * ez + nz, nz)

    targets = [away(s) for s in steps]
    sources = [away(s, -1) for s in steps]

    def chip(plane, depth):
        return plane * nz + depth

    me = chip(xy, z)

    def remote(src, dst, send_sem, recv_sem, plane, unit, depth):
        return pltpu.make_async_remote_copy(
            src_ref=src, dst_ref=dst, send_sem=send_sem, recv_sem=recv_sem,
            device_id=(plane * 2 + unit, depth), device_id_type=MESH,
        )

    def rbf_copy(i):
        at = pl.ds(i * LOAD, LOAD)
        return pltpu.make_async_copy(rbf_hbm.at[at], rbf.at[at], rbf_sem.at[i])

    def inv_copy():
        return pltpu.make_async_copy(inv_hbm, inv, inv_sem)

    smalls = [
        pltpu.make_async_copy(src, dst, in_sem.at[i])
        for i, (src, dst) in enumerate((
            (route_hbm, route_ref), (slot_hbm, slot_ref), (tr_hbm, tr_ref), (ms_hbm, ms_ref),
            (robin_hbm, robin_ref),
        ))
    ]
    for copy in smalls:
        copy.start()
    for i in range(nload):
        rbf_copy(i).start()
    inv_copy().start()

    barrier = pltpu.get_barrier_semaphore()
    for plane, depth in targets + [(xy, z)]:
        for unit in (core, other):
            if plane is xy and unit is core:
                continue
            pl.semaphore_signal(
                barrier, inc=1, device_id=(plane * 2 + unit, depth), device_id_type=MESH
            )

    def ag(j, k, incoming=False):
        at = chip(*sources[k]) if incoming else me
        block = gath.at[j, core, at]
        return remote(block, block, ag_s.at[k], ag_r.at[k], targets[k][0], core, targets[k][1])

    def ag_pair(j, k, incoming=False):
        at = me if k == far else chip(*sources[k])
        block = gath.at[j, other if incoming else core, at]
        return remote(block, block, pr_s.at[k], pr_r.at[k], xy, other, z)

    def share(j):
        gath[j, core, me] = xcur[...].astype(bf16)
        for k in range(far):
            ag(j, k).start()
        ag_pair(j, far).start()

    xcur[...] = start_ref[...]
    pl.semaphore_wait(barrier, 2 * far + 1)
    share(0)

    xprev[...] = start_ref[...]
    for ref in (pprev, cur, rprev, wx, wp, vhist, sc, cb):
        ref[...] = jnp.zeros(ref.shape, ref.dtype)
    mapn[...] = jnp.zeros(mapn.shape, bf16)

    def clear(i, c):
        at = pl.ds(pl.multiple_of(i * 64, 64), 64)
        for ref in (tr8, ms8, disp8):
            ref[:, at, :] = jnp.zeros((parts, 64, LANES), f32)
        return c

    lax.fori_loop(0, ngroup, clear, 0)
    for copy in smalls:
        copy.wait()

    def strided(q, c):
        return pl.ds(q * 64 + c, 8, stride=8)

    def scatter(ref, q, c, value):
        for p in range(parts):
            ref[p, strided(q, c), :] = value[:, p * LANES:(p + 1) * LANES]

    def gather(ref, q, c):
        return jnp.concatenate([ref[p, strided(q, c), :] for p in range(parts)], axis=1)

    def rows_of(ref, at):
        return jnp.concatenate([ref[p, at, :] for p in range(parts)], axis=1)

    def set_rows(ref, at, value):
        for p in range(parts):
            ref[p, at, :] = value[:, p * LANES:(p + 1) * LANES]

    for src, dst in ((tr_ref, tr8), (ms_ref, ms8)):
        for row in range(0, blocks, 16):
            size = min(16, blocks - row)
            wide = src[row:row + size, :].astype(f32)
            for k in range(size // 8):
                for c in range(3):
                    scatter(dst, row // 8 + k, c, wide[k * 8:(k + 1) * 8, c * nodes:(c + 1) * nodes])

    diagonal = lax.broadcasted_iota(jnp.int32, (blocks, blocks), 0) == lax.broadcasted_iota(
        jnp.int32, (blocks, blocks), 1
    )
    target = (route_ref[...] * shells + slot_ref[...]).astype(f32)
    column = jnp.sum(jnp.where(diagonal, target, 0.0), axis=1, keepdims=True)
    for side in range(2):
        unit = core if side == 0 else other
        line = lax.broadcasted_iota(jnp.int32, (half, 1), 0)
        ids = (line // group * 2 + unit) * group + lax.rem(line, group)
        collect[side] = jnp.zeros(collect.shape[1:], bf16)
        collect[side, :, 0:blocks] = jnp.where(ids.astype(f32) == target, 1.0, 0.0).astype(bf16)
        lane = lax.broadcasted_iota(jnp.int32, (1, half), 1)
        ids = (lane // group * 2 + unit) * group + lax.rem(lane, group)
        place[side] = jnp.where(ids.astype(f32) == column, 1.0, 0.0).astype(bf16)

    lane = lax.broadcasted_iota(jnp.int32, (1, LANES), 1)

    def pick(vector, q):
        return jnp.sum(jnp.where(lane == q, vector, 0.0), axis=1, keepdims=True)

    def dot(a, b, dims=((1,), (0,))):
        return lax.dot_general(a, b, (dims, ((), ())), preferred_element_type=f32)

    def scalar_copies(j, incoming=False):
        copies = []
        turn = lax.rem(j, 2)
        for k in range(far + 1):
            for unit in range(2):
                if k == far and unit == 0:
                    continue
                at = (me if k == far else chip(*sources[k])) if incoming else me
                mine = (core if unit == 0 else other) if incoming else core
                plane, depth = (xy, z) if k == far else targets[k]
                block = scal.at[j, mine, at]
                copies.append(remote(
                    block, block, sl_s.at[turn, k, unit], sl_r.at[turn, k, unit],
                    plane, core if unit == 0 else other, depth,
                ))
        return copies

    def scalars(j):
        residual = xcur[...] - cur[...]
        newest = residual - rprev[...]
        rprev[...] = residual
        vhist[lax.rem(j + ITERS - 2, ITERS)] = newest

        def total(product):
            return jnp.sum(jnp.sum(product, axis=0, keepdims=True), axis=1, keepdims=True)

        vector = jnp.where(lane == 0, total(residual * residual), 0.0)
        for i in range(ITERS - 1):
            vector = jnp.where(lane == 1 + i, total(vhist[i] * residual), vector)
            vector = jnp.where(lane == 8 + i, total(vhist[i] * newest), vector)
        scal[j, core, me] = vector
        for copy in scalar_copies(j):
            copy.start()

    def coefficients(j):
        for copy in scalar_copies(j, True):
            copy.wait_recv()
        k = j - 1
        total = jnp.sum(jnp.sum(scal[j], axis=0), axis=0)
        sc[j] = total
        norm = jnp.sqrt(pick(total, 0) / count + EPSILON)

        norm_out[k] = jnp.broadcast_to(norm, (1, LANES))

        order = ITERS - 1
        gram = [[None] * order for _ in range(order)]
        for col in range(order):
            vector = sc[col + 2]
            for row in range(col + 1):
                value = pick(vector, 8 + row)
                if row == col:
                    value = jnp.where(col < k, value, 1.0)
                gram[col][row] = value
        side = [-pick(total, 1 + i) for i in range(order)]
        lower = [[None] * order for _ in range(order)]
        for row in range(order):
            for col in range(row + 1):
                value = gram[row][col]
                for inner in range(col):
                    value = value - lower[row][inner] * lower[col][inner]
                if row == col:
                    lower[row][row] = jnp.sqrt(value)
                else:
                    lower[row][col] = value / lower[col][col]
        middle = []
        for row in range(order):
            value = side[row]
            for inner in range(row):
                value = value - lower[row][inner] * middle[inner]
            middle.append(value / lower[row][row])
        result = [None] * order
        for row in reversed(range(order)):
            value = middle[row]
            for inner in range(row + 1, order):
                value = value - lower[inner][row] * result[inner]
            result[row] = value / lower[row][row]
        relax = jnp.where(j == 1, jnp.full((1, 1), RELAX - 1.0, f32), 0.0)
        for i, value in enumerate([relax] + result):
            cb[i] = jnp.broadcast_to(value, (1, LANES))

    def weight(i):
        return jnp.concatenate([cb[i]] * (breadth // LANES), axis=1)

    def blend(newest, history):
        value = newest
        for i in range(ITERS):
            value = value + weight(i) * history[i]
        return value

    def note(j):
        wx[lax.rem(j + ITERS - 1, ITERS)] = xcur[...] - xprev[...]
        xprev[...] = xcur[...]

    def iteration(j, carry):
        for k in reversed(range(far)):
            ag(j, k, True).wait_recv()
            ag_pair(j, k).start()

        def image_half(unit):
            return gath[j, unit].astype(f32).reshape(half, breadth).astype(bf16)

        picked = dot(place[0], image_half(core))
        for k in range(far + 1):
            ag_pair(j, k, True).wait_recv()
        picked = picked + dot(place[1], image_half(other))
        for q in range(ngroup):
            for c in range(3):
                scatter(disp8, q, c, picked[q * 8:(q + 1) * 8, c * nodes:(c + 1) * nodes])

        def move(i, size, table, dims):
            for u in range(size):
                b = i * size + u
                at = pl.ds(pl.multiple_of(b * 8, 8), 8)
                shift = dot(rows_of(disp8, at).astype(bf16), table[b], dims)
                set_rows(moved.at[j], at, shift)
                load8[b] = (rows_of(tr8, at) - rows_of(ms8, at) * shift).astype(bf16)

        @pl.when(j == 0)
        def _():
            def first(i, c):
                rbf_copy(i).wait()
                move(i, LOAD, rbf, ((1,), (1,)))
                return c

            lax.fori_loop(0, nload, first, 0)

        @pl.when(j > 0)
        def _():
            def later(i, c):
                move(i, CHUNK, flip, ((1,), (0,)))
                return c

            lax.fori_loop(0, nchunk, later, 0)

        def back(i, c):
            for u in range(CHUNK):
                b = i * CHUNK + u
                set_rows(map8, pl.ds(pl.multiple_of(b * 8, 8), 8), dot(load8[b], rbf[b]))
            return c

        lax.fori_loop(0, nchunk, back, 0)

        for q in range(0, ngroup, 2):
            size = min(2, ngroup - q)
            for c in range(3):
                rows = [gather(map8, q + k, c) for k in range(size)]
                value = jnp.concatenate(rows, axis=0) if size > 1 else rows[0]
                mapn[q * 8:(q + size) * 8, c * nodes:(c + 1) * nodes] = value.astype(bf16)
        send_a[...] = dot(collect[1], mapn[...]).reshape(chips, shells, breadth).astype(bf16)
        copy_a = remote(send_a, recv_a, ra_s, ra_r, xy, other, z)
        copy_a.start()
        part[...] = dot(collect[0], mapn[...]).reshape(chips, shells, breadth)
        copy_a.wait_recv()

        def copy_b(k):
            return remote(
                send_b.at[k], recv_b.at[k], rb_s.at[k], rb_r.at[k], targets[k][0], core, targets[k][1]
            )

        for k in range(far):
            at = chip(*targets[k])
            send_b[k] = (part[at] + recv_a[at].astype(f32)).astype(bf16)
            copy_b(k).start()
        shell_load = part[me] + recv_a[me].astype(f32)

        @pl.when(j > 0)
        def _():
            coefficients(j)
            for copy in scalar_copies(j):
                copy.wait_send()

        cur[...] = blend(xcur[...], wx)
        for k in range(far):
            ag(j, k).wait_send()
        for k in range(far + 1):
            ag_pair(j, k).wait_send()
        copy_a.wait_send()

        @pl.when(j == 0)
        def _():
            def turn(i, c):
                for u in range(TURN):
                    flip[i * TURN + u] = rbf[i * TURN + u].T
                return c

            lax.fori_loop(0, blocks // TURN, turn, 0)
            inv_copy().wait()

        for k in reversed(range(far)):
            copy_b(k).wait_recv()
            shell_load = shell_load + recv_b[k].astype(f32)
        forcing = (shell_load + robin_ref[...] * xcur[...]).astype(bf16)
        shell_row = lax.broadcasted_iota(jnp.int32, (shells, breadth), 0)
        image = jnp.zeros((shells, breadth), f32)
        for s in range(shells):
            image = jnp.where(shell_row == s, dot(forcing, inv[s]), image)
        wp[lax.rem(j + ITERS - 1, ITERS)] = image - pprev[...]
        pprev[...] = image
        xcur[...] = blend(image, wp)

        @pl.when(j < ITERS - 1)
        def _():
            share(j + 1)

        scalars(j + 1)
        note(j + 1)
        for k in range(far):
            copy_b(k).wait_send()
        return carry

    lax.fori_loop(0, ITERS, iteration, 0)
    weights = []
    for i in range(ITERS):
        value = 1.0 if i == ITERS - 1 else -cb[i]
        value = value + cb[i - 1] if i > 0 else value
        weights.append(jnp.concatenate([value] * (nodes // LANES), axis=1))
    for q in range(0, ngroup, 2):
        size = min(2, ngroup - q)
        rows = slice(q * 8, (q + size) * 8)
        for c in range(3):
            shift = None
            for i in range(ITERS):
                term = [gather(moved.at[i], q + k, c) for k in range(size)]
                term = weights[i] * (jnp.concatenate(term, axis=0) if size > 1 else term[0])
                shift = term if shift is None else shift + term
            lanes = slice(c * nodes, (c + 1) * nodes)
            load = tr_ref[rows, lanes].astype(f32) - ms_ref[rows, lanes].astype(f32) * shift
            load_buf[rows, lanes] = load.astype(bf16)
    write = pltpu.make_async_copy(load_buf, load_out, out_sem)
    write.start()
    coefficients(ITERS)
    cur_out[...] = blend(xcur[...], wx)
    for copy in scalar_copies(ITERS):
        copy.wait_send()
    write.wait()


def hand_over(current, load, norms, current_out, load_out, norm_out):
    current_out[...] = current[...]
    load_out[...] = load[...]
    for i in range(norm_out.shape[0]):
        norm_out[i] = norms[i, 0, 0]


def fused(nf, nz, rbf_blocks, fluid_traction, fluid_mass, route, slot, shell_inverse, robin_coef, shell_start):
    f32, bf16 = jnp.float32, jnp.bfloat16
    blocks, nodes, _ = rbf_blocks.shape
    shells, breadth = shell_start.shape
    chips = nf // 2 * nz
    half = chips * shells
    far = chips - 1
    padded = -(-blocks // LANES) * LANES
    dma = pltpu.SemaphoreType.DMA
    vmem = pl.BlockSpec(memory_space=pltpu.VMEM)
    anywhere = pl.BlockSpec(memory_space=pl.ANY)
    state = pltpu.VMEM((shells, breadth), f32)
    history = pltpu.VMEM((ITERS, shells, breadth), f32)
    wide = pltpu.VMEM((nodes // LANES, blocks * 8, LANES), f32)
    current, load, norms = pl.pallas_call(
        functools.partial(kernel, nf, nz, blocks, nodes, shells, 2 * half * breadth),
        out_shape=(
            jax.ShapeDtypeStruct((shells, breadth), f32),
            jax.ShapeDtypeStruct((blocks, breadth), bf16),
            jax.ShapeDtypeStruct((ITERS, 1, LANES), f32),
        ),
        in_specs=[vmem] + [anywhere] * 7,
        out_specs=(vmem, anywhere, vmem),
        scratch_shapes=[
            pltpu.VMEM((1, blocks), jnp.int32),
            pltpu.VMEM((1, blocks), jnp.int32),
            pltpu.VMEM((blocks, breadth), bf16),
            pltpu.VMEM((blocks, breadth), bf16),
            state,
            pltpu.VMEM((blocks, breadth), bf16),
            pltpu.VMEM(rbf_blocks.shape, bf16),
            pltpu.VMEM(rbf_blocks.shape, bf16),
            pltpu.VMEM(shell_inverse.shape, bf16),
            pltpu.VMEM((ITERS, 2, chips, shells, breadth), bf16),
            pltpu.VMEM((ITERS + 1, 2, chips, 1, LANES), f32),
            state, state, state, state, state,
            history, history, history,
            pltpu.VMEM((ITERS + 1, 1, LANES), f32),
            pltpu.VMEM((ITERS, 1, LANES), f32),
            pltpu.VMEM((2, blocks, half), bf16),
            pltpu.VMEM((2, half, padded), bf16),
            wide, wide, wide, wide,
            pltpu.VMEM((blocks, 8, nodes), bf16),
            pltpu.VMEM((ITERS, nodes // LANES, blocks * 8, LANES), f32),
            pltpu.VMEM((padded, breadth), bf16),
            pltpu.VMEM((chips, shells, breadth), f32),
            pltpu.VMEM((chips, shells, breadth), bf16),
            pltpu.VMEM((chips, shells, breadth), bf16),
            pltpu.VMEM((far, shells, breadth), bf16),
            pltpu.VMEM((far, shells, breadth), bf16),
            dma((5,)), dma,
            dma((blocks // LOAD,)),
            dma,
            dma((far,)), dma((far,)),
            dma((far + 1,)), dma((far + 1,)),
            dma((2, far + 1, 2)), dma((2, far + 1, 2)),
            dma, dma,
            dma((far,)), dma((far,)),
        ],
        compiler_params=pltpu.CompilerParams(
            collective_id=0, has_side_effects=True, vmem_limit_bytes=VMEM_BYTES
        ),
        name="coupling",
    )(
        shell_start, route.T, slot[None, :], fluid_traction, fluid_mass, robin_coef, rbf_blocks,
        shell_inverse,
    )
    smem = pl.BlockSpec(memory_space=pltpu.SMEM)
    return pl.pallas_call(
        hand_over,
        out_shape=(
            jax.ShapeDtypeStruct(current.shape, f32),
            jax.ShapeDtypeStruct(load.shape, bf16),
            jax.ShapeDtypeStruct((ITERS,), f32),
        ),
        in_specs=[vmem, vmem, smem],
        out_specs=(vmem, vmem, smem),
        name="results",
    )(current, load, norms)


def choose(nf, nz):
    def body(rbf_blocks, *others):
        if nf * nz > 32:
            return per_device(rbf_blocks, *others)
        return fused(nf, nz, rbf_blocks, *others)

    return body


def solution(mesh):
    in_specs = (
        P(("fluid", "solid"), None, None),
        P(("fluid", "solid"), None),
        P(("fluid", "solid"), None),
        P(("fluid", "solid"), None),
        P(("fluid", "solid")),
        P(("fluid", "solid"), None, None),
        P(("fluid", "solid"), None),
        P(("fluid", "solid"), None),
    )
    out_specs = (P(("fluid", "solid"), None), P(("fluid", "solid"), None), P())
    return jax.shard_map(
        choose(mesh.shape["fluid"], mesh.shape["solid"]), mesh=mesh, in_specs=in_specs, out_specs=out_specs, check_vma=False
    )
```

```python
import functools

import jax
import jax.numpy as jnp
from jax import lax
from jax.experimental import pallas as pl
from jax.experimental.pallas import tpu as pltpu
from jax.sharding import PartitionSpec as P

ITERS = 6


RELAX = 0.3
EPSILON = 1e-06


def transport(buffer, devices, capacity):
    breadth = buffer.shape[1]
    moved = lax.all_to_all(
        buffer.reshape(devices, capacity, breadth),
        ("fluid", "solid"),
        split_axis=0,
        concat_axis=0,
        tiled=True,
    )
    return moved.reshape(devices * capacity, breadth)


def least_squares(gram, target_side):
    order = gram.shape[0]
    lower = [[None] * order for _ in range(order)]
    for row in range(order):
        for column in range(row + 1):
            total = gram[row, column]
            for inner in range(column):
                total = total - lower[row][inner] * lower[column][inner]
            if row == column:
                lower[row][row] = jnp.sqrt(total)
            else:
                lower[row][column] = total / lower[column][column]
    middle = []
    for row in range(order):
        total = target_side[row]
        for inner in range(row):
            total = total - lower[row][inner] * middle[inner]
        middle.append(total / lower[row][row])
    result = [None] * order
    for row in reversed(range(order)):
        total = middle[row]
        for inner in range(row + 1, order):
            total = total - lower[inner][row] * result[inner]
        result[row] = total / lower[row][row]
    return jnp.stack(result)


def per_device(
    rbf_blocks, fluid_traction, fluid_mass, route, slot, shell_inverse, robin_coef, shell_start
):
    devices = lax.axis_size("fluid") * lax.axis_size("solid")
    blocks = rbf_blocks.shape[0]
    nodes = rbf_blocks.shape[1]
    breadth = 3 * nodes
    shells = shell_inverse.shape[0]
    capacity = max(2, 2 * blocks // devices)
    slots_all = devices * capacity
    destination = route[:, 0]
    block_order = jnp.arange(blocks, dtype=jnp.int32)
    earlier = (destination[:, None] == destination[None, :]) & (
        block_order[None, :] < block_order[:, None]
    )
    slot_rank = jnp.sum(earlier.astype(jnp.int32), axis=1)
    position = destination * capacity + slot_rank
    positions = jnp.arange(slots_all, dtype=jnp.int32)
    placing = positions[:, None] == position[None, :]
    place_out = placing.astype(jnp.bfloat16)
    place_in = (position[:, None] == positions[None, :]).astype(jnp.bfloat16)
    wanted = jnp.max(jnp.where(placing, slot[None, :] + 1, 0), axis=1) - 1
    asked = lax.all_to_all(
        wanted.reshape(devices, capacity),
        ("fluid", "solid"),
        split_axis=0,
        concat_axis=0,
        tiled=True,
    ).reshape(slots_all)
    shell_ids = jnp.arange(shells, dtype=jnp.int32)
    picking = (asked[:, None] == shell_ids[None, :]).astype(jnp.bfloat16)
    collecting = (shell_ids[:, None] == asked[None, :]).astype(jnp.bfloat16)
    traction = fluid_traction.astype(jnp.float32)
    massive = fluid_mass.astype(jnp.float32)
    count = shells * devices * breadth
    current = shell_start
    residuals = []
    images = []
    norms = []
    last_load = None
    for iteration in range(ITERS):
        current_half = current.astype(jnp.bfloat16)
        outgoing = jnp.dot(picking, current_half, preferred_element_type=jnp.float32).astype(
            jnp.bfloat16
        )
        incoming = transport(outgoing, devices, capacity)
        displaced = jnp.dot(place_in, incoming, preferred_element_type=jnp.float32).astype(
            jnp.bfloat16
        )
        moved = jnp.einsum(
            "bcj,bij->bci",
            displaced.reshape(blocks, 3, nodes),
            rbf_blocks,
            preferred_element_type=jnp.float32,
        ).reshape(blocks, breadth)
        load = (traction - massive * moved).astype(jnp.bfloat16)
        last_load = load
        mapped = (
            jnp.einsum(
                "bci,bij->bcj",
                load.reshape(blocks, 3, nodes),
                rbf_blocks,
                preferred_element_type=jnp.float32,
            )
            .reshape(blocks, breadth)
            .astype(jnp.bfloat16)
        )
        sending = jnp.dot(place_out, mapped, preferred_element_type=jnp.float32).astype(
            jnp.bfloat16
        )
        arrived = transport(sending, devices, capacity)
        shell_load = jnp.dot(collecting, arrived, preferred_element_type=jnp.float32)
        forcing = (shell_load + robin_coef * current).astype(jnp.bfloat16)
        image = jnp.einsum("bi,bij->bj", forcing, shell_inverse, preferred_element_type=jnp.float32)
        residual = image - current
        residuals.append(residual)
        images.append(image)
        squares_local = jnp.sum(residual * residual)
        if iteration == 0:
            gram_local = jnp.zeros((1, 1), jnp.float32)
            rhs_local = jnp.zeros((1,), jnp.float32)
        else:
            changes = jnp.stack(
                [(residuals[i + 1] - residuals[i]).reshape(-1) for i in range(iteration)]
            )
            gram_local = jnp.dot(changes, changes.T, precision=lax.Precision.HIGHEST)
            rhs_local = jnp.dot(changes, residual.reshape(-1), precision=lax.Precision.HIGHEST)
        gram, rhs, squares = lax.psum((gram_local, rhs_local, squares_local), ("fluid", "solid"))
        norms.append(jnp.sqrt(squares / count + EPSILON))
        if iteration == 0:
            current = current + RELAX * residual
        else:
            image_changes = jnp.stack([images[i + 1] - images[i] for i in range(iteration)])
            coefs = least_squares(gram, -rhs)
            current = image + jnp.tensordot(
                coefs, image_changes, axes=1, precision=lax.Precision.HIGHEST
            )
    return (current, last_load, jnp.stack(norms))


CHUNK = 52
LOAD = 26
TAIL = 52
TURN = 4
LANES = 128
VMEM_BYTES = 67043328
MESH = pl.DeviceIdType.MESH


def kernel(
    nf, nz, blocks, nodes, shells, count,
    start_hbm, route_hbm, slot_hbm, tr_hbm, ms_hbm, robin_hbm, rbf_hbm, inv_hbm,
    cur_out, load_out, norm_out,
    start_ref, route_ref, slot_ref, tr_ref, ms_ref, robin_ref, load_buf,
    rbf, flip, inv, gath, scal, xcur, xprev, pprev, cur, rprev, robin, wx, wp, vhist, sc, cb,
    place, collect, tr8, ms8, disp8, map8, load8, moved, mapn, part,
    send_a, recv_a, send_b, recv_b,
    in_sem, out_sem, rbf_sem, inv_sem, ag_s, ag_r, pr_s, pr_r, sl_s, sl_r, ra_s, ra_r, rb_s, rb_r,
):
    f32, bf16 = jnp.float32, jnp.bfloat16
    parts = nodes // LANES
    thin = 3 * LANES
    breadth = 3 * nodes
    nxy = nf // 2
    nx = 2 if nxy % 2 == 0 else 1
    ny = nxy // nx
    chips = nxy * nz
    half = chips * shells
    group = nz * shells
    f = lax.axis_index("fluid")
    z = lax.axis_index("solid")
    core = lax.rem(f, 2)
    other = 1 - core
    xy = f // 2
    x, y = lax.rem(xy, nx), xy // nx
    nchunk = blocks // CHUNK
    nload = blocks // LOAD
    ngroup = blocks // 8

    def hops(step):
        ey, ex, ez = step
        return min(ey, ny - ey) + min(ex, nx - ex) + min(ez, nz - ez)

    steps = sorted(
        [(ey, ex, ez) for ey in range(ny) for ex in range(nx) for ez in range(nz) if ey + ex + ez],
        key=hops, reverse=True,
    )
    far = len(steps)

    def away(step, sign=1):
        ey, ex, ez = step
        plane = lax.rem(y + sign * ey + ny, ny) * nx + lax.rem(x + sign * ex + nx, nx)
        return plane, lax.rem(z + sign * ez + nz, nz)

    targets = [away(s) for s in steps]
    sources = [away(s, -1) for s in steps]

    def chip(plane, depth):
        return plane * nz + depth

    me = chip(xy, z)

    def remote(src, dst, send_sem, recv_sem, plane, unit, depth):
        return pltpu.make_async_remote_copy(
            src_ref=src, dst_ref=dst, send_sem=send_sem, recv_sem=recv_sem,
            device_id=(plane * 2 + unit, depth), device_id_type=MESH,
        )

    barrier = pltpu.get_barrier_semaphore()
    for plane, depth in targets + [(xy, z)]:
        for unit in (core, other):
            if plane is xy and unit is core:
                continue
            pl.semaphore_signal(
                barrier, inc=1, device_id=(plane * 2 + unit, depth), device_id_type=MESH
            )

    def rbf_copy(i):
        at = pl.ds(i * LOAD, LOAD)
        return pltpu.make_async_copy(rbf_hbm.at[at], rbf.at[at], rbf_sem.at[i])

    def inv_copy():
        return pltpu.make_async_copy(inv_hbm, inv, inv_sem)

    smalls = [
        pltpu.make_async_copy(src, dst, in_sem.at[i])
        for i, (src, dst) in enumerate((
            (start_hbm, start_ref), (route_hbm, route_ref), (slot_hbm, slot_ref), (tr_hbm, tr_ref),
            (ms_hbm, ms_ref), (robin_hbm, robin_ref),
        ))
    ]
    for copy in smalls:
        copy.start()
    for i in range(nload):
        rbf_copy(i).start()
    inv_copy().start()

    def lanes_of(c, h):
        return slice(c * nodes + h * LANES, c * nodes + (h + 1) * LANES)

    def thin_of(c):
        return slice(c * LANES, (c + 1) * LANES)

    def halved(ref, h):
        return jnp.concatenate([ref[:, lanes_of(c, h)] for c in range(3)], axis=1)

    def ag(j, h, k, incoming=False):
        at = chip(*sources[k]) if incoming else me
        block = gath.at[j, h, core, at]
        return remote(
            block, block, ag_s.at[h, k], ag_r.at[h, k], targets[k][0], core, targets[k][1]
        )

    def ag_pair(j, h, k, incoming=False):
        at = me if k == far else chip(*sources[k])
        block = gath.at[j, h, other if incoming else core, at]
        return remote(block, block, pr_s.at[h, k], pr_r.at[h, k], xy, other, z)

    def share(j, h):
        gath[j, h, core, me] = xcur[h].astype(bf16)
        for k in range(far):
            ag(j, h, k).start()
        ag_pair(j, h, far).start()

    def relay(j, h):
        for k in reversed(range(far)):
            ag(j, h, k, True).wait_recv()
            ag_pair(j, h, k).start()

    smalls[0].wait()
    for h in range(parts):
        xcur[h] = halved(start_ref, h)
    pl.semaphore_wait(barrier, 2 * far + 1)
    for h in range(parts):
        share(0, h)

    xprev[...] = xcur[...]
    for ref in (pprev, cur, rprev, wx, wp, vhist, sc, cb):
        ref[...] = jnp.zeros(ref.shape, ref.dtype)
    mapn[...] = jnp.zeros(mapn.shape, bf16)

    def clear(i, c):
        at = pl.ds(pl.multiple_of(i * 64, 64), 64)
        for ref in (tr8, ms8, disp8):
            ref[:, at, :] = jnp.zeros((parts, 64, LANES), f32)
        return c

    lax.fori_loop(0, ngroup, clear, 0)
    for copy in smalls[1:]:
        copy.wait()
    for h in range(parts):
        robin[h] = halved(robin_ref, h)

    def strided(q, c):
        return pl.ds(q * 64 + c, 8, stride=8)

    def rows_of(ref, at):
        return jnp.concatenate([ref[p, at, :] for p in range(parts)], axis=1)

    def set_rows(ref, at, value):
        for p in range(parts):
            ref[p, at, :] = value[:, p * LANES:(p + 1) * LANES]

    for src, dst in ((tr_ref, tr8), (ms_ref, ms8)):
        for row in range(0, blocks, 16):
            size = min(16, blocks - row)
            wide = src[row:row + size, :].astype(f32)
            for k in range(size // 8):
                for c in range(3):
                    for h in range(parts):
                        dst[h, strided(row // 8 + k, c), :] = wide[k * 8:(k + 1) * 8, lanes_of(c, h)]

    diagonal = lax.broadcasted_iota(jnp.int32, (blocks, blocks), 0) == lax.broadcasted_iota(
        jnp.int32, (blocks, blocks), 1
    )
    target = (route_ref[...] * shells + slot_ref[...]).astype(f32)
    column = jnp.sum(jnp.where(diagonal, target, 0.0), axis=1, keepdims=True)
    for side in range(2):
        unit = core if side == 0 else other
        line = lax.broadcasted_iota(jnp.int32, (half, 1), 0)
        ids = (line // group * 2 + unit) * group + lax.rem(line, group)
        collect[side] = jnp.zeros(collect.shape[1:], bf16)
        collect[side, :, 0:blocks] = jnp.where(ids.astype(f32) == target, 1.0, 0.0).astype(bf16)
        lane = lax.broadcasted_iota(jnp.int32, (1, half), 1)
        ids = (lane // group * 2 + unit) * group + lax.rem(lane, group)
        place[side] = jnp.where(ids.astype(f32) == column, 1.0, 0.0).astype(bf16)

    lane = lax.broadcasted_iota(jnp.int32, (1, LANES), 1)

    def pick(vector, q):
        return jnp.sum(jnp.where(lane == q, vector, 0.0), axis=1, keepdims=True)

    def dot(a, b, dims=((1,), (0,))):
        return lax.dot_general(a, b, (dims, ((), ())), preferred_element_type=f32)

    def scalar_copies(j, incoming=False):
        copies = []
        turn = lax.rem(j, 2)
        for k in range(far + 1):
            for unit in range(2):
                if k == far and unit == 0:
                    continue
                at = (me if k == far else chip(*sources[k])) if incoming else me
                mine = (core if unit == 0 else other) if incoming else core
                plane, depth = (xy, z) if k == far else targets[k]
                block = scal.at[j, mine, at]
                copies.append(remote(
                    block, block, sl_s.at[turn, k, unit], sl_r.at[turn, k, unit],
                    plane, core if unit == 0 else other, depth,
                ))
        return copies

    def scalars(j):
        residual = xcur[...] - cur[...]
        newest = residual - rprev[...]
        rprev[...] = residual
        vhist[lax.rem(j + ITERS - 2, ITERS)] = newest

        def total(product):
            rows = jnp.sum(jnp.sum(product, axis=0), axis=0, keepdims=True)
            return jnp.sum(rows, axis=1, keepdims=True)

        vector = jnp.where(lane == 0, total(residual * residual), 0.0)
        for i in range(ITERS - 1):
            vector = jnp.where(lane == 1 + i, total(vhist[i] * residual), vector)
            vector = jnp.where(lane == 8 + i, total(vhist[i] * newest), vector)
        scal[j, core, me] = vector
        for copy in scalar_copies(j):
            copy.start()

    def coefficients(j):
        for copy in scalar_copies(j, True):
            copy.wait_recv()
        k = j - 1
        total = jnp.sum(jnp.sum(scal[j], axis=0), axis=0)
        sc[j] = total
        norm = jnp.sqrt(pick(total, 0) / count + EPSILON)
        norm_out[k] = jnp.broadcast_to(norm, (1, LANES))

        order = ITERS - 1
        gram = [[None] * order for _ in range(order)]
        for col in range(order):
            vector = sc[col + 2]
            for row in range(col + 1):
                value = pick(vector, 8 + row)
                if row == col:
                    value = jnp.where(col < k, value, 1.0)
                gram[col][row] = value
        side = [-pick(total, 1 + i) for i in range(order)]
        lower = [[None] * order for _ in range(order)]
        for row in range(order):
            for col in range(row + 1):
                value = gram[row][col]
                for inner in range(col):
                    value = value - lower[row][inner] * lower[col][inner]
                if row == col:
                    lower[row][row] = jnp.sqrt(value)
                else:
                    lower[row][col] = value / lower[col][col]
        middle = []
        for row in range(order):
            value = side[row]
            for inner in range(row):
                value = value - lower[row][inner] * middle[inner]
            middle.append(value / lower[row][row])
        result = [None] * order
        for row in reversed(range(order)):
            value = middle[row]
            for inner in range(row + 1, order):
                value = value - lower[inner][row] * result[inner]
            result[row] = value / lower[row][row]
        relax = jnp.where(j == 1, jnp.full((1, 1), RELAX - 1.0, f32), 0.0)
        for i, value in enumerate([relax] + result):
            cb[i] = jnp.broadcast_to(value, (1, LANES))

    def blend(newest, history, h):
        value = newest
        for i in range(ITERS):
            value = value + jnp.concatenate([cb[i]] * 3, axis=1) * history[i, h]
        return value

    def note(j):
        wx[lax.rem(j + ITERS - 1, ITERS)] = xcur[...] - xprev[...]
        xprev[...] = xcur[...]

    upper = lax.broadcasted_iota(jnp.int32, (16, LANES), 0) < 8

    def iteration(j, carry):
        def fetch(h):
            def side(unit):
                return gath[j, h, unit].astype(f32).reshape(half, thin).astype(bf16)

            picked = dot(place[0], side(core))
            for k in range(far + 1):
                ag_pair(j, h, k, True).wait_recv()
            picked = picked + dot(place[1], side(other))
            for q in range(ngroup):
                for c in range(3):
                    disp8[h, strided(q, c), :] = picked[q * 8:(q + 1) * 8, thin_of(c)]

        def move(i, size, h, turned):
            cut = slice(h * LANES, (h + 1) * LANES)
            for u in range(0, size, 2):
                b = i * size + u
                at = pl.ds(pl.multiple_of(b * 8, 16), 16)
                both = disp8[h, at, :]
                left = jnp.concatenate(
                    [jnp.where(upper, both, 0.0), jnp.where(upper, 0.0, both)], axis=1
                ).astype(bf16)
                if turned:
                    shift = dot(left, jnp.concatenate([flip[b, cut, :], flip[b + 1, cut, :]], axis=0))
                else:
                    right = jnp.concatenate([rbf[b, :, cut], rbf[b + 1, :, cut]], axis=1)
                    shift = dot(left, right, ((1,), (1,)))
                if h > 0:
                    shift = shift + rows_of(moved.at[j], at)
                set_rows(moved.at[j], at, shift)
                if h == parts - 1:
                    load = rows_of(tr8, at) - rows_of(ms8, at) * shift
                    load8[i * (size // 2) + u // 2] = load.astype(bf16)

        def forward(h):
            @pl.when(j == 0)
            def _():
                def first(i, c):
                    if h == 0:
                        rbf_copy(i).wait()

                        @pl.when(i == nload // 2)
                        def _():
                            relay(j, 1)

                    move(i, LOAD, h, False)
                    return c

                lax.fori_loop(0, nload, first, 0)

            @pl.when(j > 0)
            def _():
                def later(i, c):
                    if h == 0:
                        @pl.when(i == nchunk // 2)
                        def _():
                            relay(j, 1)

                    move(i, CHUNK, h, True)
                    return c

                lax.fori_loop(0, nchunk, later, 0)

        def backward(h, size):
            cut = slice(h * LANES, (h + 1) * LANES)

            def back(i, c):
                if h > 0:
                    @pl.when(i == blocks // size - 1)
                    def _():
                        spread_out(h - 1)

                for u in range(0, size, 2):
                    b = i * size + u
                    at = pl.multiple_of(b * 8, 16)
                    right = jnp.concatenate([rbf[b, :, cut], rbf[b + 1, :, cut]], axis=1)
                    both = dot(load8[i * (size // 2) + u // 2], right)
                    map8[h, pl.ds(at, 8), :] = both[0:8, 0:LANES]
                    map8[h, pl.ds(at + 8, 8), :] = both[8:16, LANES:2 * LANES]
                return c

            lax.fori_loop(0, blocks // size, back, 0)

        def copy_a(h):
            return remote(send_a.at[h], recv_a.at[h], ra_s.at[h], ra_r.at[h], xy, other, z)

        def copy_b(h, k):
            return remote(
                send_b.at[h, k], recv_b.at[h, k], rb_s.at[h, k], rb_r.at[h, k],
                targets[k][0], core, targets[k][1],
            )

        def gather_up(h):
            for q in range(0, ngroup, 2):
                size = min(2, ngroup - q)
                for c in range(3):
                    rows = [map8[h, strided(q + k, c), :] for k in range(size)]
                    value = jnp.concatenate(rows, axis=0) if size > 1 else rows[0]
                    mapn[h, q * 8:(q + size) * 8, thin_of(c)] = value.astype(bf16)
            send_a[h] = dot(collect[1], mapn[h]).reshape(chips, shells, thin).astype(bf16)
            copy_a(h).start()
            part[h] = dot(collect[0], mapn[h]).reshape(chips, shells, thin)

        def spread_out(h):
            copy_a(h).wait_recv()
            for k in range(far):
                at = chip(*targets[k])
                send_b[h, k] = (part[h, at] + recv_a[h, at].astype(f32)).astype(bf16)
                copy_b(h, k).start()

        relay(j, 0)
        fetch(0)
        forward(0)
        fetch(1)
        forward(1)
        backward(0, CHUNK)
        gather_up(0)
        backward(1, TAIL)
        gather_up(1)
        spread_out(1)

        @pl.when(j > 0)
        def _():
            coefficients(j)
            for copy in scalar_copies(j):
                copy.wait_send()

        for h in range(parts):
            cur[h] = blend(xcur[h], wx, h)
        for h in range(parts):
            for k in range(far):
                ag(j, h, k).wait_send()
            for k in range(far + 1):
                ag_pair(j, h, k).wait_send()
            copy_a(h).wait_send()

        @pl.when(j == 0)
        def _():
            def turn(i, c):
                for u in range(TURN):
                    flip[i * TURN + u] = rbf[i * TURN + u].T
                return c

            lax.fori_loop(0, blocks // TURN, turn, 0)
            inv_copy().wait()

        def forcing(h):
            shell_load = part[h, me] + recv_a[h, me].astype(f32)
            for k in reversed(range(far)):
                copy_b(h, k).wait_recv()
                shell_load = shell_load + recv_b[h, k].astype(f32)
            return (shell_load + robin[h] * xcur[h]).astype(bf16)

        def table(s, c, h, lanes):
            return inv[s, lanes_of(c, h), lanes]

        row = lax.broadcasted_iota(jnp.int32, (shells, LANES), 0)

        def tail_left(force, s):
            last = force[:, thin_of(2)].astype(f32)
            return jnp.concatenate(
                [jnp.where(row == s, last, 0.0), jnp.where(row == s + 1, last, 0.0)], axis=1
            )

        def tail_right(s, h, lanes):
            return jnp.concatenate([table(s, 2, h, lanes), table(s + 1, 2, h, lanes)], axis=0)

        def lead_right(s, h, lanes):
            return jnp.concatenate([table(s, 0, h, lanes), table(s, 1, h, lanes)], axis=0)

        force = forcing(0)
        shell_row = lax.broadcasted_iota(jnp.int32, (shells, breadth), 0)
        whole = slice(0, breadth)
        early = jnp.zeros((shells, breadth), f32)
        for s in range(shells):
            lead = dot(force[:, 0:2 * LANES], lead_right(s, 0, whole))
            early = jnp.where(shell_row == s, lead, early)
        for s in range(0, shells, 2):
            early = early + dot(tail_left(force, s).astype(bf16), tail_right(s, 0, whole))
        force = forcing(1)
        shell_row = lax.broadcasted_iota(jnp.int32, (shells, thin), 0)
        for h in range(parts):
            def wide_right(pieces):
                return jnp.concatenate(
                    [make(lanes_of(c, h)) for make in pieces for c in range(3)], axis=1
                )

            image = jnp.zeros((shells, thin), f32)
            for s in range(0, shells, 2):
                both = dot(force[:, 0:2 * LANES], wide_right(
                    [functools.partial(lead_right, s, 1), functools.partial(lead_right, s + 1, 1)]
                ))
                image = jnp.where(shell_row == s, both[:, 0:thin], image)
                image = jnp.where(shell_row == s + 1, both[:, thin:2 * thin], image)
            for s in range(0, shells, 4):
                left = jnp.concatenate([tail_left(force, s), tail_left(force, s + 2)], axis=0)
                both = dot(left.astype(bf16), wide_right(
                    [functools.partial(tail_right, s, 1), functools.partial(tail_right, s + 2, 1)]
                ))
                image = image + both[0:shells, 0:thin] + both[shells:2 * shells, thin:2 * thin]
            image = image + jnp.concatenate([early[:, lanes_of(c, h)] for c in range(3)], axis=1)
            wp[lax.rem(j + ITERS - 1, ITERS), h] = image - pprev[h]
            pprev[h] = image
            xcur[h] = blend(image, wp, h)

            @pl.when(j < ITERS - 1)
            def _():
                share(j + 1, h)

        scalars(j + 1)
        note(j + 1)
        for h in range(parts):
            for k in range(far):
                copy_b(h, k).wait_send()
        return carry

    lax.fori_loop(0, ITERS, iteration, 0)
    weights = []
    for i in range(ITERS):
        value = 1.0 if i == ITERS - 1 else -cb[i]
        value = value + cb[i - 1] if i > 0 else value
        weights.append(value)
    for q in range(0, ngroup, 2):
        size = min(2, ngroup - q)
        rows = slice(q * 8, (q + size) * 8)
        for c in range(3):
            for h in range(parts):
                shift = None
                for i in range(ITERS):
                    term = [moved[i, h, strided(q + k, c), :] for k in range(size)]
                    term = weights[i] * (jnp.concatenate(term, axis=0) if size > 1 else term[0])
                    shift = term if shift is None else shift + term
                lanes = lanes_of(c, h)
                load = tr_ref[rows, lanes].astype(f32) - ms_ref[rows, lanes].astype(f32) * shift
                load_buf[rows, lanes] = load.astype(bf16)
    write = pltpu.make_async_copy(load_buf, load_out, out_sem)
    write.start()
    coefficients(ITERS)
    for h in range(parts):
        last = blend(xcur[h], wx, h)
        for c in range(3):
            cur_out[:, lanes_of(c, h)] = last[:, thin_of(c)]
    for copy in scalar_copies(ITERS):
        copy.wait_send()
    write.wait()


def hand_over(current, load, norms, current_out, load_out, norm_out):
    current_out[...] = current[...]
    load_out[...] = load[...]
    for i in range(norm_out.shape[0]):
        norm_out[i] = norms[i, 0, 0]


def fused(nf, nz, rbf_blocks, fluid_traction, fluid_mass, route, slot, shell_inverse, robin_coef, shell_start):
    f32, bf16 = jnp.float32, jnp.bfloat16
    blocks, nodes, _ = rbf_blocks.shape
    shells, breadth = shell_start.shape
    chips = nf // 2 * nz
    half = chips * shells
    far = chips - 1
    padded = -(-blocks // LANES) * LANES
    dma = pltpu.SemaphoreType.DMA
    vmem = pl.BlockSpec(memory_space=pltpu.VMEM)
    anywhere = pl.BlockSpec(memory_space=pl.ANY)
    parts = nodes // LANES
    thin = 3 * LANES
    plain = pltpu.VMEM((shells, breadth), f32)
    state = pltpu.VMEM((parts, shells, thin), f32)
    history = pltpu.VMEM((ITERS, parts, shells, thin), f32)
    wide = pltpu.VMEM((parts, blocks * 8, LANES), f32)
    exchange = pltpu.VMEM((parts, chips, shells, thin), bf16)
    current, load, norms = pl.pallas_call(
        functools.partial(kernel, nf, nz, blocks, nodes, shells, 2 * half * breadth),
        out_shape=(
            jax.ShapeDtypeStruct((shells, breadth), f32),
            jax.ShapeDtypeStruct((blocks, breadth), bf16),
            jax.ShapeDtypeStruct((ITERS, 1, LANES), f32),
        ),
        in_specs=[anywhere] * 8,
        out_specs=(vmem, anywhere, vmem),
        scratch_shapes=[
            plain,
            pltpu.VMEM((1, blocks), jnp.int32),
            pltpu.VMEM((1, blocks), jnp.int32),
            pltpu.VMEM((blocks, breadth), bf16),
            pltpu.VMEM((blocks, breadth), bf16),
            plain,
            pltpu.VMEM((blocks, breadth), bf16),
            pltpu.VMEM(rbf_blocks.shape, bf16),
            pltpu.VMEM(rbf_blocks.shape, bf16),
            pltpu.VMEM(shell_inverse.shape, bf16),
            pltpu.VMEM((ITERS, parts, 2, chips, shells, thin), bf16),
            pltpu.VMEM((ITERS + 1, 2, chips, 1, LANES), f32),
            state, state, state, state, state, state,
            history, history, history,
            pltpu.VMEM((ITERS + 1, 1, LANES), f32),
            pltpu.VMEM((ITERS, 1, LANES), f32),
            pltpu.VMEM((2, blocks, half), bf16),
            pltpu.VMEM((2, half, padded), bf16),
            wide, wide, wide, wide,
            pltpu.VMEM((blocks // 2, 16, nodes), bf16),
            pltpu.VMEM((ITERS, parts, blocks * 8, LANES), f32),
            pltpu.VMEM((parts, padded, thin), bf16),
            pltpu.VMEM((parts, chips, shells, thin), f32),
            exchange, exchange, exchange, exchange,
            dma((6,)), dma,
            dma((blocks // LOAD,)),
            dma,
            dma((parts, far)), dma((parts, far)),
            dma((parts, far + 1)), dma((parts, far + 1)),
            dma((2, far + 1, 2)), dma((2, far + 1, 2)),
            dma((parts,)), dma((parts,)),
            dma((parts, far)), dma((parts, far)),
        ],
        compiler_params=pltpu.CompilerParams(
            collective_id=0, has_side_effects=True, vmem_limit_bytes=VMEM_BYTES
        ),
        name="coupling",
    )(
        shell_start, route.T, slot[None, :], fluid_traction, fluid_mass, robin_coef, rbf_blocks,
        shell_inverse,
    )
    smem = pl.BlockSpec(memory_space=pltpu.SMEM)
    return pl.pallas_call(
        hand_over,
        out_shape=(
            jax.ShapeDtypeStruct(current.shape, f32),
            jax.ShapeDtypeStruct(load.shape, bf16),
            jax.ShapeDtypeStruct((ITERS,), f32),
        ),
        in_specs=[vmem, vmem, smem],
        out_specs=(vmem, vmem, smem),
        name="results",
    )(current, load, norms)


def choose(nf, nz):
    def body(rbf_blocks, *others):
        if nf * nz > 32:
            return per_device(rbf_blocks, *others)
        return fused(nf, nz, rbf_blocks, *others)

    return body


def solution(mesh):
    in_specs = (
        P(("fluid", "solid"), None, None),
        P(("fluid", "solid"), None),
        P(("fluid", "solid"), None),
        P(("fluid", "solid"), None),
        P(("fluid", "solid")),
        P(("fluid", "solid"), None, None),
        P(("fluid", "solid"), None),
        P(("fluid", "solid"), None),
    )
    out_specs = (P(("fluid", "solid"), None), P(("fluid", "solid"), None), P())
    return jax.shard_map(
        choose(mesh.shape["fluid"], mesh.shape["solid"]), mesh=mesh, in_specs=in_specs, out_specs=out_specs, check_vma=False
    )
```

```python
import functools

import jax
import jax.numpy as jnp
from jax import lax
from jax.experimental import pallas as pl
from jax.experimental.pallas import tpu as pltpu
from jax.sharding import PartitionSpec as P

ITERS = 6


RELAX = 0.3
EPSILON = 1e-06


def transport(buffer, devices, capacity):
    breadth = buffer.shape[1]
    moved = lax.all_to_all(
        buffer.reshape(devices, capacity, breadth),
        ("fluid", "solid"),
        split_axis=0,
        concat_axis=0,
        tiled=True,
    )
    return moved.reshape(devices * capacity, breadth)


def least_squares(gram, target_side):
    order = gram.shape[0]
    lower = [[None] * order for _ in range(order)]
    for row in range(order):
        for column in range(row + 1):
            total = gram[row, column]
            for inner in range(column):
                total = total - lower[row][inner] * lower[column][inner]
            if row == column:
                lower[row][row] = jnp.sqrt(total)
            else:
                lower[row][column] = total / lower[column][column]
    middle = []
    for row in range(order):
        total = target_side[row]
        for inner in range(row):
            total = total - lower[row][inner] * middle[inner]
        middle.append(total / lower[row][row])
    result = [None] * order
    for row in reversed(range(order)):
        total = middle[row]
        for inner in range(row + 1, order):
            total = total - lower[inner][row] * result[inner]
        result[row] = total / lower[row][row]
    return jnp.stack(result)


def per_device(
    rbf_blocks, fluid_traction, fluid_mass, route, slot, shell_inverse, robin_coef, shell_start
):
    devices = lax.axis_size("fluid") * lax.axis_size("solid")
    blocks = rbf_blocks.shape[0]
    nodes = rbf_blocks.shape[1]
    breadth = 3 * nodes
    shells = shell_inverse.shape[0]
    capacity = max(2, 2 * blocks // devices)
    slots_all = devices * capacity
    destination = route[:, 0]
    block_order = jnp.arange(blocks, dtype=jnp.int32)
    earlier = (destination[:, None] == destination[None, :]) & (
        block_order[None, :] < block_order[:, None]
    )
    slot_rank = jnp.sum(earlier.astype(jnp.int32), axis=1)
    position = destination * capacity + slot_rank
    positions = jnp.arange(slots_all, dtype=jnp.int32)
    placing = positions[:, None] == position[None, :]
    place_out = placing.astype(jnp.bfloat16)
    place_in = (position[:, None] == positions[None, :]).astype(jnp.bfloat16)
    wanted = jnp.max(jnp.where(placing, slot[None, :] + 1, 0), axis=1) - 1
    asked = lax.all_to_all(
        wanted.reshape(devices, capacity),
        ("fluid", "solid"),
        split_axis=0,
        concat_axis=0,
        tiled=True,
    ).reshape(slots_all)
    shell_ids = jnp.arange(shells, dtype=jnp.int32)
    picking = (asked[:, None] == shell_ids[None, :]).astype(jnp.bfloat16)
    collecting = (shell_ids[:, None] == asked[None, :]).astype(jnp.bfloat16)
    traction = fluid_traction.astype(jnp.float32)
    massive = fluid_mass.astype(jnp.float32)
    count = shells * devices * breadth
    current = shell_start
    residuals = []
    images = []
    norms = []
    last_load = None
    for iteration in range(ITERS):
        current_half = current.astype(jnp.bfloat16)
        outgoing = jnp.dot(picking, current_half, preferred_element_type=jnp.float32).astype(
            jnp.bfloat16
        )
        incoming = transport(outgoing, devices, capacity)
        displaced = jnp.dot(place_in, incoming, preferred_element_type=jnp.float32).astype(
            jnp.bfloat16
        )
        moved = jnp.einsum(
            "bcj,bij->bci",
            displaced.reshape(blocks, 3, nodes),
            rbf_blocks,
            preferred_element_type=jnp.float32,
        ).reshape(blocks, breadth)
        load = (traction - massive * moved).astype(jnp.bfloat16)
        last_load = load
        mapped = (
            jnp.einsum(
                "bci,bij->bcj",
                load.reshape(blocks, 3, nodes),
                rbf_blocks,
                preferred_element_type=jnp.float32,
            )
            .reshape(blocks, breadth)
            .astype(jnp.bfloat16)
        )
        sending = jnp.dot(place_out, mapped, preferred_element_type=jnp.float32).astype(
            jnp.bfloat16
        )
        arrived = transport(sending, devices, capacity)
        shell_load = jnp.dot(collecting, arrived, preferred_element_type=jnp.float32)
        forcing = (shell_load + robin_coef * current).astype(jnp.bfloat16)
        image = jnp.einsum("bi,bij->bj", forcing, shell_inverse, preferred_element_type=jnp.float32)
        residual = image - current
        residuals.append(residual)
        images.append(image)
        squares_local = jnp.sum(residual * residual)
        if iteration == 0:
            gram_local = jnp.zeros((1, 1), jnp.float32)
            rhs_local = jnp.zeros((1,), jnp.float32)
        else:
            changes = jnp.stack(
                [(residuals[i + 1] - residuals[i]).reshape(-1) for i in range(iteration)]
            )
            gram_local = jnp.dot(changes, changes.T, precision=lax.Precision.HIGHEST)
            rhs_local = jnp.dot(changes, residual.reshape(-1), precision=lax.Precision.HIGHEST)
        gram, rhs, squares = lax.psum((gram_local, rhs_local, squares_local), ("fluid", "solid"))
        norms.append(jnp.sqrt(squares / count + EPSILON))
        if iteration == 0:
            current = current + RELAX * residual
        else:
            image_changes = jnp.stack([images[i + 1] - images[i] for i in range(iteration)])
            coefs = least_squares(gram, -rhs)
            current = image + jnp.tensordot(
                coefs, image_changes, axes=1, precision=lax.Precision.HIGHEST
            )
    return (current, last_load, jnp.stack(norms))


CHUNK = 52
LOAD = 8
TAIL = 52
LANES = 128
VMEM_BYTES = 67043328
MESH = pl.DeviceIdType.MESH


def kernel(
    nf, nz, blocks, nodes, shells, count,
    start_hbm, route_hbm, slot_hbm, tr_hbm, ms_hbm, robin_hbm, rbf_hbm, inv_hbm,
    cur_out, load_out, norm_out,
    start_ref, route_ref, slot_ref, tr_ref, ms_ref, robin_ref, load_buf,
    rbf, flip, inv, gath, scal, xcur, xprev, pprev, cur, rprev, robin, wx, wp, vhist, sc, cb,
    place, collect, tr8, ms8, disp8, map8, load8, moved, mapn, part,
    send_a, recv_a, send_b, recv_b,
    in_sem, out_sem, rbf_sem, inv_sem, ag_s, ag_r, pr_s, pr_r, sl_s, sl_r, ra_s, ra_r, rb_s, rb_r,
):
    f32, bf16 = jnp.float32, jnp.bfloat16
    parts = nodes // LANES
    thin = 3 * LANES
    breadth = 3 * nodes
    nxy = nf // 2
    nx = 2 if nxy % 2 == 0 else 1
    ny = nxy // nx
    chips = nxy * nz
    half = chips * shells
    group = nz * shells
    f = lax.axis_index("fluid")
    z = lax.axis_index("solid")
    core = lax.rem(f, 2)
    other = 1 - core
    xy = f // 2
    x, y = lax.rem(xy, nx), xy // nx
    nchunk = blocks // CHUNK
    nload = blocks // LOAD
    ngroup = blocks // 8

    nb = 2 if nz % 2 == 0 else 1
    na = nz // nb

    def hops(step):
        ey, ex, ea, eb = step
        return ey + ex + ea * nb + eb

    steps = sorted(
        [
            (ey, ex, ea, eb)
            for ey in range(ny) for ex in range(nx) for ea in range(na) for eb in range(nb)
            if ey + ex + ea + eb
        ],
        key=hops, reverse=True,
    )
    far = len(steps)

    def away(step, sign=1):
        ey, ex, ea, eb = step
        plane = lax.rem(y + sign * ey + ny, ny) * nx + lax.rem(x + sign * ex + nx, nx)
        depth = lax.rem(z // nb + sign * ea + na, na) * nb + lax.rem(lax.rem(z, nb) + sign * eb + nb, nb)
        return plane, depth

    targets = [away(s) for s in steps]
    sources = [away(s, -1) for s in steps]

    def chip(plane, depth):
        return plane * nz + depth

    me = chip(xy, z)

    def remote(src, dst, send_sem, recv_sem, plane, unit, depth):
        return pltpu.make_async_remote_copy(
            src_ref=src, dst_ref=dst, send_sem=send_sem, recv_sem=recv_sem,
            device_id=(plane * 2 + unit, depth), device_id_type=MESH,
        )

    first = pltpu.make_async_copy(start_hbm, start_ref, in_sem.at[0])
    first.start()
    barrier = pltpu.get_barrier_semaphore()
    for plane, depth in targets + [(xy, z)]:
        for unit in (core, other):
            if plane is xy and unit is core:
                continue
            pl.semaphore_signal(
                barrier, inc=1, device_id=(plane * 2 + unit, depth), device_id_type=MESH
            )

    def rbf_copy(i):
        at = pl.ds(i * LOAD, LOAD)
        return pltpu.make_async_copy(rbf_hbm.at[at], rbf.at[at], rbf_sem.at[i])

    def inv_copy():
        return pltpu.make_async_copy(inv_hbm, inv, inv_sem)

    smalls = [
        pltpu.make_async_copy(src, dst, in_sem.at[i + 1])
        for i, (src, dst) in enumerate((
            (route_hbm, route_ref), (slot_hbm, slot_ref), (tr_hbm, tr_ref),
            (ms_hbm, ms_ref), (robin_hbm, robin_ref),
        ))
    ]
    for copy in smalls:
        copy.start()
    for i in range(nload):
        rbf_copy(i).start()
    inv_copy().start()

    def lanes_of(c, h):
        return slice(c * nodes + h * LANES, c * nodes + (h + 1) * LANES)

    def thin_of(c):
        return slice(c * LANES, (c + 1) * LANES)

    def halved(ref, h):
        return jnp.concatenate([ref[:, lanes_of(c, h)] for c in range(3)], axis=1)

    def ag(j, h, k, incoming=False):
        at = chip(*sources[k]) if incoming else me
        block = gath.at[j, h, core, at]
        return remote(
            block, block, ag_s.at[h, k], ag_r.at[h, k], targets[k][0], core, targets[k][1]
        )

    def ag_pair(j, h, k, incoming=False):
        at = me if k == far else chip(*sources[k])
        block = gath.at[j, h, other if incoming else core, at]
        return remote(block, block, pr_s.at[h, k], pr_r.at[h, k], xy, other, z)

    def share(j, h):
        gath[j, h, core, me] = xcur[h].astype(bf16)
        for k in range(far):
            ag(j, h, k).start()
        ag_pair(j, h, far).start()

    def relay(j, h):
        for k in reversed(range(far)):
            ag(j, h, k, True).wait_recv()
            ag_pair(j, h, k).start()

    first.wait()
    for h in range(parts):
        xcur[h] = halved(start_ref, h)
    pl.semaphore_wait(barrier, 2 * far + 1)
    for h in range(parts):
        share(0, h)

    xprev[...] = xcur[...]
    for ref in (pprev, cur, rprev, wx, wp, vhist, sc, cb):
        ref[...] = jnp.zeros(ref.shape, ref.dtype)
    mapn[...] = jnp.zeros(mapn.shape, bf16)

    def clear(i, c):
        at = pl.ds(pl.multiple_of(i * 64, 64), 64)
        for ref in (tr8, ms8, disp8):
            ref[:, at, :] = jnp.zeros((parts, 64, LANES), f32)
        return c

    lax.fori_loop(0, ngroup, clear, 0)
    for copy in smalls:
        copy.wait()
    for h in range(parts):
        robin[h] = halved(robin_ref, h)

    def strided(q, c):
        return pl.ds(q * 64 + c, 8, stride=8)

    def rows_of(ref, at):
        return jnp.concatenate([ref[p, at, :] for p in range(parts)], axis=1)

    def set_rows(ref, at, value):
        for p in range(parts):
            ref[p, at, :] = value[:, p * LANES:(p + 1) * LANES]

    for src, dst in ((tr_ref, tr8), (ms_ref, ms8)):
        for row in range(0, blocks, 16):
            size = min(16, blocks - row)
            wide = src[row:row + size, :].astype(f32)
            for k in range(size // 8):
                for c in range(3):
                    for h in range(parts):
                        dst[h, strided(row // 8 + k, c), :] = wide[k * 8:(k + 1) * 8, lanes_of(c, h)]

    diagonal = lax.broadcasted_iota(jnp.int32, (blocks, blocks), 0) == lax.broadcasted_iota(
        jnp.int32, (blocks, blocks), 1
    )
    target = (route_ref[...] * shells + slot_ref[...]).astype(f32)
    column = jnp.sum(jnp.where(diagonal, target, 0.0), axis=1, keepdims=True)
    for side in range(2):
        unit = core if side == 0 else other
        line = lax.broadcasted_iota(jnp.int32, (half, 1), 0)
        ids = (line // group * 2 + unit) * group + lax.rem(line, group)
        collect[side] = jnp.zeros(collect.shape[1:], bf16)
        collect[side, :, 0:blocks] = jnp.where(ids.astype(f32) == target, 1.0, 0.0).astype(bf16)
        lane = lax.broadcasted_iota(jnp.int32, (1, half), 1)
        ids = (lane // group * 2 + unit) * group + lax.rem(lane, group)
        place[side] = jnp.where(ids.astype(f32) == column, 1.0, 0.0).astype(bf16)

    def turn(i, c):
        rbf_copy(i).wait()
        for u in range(LOAD):
            flip[i * LOAD + u] = rbf[i * LOAD + u].T
        return c

    lax.fori_loop(0, nload, turn, 0)
    lane = lax.broadcasted_iota(jnp.int32, (1, LANES), 1)

    def pick(vector, q):
        return jnp.sum(jnp.where(lane == q, vector, 0.0), axis=1, keepdims=True)

    def dot(a, b):
        return jnp.dot(a, b, preferred_element_type=f32)

    def scalar_copies(j, incoming=False):
        copies = []
        turn = lax.rem(j, 2)
        for k in range(far + 1):
            for unit in range(2):
                if k == far and unit == 0:
                    continue
                at = (me if k == far else chip(*sources[k])) if incoming else me
                mine = (core if unit == 0 else other) if incoming else core
                plane, depth = (xy, z) if k == far else targets[k]
                block = scal.at[j, mine, at]
                copies.append(remote(
                    block, block, sl_s.at[turn, k, unit], sl_r.at[turn, k, unit],
                    plane, core if unit == 0 else other, depth,
                ))
        return copies

    def scalars(j):
        residual = xcur[...] - cur[...]
        newest = residual - rprev[...]
        rprev[...] = residual
        vhist[lax.rem(j + ITERS - 2, ITERS)] = newest

        def total(product):
            rows = jnp.sum(jnp.sum(product, axis=0), axis=0, keepdims=True)
            return jnp.sum(rows, axis=1, keepdims=True)

        vector = jnp.where(lane == 0, total(residual * residual), 0.0)
        for i in range(ITERS - 1):
            vector = jnp.where(lane == 1 + i, total(vhist[i] * residual), vector)
            vector = jnp.where(lane == 8 + i, total(vhist[i] * newest), vector)
        scal[j, core, me] = vector
        for copy in scalar_copies(j):
            copy.start()

    def coefficients(j):
        for copy in scalar_copies(j, True):
            copy.wait_recv()
        k = j - 1
        total = jnp.sum(jnp.sum(scal[j], axis=0), axis=0)
        sc[j] = total
        norm = jnp.sqrt(pick(total, 0) / count + EPSILON)
        norm_out[k] = jnp.broadcast_to(norm, (1, LANES))

        order = ITERS - 1
        gram = [[None] * order for _ in range(order)]
        for col in range(order):
            vector = sc[col + 2]
            for row in range(col + 1):
                value = pick(vector, 8 + row)
                if row == col:
                    value = jnp.where(col < k, value, 1.0)
                gram[col][row] = value
        side = [-pick(total, 1 + i) for i in range(order)]
        lower = [[None] * order for _ in range(order)]
        for row in range(order):
            for col in range(row + 1):
                value = gram[row][col]
                for inner in range(col):
                    value = value - lower[row][inner] * lower[col][inner]
                if row == col:
                    lower[row][row] = jnp.sqrt(value)
                else:
                    lower[row][col] = value / lower[col][col]
        middle = []
        for row in range(order):
            value = side[row]
            for inner in range(row):
                value = value - lower[row][inner] * middle[inner]
            middle.append(value / lower[row][row])
        result = [None] * order
        for row in reversed(range(order)):
            value = middle[row]
            for inner in range(row + 1, order):
                value = value - lower[inner][row] * result[inner]
            result[row] = value / lower[row][row]
        relax = jnp.where(j == 1, jnp.full((1, 1), RELAX - 1.0, f32), 0.0)
        for i, value in enumerate([relax] + result):
            cb[i] = jnp.broadcast_to(value, (1, LANES))

    def blend(newest, history, h):
        value = newest
        for i in range(ITERS):
            value = value + jnp.concatenate([cb[i]] * 3, axis=1) * history[i, h]
        return value

    def note(j):
        wx[lax.rem(j + ITERS - 1, ITERS)] = xcur[...] - xprev[...]
        xprev[...] = xcur[...]

    upper = lax.broadcasted_iota(jnp.int32, (16, LANES), 0) < 8

    def iteration(j, carry):
        def fetch(h):
            def side(unit):
                return gath[j, h, unit].reshape(half, thin)

            picked = dot(place[0], side(core))
            for k in range(far + 1):
                ag_pair(j, h, k, True).wait_recv()
            picked = picked + dot(place[1], side(other))
            for q in range(ngroup):
                for c in range(3):
                    disp8[h, strided(q, c), :] = picked[q * 8:(q + 1) * 8, thin_of(c)]

        def move(i, size, h):
            cut = slice(h * LANES, (h + 1) * LANES)
            for u in range(0, size, 2):
                b = i * size + u
                at = pl.ds(pl.multiple_of(b * 8, 16), 16)
                both = disp8[h, at, :]
                left = jnp.concatenate(
                    [jnp.where(upper, both, 0.0), jnp.where(upper, 0.0, both)], axis=1
                ).astype(bf16)
                shift = dot(left, jnp.concatenate([flip[b, cut, :], flip[b + 1, cut, :]], axis=0))
                if h > 0:
                    shift = shift + rows_of(moved.at[j], at)
                set_rows(moved.at[j], at, shift)
                if h == parts - 1:
                    load = rows_of(tr8, at) - rows_of(ms8, at) * shift
                    load8[i * (size // 2) + u // 2] = load.astype(bf16)

        def forward(h):
            def step(i, c):
                if h == 0:
                    @pl.when(i == nchunk // 2)
                    def _():
                        relay(j, 1)

                move(i, CHUNK, h)
                return c

            lax.fori_loop(0, nchunk, step, 0)

        def backward(h, size):
            cut = slice(h * LANES, (h + 1) * LANES)

            def back(i, c):
                if h > 0:
                    @pl.when(i == blocks // size - 1)
                    def _():
                        spread_out(h - 1)

                for u in range(0, size, 2):
                    b = i * size + u
                    at = pl.multiple_of(b * 8, 16)
                    right = jnp.concatenate([rbf[b, :, cut], rbf[b + 1, :, cut]], axis=1)
                    both = dot(load8[i * (size // 2) + u // 2], right)
                    map8[h, pl.ds(at, 8), :] = both[0:8, 0:LANES]
                    map8[h, pl.ds(at + 8, 8), :] = both[8:16, LANES:2 * LANES]
                return c

            lax.fori_loop(0, blocks // size, back, 0)

        def copy_a(h):
            return remote(send_a.at[h], recv_a.at[h], ra_s.at[h], ra_r.at[h], xy, other, z)

        def copy_b(h, k):
            return remote(
                send_b.at[h, k], recv_b.at[h, k], rb_s.at[h, k], rb_r.at[h, k],
                targets[k][0], core, targets[k][1],
            )

        def gather_up(h):
            for q in range(0, ngroup, 2):
                size = min(2, ngroup - q)
                for c in range(3):
                    rows = [map8[h, strided(q + k, c), :] for k in range(size)]
                    value = jnp.concatenate(rows, axis=0) if size > 1 else rows[0]
                    mapn[h, q * 8:(q + size) * 8, thin_of(c)] = value.astype(bf16)
            send_a[h] = dot(collect[1], mapn[h]).reshape(chips, shells, thin).astype(bf16)
            copy_a(h).start()
            part[h] = dot(collect[0], mapn[h]).reshape(chips, shells, thin)

        def spread_out(h):
            copy_a(h).wait_recv()
            for k in range(far):
                at = chip(*targets[k])
                send_b[h, k] = (part[h, at] + recv_a[h, at].astype(f32)).astype(bf16)
                copy_b(h, k).start()

        relay(j, 0)
        fetch(0)
        forward(0)
        fetch(1)
        forward(1)
        backward(0, CHUNK)
        gather_up(0)
        backward(1, TAIL)
        gather_up(1)
        spread_out(1)

        @pl.when(j > 0)
        def _():
            coefficients(j)
            for copy in scalar_copies(j):
                copy.wait_send()

        for h in range(parts):
            cur[h] = blend(xcur[h], wx, h)
        for h in range(parts):
            for k in range(far):
                ag(j, h, k).wait_send()
            for k in range(far + 1):
                ag_pair(j, h, k).wait_send()
            copy_a(h).wait_send()

        @pl.when(j == 0)
        def _():
            inv_copy().wait()

        def forcing(h):
            shell_load = part[h, me] + recv_a[h, me].astype(f32)
            for k in reversed(range(far)):
                copy_b(h, k).wait_recv()
                shell_load = shell_load + recv_b[h, k].astype(f32)
            return (shell_load + robin[h] * xcur[h]).astype(bf16)

        def table(s, c, h, lanes):
            return inv[s, lanes_of(c, h), lanes]

        row = lax.broadcasted_iota(jnp.int32, (shells, LANES), 0)

        def tail_left(force, s):
            last = force[:, thin_of(2)].astype(f32)
            return jnp.concatenate(
                [jnp.where(row == s, last, 0.0), jnp.where(row == s + 1, last, 0.0)], axis=1
            )

        def tail_right(s, h, lanes):
            return jnp.concatenate([table(s, 2, h, lanes), table(s + 1, 2, h, lanes)], axis=0)

        def lead_right(s, h, lanes):
            return jnp.concatenate([table(s, 0, h, lanes), table(s, 1, h, lanes)], axis=0)

        force = forcing(0)
        shell_row = lax.broadcasted_iota(jnp.int32, (shells, breadth), 0)
        whole = slice(0, breadth)
        early = jnp.zeros((shells, breadth), f32)
        for s in range(shells):
            lead = dot(force[:, 0:2 * LANES], lead_right(s, 0, whole))
            early = jnp.where(shell_row == s, lead, early)
        for s in range(0, shells, 2):
            early = early + dot(tail_left(force, s).astype(bf16), tail_right(s, 0, whole))
        force = forcing(1)
        shell_row = lax.broadcasted_iota(jnp.int32, (shells, thin), 0)
        for h in range(parts):
            def wide_right(pieces):
                return jnp.concatenate(
                    [make(lanes_of(c, h)) for make in pieces for c in range(3)], axis=1
                )

            image = jnp.zeros((shells, thin), f32)
            for s in range(0, shells, 2):
                both = dot(force[:, 0:2 * LANES], wide_right(
                    [functools.partial(lead_right, s, 1), functools.partial(lead_right, s + 1, 1)]
                ))
                image = jnp.where(shell_row == s, both[:, 0:thin], image)
                image = jnp.where(shell_row == s + 1, both[:, thin:2 * thin], image)
            for s in range(0, shells, 4):
                left = jnp.concatenate([tail_left(force, s), tail_left(force, s + 2)], axis=0)
                both = dot(left.astype(bf16), wide_right(
                    [functools.partial(tail_right, s, 1), functools.partial(tail_right, s + 2, 1)]
                ))
                image = image + both[0:shells, 0:thin] + both[shells:2 * shells, thin:2 * thin]
            image = image + jnp.concatenate([early[:, lanes_of(c, h)] for c in range(3)], axis=1)
            wp[lax.rem(j + ITERS - 1, ITERS), h] = image - pprev[h]
            pprev[h] = image
            xcur[h] = blend(image, wp, h)

            @pl.when(j < ITERS - 1)
            def _():
                share(j + 1, h)

        scalars(j + 1)
        note(j + 1)
        for h in range(parts):
            for k in range(far):
                copy_b(h, k).wait_send()
        return carry

    lax.fori_loop(0, ITERS, iteration, 0)
    weights = []
    for i in range(ITERS):
        value = 1.0 if i == ITERS - 1 else -cb[i]
        value = value + cb[i - 1] if i > 0 else value
        weights.append(value)
    for q in range(0, ngroup, 2):
        size = min(2, ngroup - q)
        rows = slice(q * 8, (q + size) * 8)
        for c in range(3):
            for h in range(parts):
                shift = None
                for i in range(ITERS):
                    term = [moved[i, h, strided(q + k, c), :] for k in range(size)]
                    term = weights[i] * (jnp.concatenate(term, axis=0) if size > 1 else term[0])
                    shift = term if shift is None else shift + term
                lanes = lanes_of(c, h)
                load = tr_ref[rows, lanes].astype(f32) - ms_ref[rows, lanes].astype(f32) * shift
                load_buf[rows, lanes] = load.astype(bf16)
    write = pltpu.make_async_copy(load_buf, load_out, out_sem)
    write.start()
    coefficients(ITERS)
    for h in range(parts):
        last = blend(xcur[h], wx, h)
        for c in range(3):
            cur_out[:, lanes_of(c, h)] = last[:, thin_of(c)]
    for copy in scalar_copies(ITERS):
        copy.wait_send()
    write.wait()


def hand_over(current, load, norms, current_out, load_out, norm_out):
    current_out[...] = current[...]
    load_out[...] = load[...]
    for i in range(norm_out.shape[0]):
        norm_out[i] = norms[i, 0, 0]


def fused(nf, nz, rbf_blocks, fluid_traction, fluid_mass, route, slot, shell_inverse, robin_coef, shell_start):
    f32, bf16 = jnp.float32, jnp.bfloat16
    blocks, nodes, _ = rbf_blocks.shape
    shells, breadth = shell_start.shape
    chips = nf // 2 * nz
    half = chips * shells
    far = chips - 1
    padded = -(-blocks // LANES) * LANES
    dma = pltpu.SemaphoreType.DMA
    vmem = pl.BlockSpec(memory_space=pltpu.VMEM)
    anywhere = pl.BlockSpec(memory_space=pl.ANY)
    parts = nodes // LANES
    thin = 3 * LANES
    plain = pltpu.VMEM((shells, breadth), f32)
    state = pltpu.VMEM((parts, shells, thin), f32)
    history = pltpu.VMEM((ITERS, parts, shells, thin), f32)
    wide = pltpu.VMEM((parts, blocks * 8, LANES), f32)
    exchange = pltpu.VMEM((parts, chips, shells, thin), bf16)
    current, load, norms = pl.pallas_call(
        functools.partial(kernel, nf, nz, blocks, nodes, shells, 2 * half * breadth),
        out_shape=(
            jax.ShapeDtypeStruct((shells, breadth), f32),
            jax.ShapeDtypeStruct((blocks, breadth), bf16),
            jax.ShapeDtypeStruct((ITERS, 1, LANES), f32),
        ),
        in_specs=[anywhere] * 8,
        out_specs=(vmem, anywhere, vmem),
        scratch_shapes=[
            plain,
            pltpu.VMEM((1, blocks), jnp.int32),
            pltpu.VMEM((1, blocks), jnp.int32),
            pltpu.VMEM((blocks, breadth), bf16),
            pltpu.VMEM((blocks, breadth), bf16),
            plain,
            pltpu.VMEM((blocks, breadth), bf16),
            pltpu.VMEM(rbf_blocks.shape, bf16),
            pltpu.VMEM(rbf_blocks.shape, bf16),
            pltpu.VMEM(shell_inverse.shape, bf16),
            pltpu.VMEM((ITERS, parts, 2, chips, shells, thin), bf16),
            pltpu.VMEM((ITERS + 1, 2, chips, 1, LANES), f32),
            state, state, state, state, state, state,
            history, history, history,
            pltpu.VMEM((ITERS + 1, 1, LANES), f32),
            pltpu.VMEM((ITERS, 1, LANES), f32),
            pltpu.VMEM((2, blocks, half), bf16),
            pltpu.VMEM((2, half, padded), bf16),
            wide, wide, wide, wide,
            pltpu.VMEM((blocks // 2, 16, nodes), bf16),
            pltpu.VMEM((ITERS, parts, blocks * 8, LANES), f32),
            pltpu.VMEM((parts, padded, thin), bf16),
            pltpu.VMEM((parts, chips, shells, thin), f32),
            exchange, exchange, exchange, exchange,
            dma((6,)), dma,
            dma((blocks // LOAD,)),
            dma,
            dma((parts, far)), dma((parts, far)),
            dma((parts, far + 1)), dma((parts, far + 1)),
            dma((2, far + 1, 2)), dma((2, far + 1, 2)),
            dma((parts,)), dma((parts,)),
            dma((parts, far)), dma((parts, far)),
        ],
        compiler_params=pltpu.CompilerParams(
            collective_id=0, has_side_effects=True, vmem_limit_bytes=VMEM_BYTES
        ),
        name="coupling",
    )(
        shell_start, route.T, slot[None, :], fluid_traction, fluid_mass, robin_coef, rbf_blocks,
        shell_inverse,
    )
    smem = pl.BlockSpec(memory_space=pltpu.SMEM)
    return pl.pallas_call(
        hand_over,
        out_shape=(
            jax.ShapeDtypeStruct(current.shape, f32),
            jax.ShapeDtypeStruct(load.shape, bf16),
            jax.ShapeDtypeStruct((ITERS,), f32),
        ),
        in_specs=[vmem, vmem, smem],
        out_specs=(vmem, vmem, smem),
        name="results",
    )(current, load, norms)


def choose(nf, nz):
    def body(rbf_blocks, *others):
        if nf * nz > 32:
            return per_device(rbf_blocks, *others)
        return fused(nf, nz, rbf_blocks, *others)

    return body


def solution(mesh):
    in_specs = (
        P(("fluid", "solid"), None, None),
        P(("fluid", "solid"), None),
        P(("fluid", "solid"), None),
        P(("fluid", "solid"), None),
        P(("fluid", "solid")),
        P(("fluid", "solid"), None, None),
        P(("fluid", "solid"), None),
        P(("fluid", "solid"), None),
    )
    out_specs = (P(("fluid", "solid"), None), P(("fluid", "solid"), None), P())
    return jax.shard_map(
        choose(mesh.shape["fluid"], mesh.shape["solid"]), mesh=mesh, in_specs=in_specs, out_specs=out_specs, check_vma=False
    )
```

```python
import functools

import jax
import jax.numpy as jnp
from jax import lax
from jax.experimental import pallas as pl
from jax.experimental.pallas import tpu as pltpu
from jax.sharding import PartitionSpec as P

ITERS = 6


RELAX = 0.3
EPSILON = 1e-06


def transport(buffer, devices, capacity):
    breadth = buffer.shape[1]
    moved = lax.all_to_all(
        buffer.reshape(devices, capacity, breadth),
        ("fluid", "solid"),
        split_axis=0,
        concat_axis=0,
        tiled=True,
    )
    return moved.reshape(devices * capacity, breadth)


def least_squares(gram, target_side):
    order = gram.shape[0]
    lower = [[None] * order for _ in range(order)]
    for row in range(order):
        for column in range(row + 1):
            total = gram[row, column]
            for inner in range(column):
                total = total - lower[row][inner] * lower[column][inner]
            if row == column:
                lower[row][row] = jnp.sqrt(total)
            else:
                lower[row][column] = total / lower[column][column]
    middle = []
    for row in range(order):
        total = target_side[row]
        for inner in range(row):
            total = total - lower[row][inner] * middle[inner]
        middle.append(total / lower[row][row])
    result = [None] * order
    for row in reversed(range(order)):
        total = middle[row]
        for inner in range(row + 1, order):
            total = total - lower[inner][row] * result[inner]
        result[row] = total / lower[row][row]
    return jnp.stack(result)


def per_device(
    rbf_blocks, fluid_traction, fluid_mass, route, slot, shell_inverse, robin_coef, shell_start
):
    devices = lax.axis_size("fluid") * lax.axis_size("solid")
    blocks = rbf_blocks.shape[0]
    nodes = rbf_blocks.shape[1]
    breadth = 3 * nodes
    shells = shell_inverse.shape[0]
    capacity = max(2, 2 * blocks // devices)
    slots_all = devices * capacity
    destination = route[:, 0]
    block_order = jnp.arange(blocks, dtype=jnp.int32)
    earlier = (destination[:, None] == destination[None, :]) & (
        block_order[None, :] < block_order[:, None]
    )
    slot_rank = jnp.sum(earlier.astype(jnp.int32), axis=1)
    position = destination * capacity + slot_rank
    positions = jnp.arange(slots_all, dtype=jnp.int32)
    placing = positions[:, None] == position[None, :]
    place_out = placing.astype(jnp.bfloat16)
    place_in = (position[:, None] == positions[None, :]).astype(jnp.bfloat16)
    wanted = jnp.max(jnp.where(placing, slot[None, :] + 1, 0), axis=1) - 1
    asked = lax.all_to_all(
        wanted.reshape(devices, capacity),
        ("fluid", "solid"),
        split_axis=0,
        concat_axis=0,
        tiled=True,
    ).reshape(slots_all)
    shell_ids = jnp.arange(shells, dtype=jnp.int32)
    picking = (asked[:, None] == shell_ids[None, :]).astype(jnp.bfloat16)
    collecting = (shell_ids[:, None] == asked[None, :]).astype(jnp.bfloat16)
    traction = fluid_traction.astype(jnp.float32)
    massive = fluid_mass.astype(jnp.float32)
    count = shells * devices * breadth
    current = shell_start
    residuals = []
    images = []
    norms = []
    last_load = None
    for iteration in range(ITERS):
        current_half = current.astype(jnp.bfloat16)
        outgoing = jnp.dot(picking, current_half, preferred_element_type=jnp.float32).astype(
            jnp.bfloat16
        )
        incoming = transport(outgoing, devices, capacity)
        displaced = jnp.dot(place_in, incoming, preferred_element_type=jnp.float32).astype(
            jnp.bfloat16
        )
        moved = jnp.einsum(
            "bcj,bij->bci",
            displaced.reshape(blocks, 3, nodes),
            rbf_blocks,
            preferred_element_type=jnp.float32,
        ).reshape(blocks, breadth)
        load = (traction - massive * moved).astype(jnp.bfloat16)
        last_load = load
        mapped = (
            jnp.einsum(
                "bci,bij->bcj",
                load.reshape(blocks, 3, nodes),
                rbf_blocks,
                preferred_element_type=jnp.float32,
            )
            .reshape(blocks, breadth)
            .astype(jnp.bfloat16)
        )
        sending = jnp.dot(place_out, mapped, preferred_element_type=jnp.float32).astype(
            jnp.bfloat16
        )
        arrived = transport(sending, devices, capacity)
        shell_load = jnp.dot(collecting, arrived, preferred_element_type=jnp.float32)
        forcing = (shell_load + robin_coef * current).astype(jnp.bfloat16)
        image = jnp.einsum("bi,bij->bj", forcing, shell_inverse, preferred_element_type=jnp.float32)
        residual = image - current
        residuals.append(residual)
        images.append(image)
        squares_local = jnp.sum(residual * residual)
        if iteration == 0:
            gram_local = jnp.zeros((1, 1), jnp.float32)
            rhs_local = jnp.zeros((1,), jnp.float32)
        else:
            changes = jnp.stack(
                [(residuals[i + 1] - residuals[i]).reshape(-1) for i in range(iteration)]
            )
            gram_local = jnp.dot(changes, changes.T, precision=lax.Precision.HIGHEST)
            rhs_local = jnp.dot(changes, residual.reshape(-1), precision=lax.Precision.HIGHEST)
        gram, rhs, squares = lax.psum((gram_local, rhs_local, squares_local), ("fluid", "solid"))
        norms.append(jnp.sqrt(squares / count + EPSILON))
        if iteration == 0:
            current = current + RELAX * residual
        else:
            image_changes = jnp.stack([images[i + 1] - images[i] for i in range(iteration)])
            coefs = least_squares(gram, -rhs)
            current = image + jnp.tensordot(
                coefs, image_changes, axes=1, precision=lax.Precision.HIGHEST
            )
    return (current, last_load, jnp.stack(norms))


LOAD = 8
FIRST = 0
LAST = 52
LANES = 128
VMEM_BYTES = 67043328
MESH = pl.DeviceIdType.MESH


def kernel(
    nf, nz, blocks, nodes, shells, count,
    start_hbm, route_hbm, slot_hbm, tr_hbm, ms_hbm, robin_hbm, rbf_hbm, inv_hbm,
    cur_out, load_out, norm_out,
    start_ref, route_ref, slot_ref, tr_ref, ms_ref, robin_ref, load_buf,
    rbf, flip, inv, gath, scal, xcur, xprev, pprev, cur, rprev, robin, wx, wp, vhist, sc, cb,
    place, collect, tr8, ms8, disp8, map8, load8, moved, mapn, part,
    send_a, recv_a, send_b, recv_b,
    in_sem, out_sem, rbf_sem, inv_sem, ag_s, ag_r, pr_s, pr_r, sl_s, sl_r, ra_s, ra_r, rb_s, rb_r,
):
    f32, bf16 = jnp.float32, jnp.bfloat16
    parts = nodes // LANES
    thin = 3 * LANES
    breadth = 3 * nodes
    nxy = nf // 2
    nx = 2 if nxy % 2 == 0 else 1
    ny = nxy // nx
    chips = nxy * nz
    half = chips * shells
    group = nz * shells
    f = lax.axis_index("fluid")
    z = lax.axis_index("solid")
    core = lax.rem(f, 2)
    other = 1 - core
    xy = f // 2
    x, y = lax.rem(xy, nx), xy // nx
    nload = blocks // LOAD
    ngroup = blocks // 8

    nb = 2 if nz % 2 == 0 else 1
    na = nz // nb

    def hops(step):
        ey, ex, ea, eb = step
        return ey + ex + ea * nb + eb

    steps = sorted(
        [
            (ey, ex, ea, eb)
            for ey in range(ny) for ex in range(nx) for ea in range(na) for eb in range(nb)
            if ey + ex + ea + eb
        ],
        key=hops, reverse=True,
    )
    far = len(steps)

    def away(step, sign=1):
        ey, ex, ea, eb = step
        plane = lax.rem(y + sign * ey + ny, ny) * nx + lax.rem(x + sign * ex + nx, nx)
        depth = lax.rem(z // nb + sign * ea + na, na) * nb + lax.rem(lax.rem(z, nb) + sign * eb + nb, nb)
        return plane, depth

    targets = [away(s) for s in steps]
    sources = [away(s, -1) for s in steps]

    def chip(plane, depth):
        return plane * nz + depth

    me = chip(xy, z)

    def remote(src, dst, send_sem, recv_sem, plane, unit, depth):
        return pltpu.make_async_remote_copy(
            src_ref=src, dst_ref=dst, send_sem=send_sem, recv_sem=recv_sem,
            device_id=(plane * 2 + unit, depth), device_id_type=MESH,
        )

    first = pltpu.make_async_copy(start_hbm, start_ref, in_sem.at[0])
    first.start()
    barrier = pltpu.get_barrier_semaphore()
    for plane, depth in targets + [(xy, z)]:
        for unit in (core, other):
            if plane is xy and unit is core:
                continue
            pl.semaphore_signal(
                barrier, inc=1, device_id=(plane * 2 + unit, depth), device_id_type=MESH
            )

    def rbf_copy(i):
        at = pl.ds(i * LOAD, LOAD)
        return pltpu.make_async_copy(rbf_hbm.at[at], rbf.at[at], rbf_sem.at[i])

    def inv_copy():
        return pltpu.make_async_copy(inv_hbm, inv, inv_sem)

    smalls = [
        pltpu.make_async_copy(src, dst, in_sem.at[i + 1])
        for i, (src, dst) in enumerate((
            (route_hbm, route_ref), (slot_hbm, slot_ref), (tr_hbm, tr_ref),
            (ms_hbm, ms_ref), (robin_hbm, robin_ref),
        ))
    ]
    for copy in smalls:
        copy.start()
    for i in range(nload):
        rbf_copy(i).start()
    inv_copy().start()

    def lanes_of(c, h):
        return slice(c * nodes + h * LANES, c * nodes + (h + 1) * LANES)

    def thin_of(c):
        return slice(c * LANES, (c + 1) * LANES)

    def halved(ref, h):
        return jnp.concatenate([ref[:, lanes_of(c, h)] for c in range(3)], axis=1)

    def ag(j, h, k, incoming=False):
        at = chip(*sources[k]) if incoming else me
        block = gath.at[j, h, core, at]
        return remote(
            block, block, ag_s.at[h, k], ag_r.at[h, k], targets[k][0], core, targets[k][1]
        )

    def ag_pair(j, h, k, incoming=False):
        at = me if k == far else chip(*sources[k])
        block = gath.at[j, h, other if incoming else core, at]
        return remote(block, block, pr_s.at[h, k], pr_r.at[h, k], xy, other, z)

    def share(j, h):
        gath[j, h, core, me] = xcur[h].astype(bf16)
        for k in range(far):
            ag(j, h, k).start()
        ag_pair(j, h, far).start()

    def relay(j, h):
        for k in reversed(range(far)):
            ag(j, h, k, True).wait_recv()
            ag_pair(j, h, k).start()

    first.wait()
    for h in range(parts):
        xcur[h] = halved(start_ref, h)
    pl.semaphore_wait(barrier, 2 * far + 1)
    for h in range(parts):
        share(0, h)

    xprev[...] = xcur[...]
    for ref in (pprev, cur, rprev, wx, wp, vhist, sc, cb):
        ref[...] = jnp.zeros(ref.shape, ref.dtype)
    mapn[...] = jnp.zeros(mapn.shape, bf16)

    def clear(i, c):
        at = pl.ds(pl.multiple_of(i * 64, 64), 64)
        for ref in (tr8, ms8, disp8):
            ref[:, at, :] = jnp.zeros((parts, 64, LANES), f32)
        return c

    lax.fori_loop(0, ngroup, clear, 0)
    for copy in smalls:
        copy.wait()
    for h in range(parts):
        robin[h] = halved(robin_ref, h)

    def strided(q, c):
        return pl.ds(q * 64 + c, 8, stride=8)

    def rows_of(ref, at):
        return jnp.concatenate([ref[p, at, :] for p in range(parts)], axis=1)

    def set_rows(ref, at, value):
        for p in range(parts):
            ref[p, at, :] = value[:, p * LANES:(p + 1) * LANES]

    for src, dst in ((tr_ref, tr8), (ms_ref, ms8)):
        for row in range(0, blocks, 16):
            size = min(16, blocks - row)
            wide = src[row:row + size, :].astype(f32)
            for k in range(size // 8):
                for c in range(3):
                    for h in range(parts):
                        dst[h, strided(row // 8 + k, c), :] = wide[k * 8:(k + 1) * 8, lanes_of(c, h)]

    diagonal = lax.broadcasted_iota(jnp.int32, (blocks, blocks), 0) == lax.broadcasted_iota(
        jnp.int32, (blocks, blocks), 1
    )
    target = (route_ref[...] * shells + slot_ref[...]).astype(f32)
    column = jnp.sum(jnp.where(diagonal, target, 0.0), axis=1, keepdims=True)
    for side in range(2):
        unit = core if side == 0 else other
        line = lax.broadcasted_iota(jnp.int32, (half, 1), 0)
        ids = (line // group * 2 + unit) * group + lax.rem(line, group)
        collect[side] = jnp.zeros(collect.shape[1:], bf16)
        collect[side, :, 0:blocks] = jnp.where(ids.astype(f32) == target, 1.0, 0.0).astype(bf16)
        lane = lax.broadcasted_iota(jnp.int32, (1, half), 1)
        ids = (lane // group * 2 + unit) * group + lax.rem(lane, group)
        place[side] = jnp.where(ids.astype(f32) == column, 1.0, 0.0).astype(bf16)

    def turn(i, c):
        rbf_copy(i).wait()
        for u in range(LOAD):
            flip[i * LOAD + u] = rbf[i * LOAD + u].T
        return c

    lax.fori_loop(0, nload, turn, 0)
    lane = lax.broadcasted_iota(jnp.int32, (1, LANES), 1)

    def pick(vector, q):
        return jnp.sum(jnp.where(lane == q, vector, 0.0), axis=1, keepdims=True)

    def dot(a, b):
        return jnp.dot(a, b, preferred_element_type=f32)

    def scalar_copies(j, incoming=False):
        copies = []
        turn = lax.rem(j, 2)
        for k in range(far + 1):
            for unit in range(2):
                if k == far and unit == 0:
                    continue
                at = (me if k == far else chip(*sources[k])) if incoming else me
                mine = (core if unit == 0 else other) if incoming else core
                plane, depth = (xy, z) if k == far else targets[k]
                block = scal.at[j, mine, at]
                copies.append(remote(
                    block, block, sl_s.at[turn, k, unit], sl_r.at[turn, k, unit],
                    plane, core if unit == 0 else other, depth,
                ))
        return copies

    def scalars(j):
        residual = xcur[...] - cur[...]
        newest = residual - rprev[...]
        rprev[...] = residual
        vhist[lax.rem(j + ITERS - 2, ITERS)] = newest

        def total(product):
            rows = jnp.sum(jnp.sum(product, axis=0), axis=0, keepdims=True)
            return jnp.sum(rows, axis=1, keepdims=True)

        vector = jnp.where(lane == 0, total(residual * residual), 0.0)
        for i in range(ITERS - 1):
            vector = jnp.where(lane == 1 + i, total(vhist[i] * residual), vector)
            vector = jnp.where(lane == 8 + i, total(vhist[i] * newest), vector)
        scal[j, core, me] = vector
        for copy in scalar_copies(j):
            copy.start()

    def coefficients(j):
        for copy in scalar_copies(j, True):
            copy.wait_recv()
        k = j - 1
        total = jnp.sum(jnp.sum(scal[j], axis=0), axis=0)
        sc[j] = total
        norm = jnp.sqrt(pick(total, 0) / count + EPSILON)
        norm_out[k] = jnp.broadcast_to(norm, (1, LANES))

        order = ITERS - 1
        gram = [[None] * order for _ in range(order)]
        for col in range(order):
            vector = sc[col + 2]
            for row in range(col + 1):
                value = pick(vector, 8 + row)
                if row == col:
                    value = jnp.where(col < k, value, 1.0)
                gram[col][row] = value
        side = [-pick(total, 1 + i) for i in range(order)]
        lower = [[None] * order for _ in range(order)]
        for row in range(order):
            for col in range(row + 1):
                value = gram[row][col]
                for inner in range(col):
                    value = value - lower[row][inner] * lower[col][inner]
                if row == col:
                    lower[row][row] = jnp.sqrt(value)
                else:
                    lower[row][col] = value / lower[col][col]
        middle = []
        for row in range(order):
            value = side[row]
            for inner in range(row):
                value = value - lower[row][inner] * middle[inner]
            middle.append(value / lower[row][row])
        result = [None] * order
        for row in reversed(range(order)):
            value = middle[row]
            for inner in range(row + 1, order):
                value = value - lower[inner][row] * result[inner]
            result[row] = value / lower[row][row]
        relax = jnp.where(j == 1, jnp.full((1, 1), RELAX - 1.0, f32), 0.0)
        for i, value in enumerate([relax] + result):
            cb[i] = jnp.broadcast_to(value, (1, LANES))

    def blend(newest, history, h):
        value = newest
        for i in range(ITERS):
            value = value + jnp.concatenate([cb[i]] * 3, axis=1) * history[i, h]
        return value

    def note(j):
        wx[lax.rem(j + ITERS - 1, ITERS)] = xcur[...] - xprev[...]
        xprev[...] = xcur[...]

    upper = lax.broadcasted_iota(jnp.int32, (16, LANES), 0) < 8

    def iteration(j, carry):
        def fetch(h):
            def side(unit):
                return gath[j, h, unit].reshape(half, thin)

            picked = dot(place[0], side(core))
            for k in range(far + 1):
                ag_pair(j, h, k, True).wait_recv()
            picked = picked + dot(place[1], side(other))
            for q in range(ngroup):
                for c in range(3):
                    disp8[h, strided(q, c), :] = picked[q * 8:(q + 1) * 8, thin_of(c)]

        def move(begin, end, h):
            cut = slice(h * LANES, (h + 1) * LANES)
            for b in range(begin, end, 2):
                at = pl.ds(b * 8, 16)
                both = disp8[h, at, :]
                left = jnp.concatenate(
                    [jnp.where(upper, both, 0.0), jnp.where(upper, 0.0, both)], axis=1
                ).astype(bf16)
                shift = dot(left, jnp.concatenate([flip[b, cut, :], flip[b + 1, cut, :]], axis=0))
                if h > 0:
                    shift = shift + rows_of(moved.at[j], at)
                set_rows(moved.at[j], at, shift)
                if h == parts - 1:
                    load = rows_of(tr8, at) - rows_of(ms8, at) * shift
                    load8[b // 2] = load.astype(bf16)

        def back(begin, end, h):
            cut = slice(h * LANES, (h + 1) * LANES)
            for b in range(begin, end, 2):
                right = jnp.concatenate([rbf[b, :, cut], rbf[b + 1, :, cut]], axis=1)
                both = dot(load8[b // 2], right)
                map8[h, pl.ds(b * 8, 8), :] = both[0:8, 0:LANES]
                map8[h, pl.ds(b * 8 + 8, 8), :] = both[8:16, LANES:2 * LANES]

        def copy_a(h):
            return remote(send_a.at[h], recv_a.at[h], ra_s.at[h], ra_r.at[h], xy, other, z)

        def copy_b(h, k):
            return remote(
                send_b.at[h, k], recv_b.at[h, k], rb_s.at[h, k], rb_r.at[h, k],
                targets[k][0], core, targets[k][1],
            )

        def gather_up(h):
            for q in range(0, ngroup, 2):
                size = min(2, ngroup - q)
                for c in range(3):
                    rows = [map8[h, strided(q + k, c), :] for k in range(size)]
                    value = jnp.concatenate(rows, axis=0) if size > 1 else rows[0]
                    mapn[h, q * 8:(q + size) * 8, thin_of(c)] = value.astype(bf16)
            send_a[h] = dot(collect[1], mapn[h]).reshape(chips, shells, thin).astype(bf16)
            copy_a(h).start()
            part[h] = dot(collect[0], mapn[h]).reshape(chips, shells, thin)

        def spread_out(h):
            copy_a(h).wait_recv()
            for k in range(far):
                at = chip(*targets[k])
                send_b[h, k] = (part[h, at] + recv_a[h, at].astype(f32)).astype(bf16)
                copy_b(h, k).start()

        relay(j, 0)
        fetch(0)
        move(0, FIRST, 0)
        relay(j, 1)
        move(FIRST, blocks, 0)
        fetch(1)
        move(0, blocks, 1)
        back(0, blocks, 0)
        gather_up(0)
        back(0, LAST, 1)
        spread_out(0)
        back(LAST, blocks, 1)
        gather_up(1)
        spread_out(1)

        @pl.when(j > 0)
        def _():
            coefficients(j)
            for copy in scalar_copies(j):
                copy.wait_send()

        for h in range(parts):
            cur[h] = blend(xcur[h], wx, h)
        for h in range(parts):
            for k in range(far):
                ag(j, h, k).wait_send()
            for k in range(far + 1):
                ag_pair(j, h, k).wait_send()
            copy_a(h).wait_send()

        @pl.when(j == 0)
        def _():
            inv_copy().wait()

        def forcing(h):
            shell_load = part[h, me] + recv_a[h, me].astype(f32)
            for k in reversed(range(far)):
                copy_b(h, k).wait_recv()
                shell_load = shell_load + recv_b[h, k].astype(f32)
            return (shell_load + robin[h] * xcur[h]).astype(bf16)

        def table(s, c, h, lanes):
            return inv[s, lanes_of(c, h), lanes]

        row = lax.broadcasted_iota(jnp.int32, (shells, LANES), 0)

        def tail_left(force, s):
            last = force[:, thin_of(2)].astype(f32)
            return jnp.concatenate(
                [jnp.where(row == s, last, 0.0), jnp.where(row == s + 1, last, 0.0)], axis=1
            )

        def tail_right(s, h, lanes):
            return jnp.concatenate([table(s, 2, h, lanes), table(s + 1, 2, h, lanes)], axis=0)

        def lead_right(s, h, lanes):
            return jnp.concatenate([table(s, 0, h, lanes), table(s, 1, h, lanes)], axis=0)

        force = forcing(0)
        shell_row = lax.broadcasted_iota(jnp.int32, (shells, breadth), 0)
        whole = slice(0, breadth)
        early = jnp.zeros((shells, breadth), f32)
        for s in range(shells):
            lead = dot(force[:, 0:2 * LANES], lead_right(s, 0, whole))
            early = jnp.where(shell_row == s, lead, early)
        for s in range(0, shells, 2):
            early = early + dot(tail_left(force, s).astype(bf16), tail_right(s, 0, whole))
        force = forcing(1)
        shell_row = lax.broadcasted_iota(jnp.int32, (shells, thin), 0)
        for h in range(parts):
            def wide_right(pieces):
                return jnp.concatenate(
                    [make(lanes_of(c, h)) for make in pieces for c in range(3)], axis=1
                )

            image = jnp.zeros((shells, thin), f32)
            for s in range(0, shells, 2):
                both = dot(force[:, 0:2 * LANES], wide_right(
                    [functools.partial(lead_right, s, 1), functools.partial(lead_right, s + 1, 1)]
                ))
                image = jnp.where(shell_row == s, both[:, 0:thin], image)
                image = jnp.where(shell_row == s + 1, both[:, thin:2 * thin], image)
            for s in range(0, shells, 4):
                left = jnp.concatenate([tail_left(force, s), tail_left(force, s + 2)], axis=0)
                both = dot(left.astype(bf16), wide_right(
                    [functools.partial(tail_right, s, 1), functools.partial(tail_right, s + 2, 1)]
                ))
                image = image + both[0:shells, 0:thin] + both[shells:2 * shells, thin:2 * thin]
            image = image + jnp.concatenate([early[:, lanes_of(c, h)] for c in range(3)], axis=1)
            wp[lax.rem(j + ITERS - 1, ITERS), h] = image - pprev[h]
            pprev[h] = image
            xcur[h] = blend(image, wp, h)

            @pl.when(j < ITERS - 1)
            def _():
                share(j + 1, h)

        scalars(j + 1)
        note(j + 1)
        for h in range(parts):
            for k in range(far):
                copy_b(h, k).wait_send()
        return carry

    lax.fori_loop(0, ITERS, iteration, 0)
    weights = []
    for i in range(ITERS):
        value = 1.0 if i == ITERS - 1 else -cb[i]
        value = value + cb[i - 1] if i > 0 else value
        weights.append(value)
    for q in range(0, ngroup, 2):
        size = min(2, ngroup - q)
        rows = slice(q * 8, (q + size) * 8)
        for c in range(3):
            for h in range(parts):
                shift = None
                for i in range(ITERS):
                    term = [moved[i, h, strided(q + k, c), :] for k in range(size)]
                    term = weights[i] * (jnp.concatenate(term, axis=0) if size > 1 else term[0])
                    shift = term if shift is None else shift + term
                lanes = lanes_of(c, h)
                load = tr_ref[rows, lanes].astype(f32) - ms_ref[rows, lanes].astype(f32) * shift
                load_buf[rows, lanes] = load.astype(bf16)
    write = pltpu.make_async_copy(load_buf, load_out, out_sem)
    write.start()
    coefficients(ITERS)
    for h in range(parts):
        last = blend(xcur[h], wx, h)
        for c in range(3):
            cur_out[:, lanes_of(c, h)] = last[:, thin_of(c)]
    for copy in scalar_copies(ITERS):
        copy.wait_send()
    write.wait()


def hand_over(current, load, norms, current_out, load_out, norm_out):
    current_out[...] = current[...]
    load_out[...] = load[...]
    for i in range(norm_out.shape[0]):
        norm_out[i] = norms[i, 0, 0]


def fused(nf, nz, rbf_blocks, fluid_traction, fluid_mass, route, slot, shell_inverse, robin_coef, shell_start):
    f32, bf16 = jnp.float32, jnp.bfloat16
    blocks, nodes, _ = rbf_blocks.shape
    shells, breadth = shell_start.shape
    chips = nf // 2 * nz
    half = chips * shells
    far = chips - 1
    padded = -(-blocks // LANES) * LANES
    dma = pltpu.SemaphoreType.DMA
    vmem = pl.BlockSpec(memory_space=pltpu.VMEM)
    anywhere = pl.BlockSpec(memory_space=pl.ANY)
    parts = nodes // LANES
    thin = 3 * LANES
    plain = pltpu.VMEM((shells, breadth), f32)
    state = pltpu.VMEM((parts, shells, thin), f32)
    history = pltpu.VMEM((ITERS, parts, shells, thin), f32)
    wide = pltpu.VMEM((parts, blocks * 8, LANES), f32)
    exchange = pltpu.VMEM((parts, chips, shells, thin), bf16)
    current, load, norms = pl.pallas_call(
        functools.partial(kernel, nf, nz, blocks, nodes, shells, 2 * half * breadth),
        out_shape=(
            jax.ShapeDtypeStruct((shells, breadth), f32),
            jax.ShapeDtypeStruct((blocks, breadth), bf16),
            jax.ShapeDtypeStruct((ITERS, 1, LANES), f32),
        ),
        in_specs=[anywhere] * 8,
        out_specs=(vmem, anywhere, vmem),
        scratch_shapes=[
            plain,
            pltpu.VMEM((1, blocks), jnp.int32),
            pltpu.VMEM((1, blocks), jnp.int32),
            pltpu.VMEM((blocks, breadth), bf16),
            pltpu.VMEM((blocks, breadth), bf16),
            plain,
            pltpu.VMEM((blocks, breadth), bf16),
            pltpu.VMEM(rbf_blocks.shape, bf16),
            pltpu.VMEM(rbf_blocks.shape, bf16),
            pltpu.VMEM(shell_inverse.shape, bf16),
            pltpu.VMEM((ITERS, parts, 2, chips, shells, thin), bf16),
            pltpu.VMEM((ITERS + 1, 2, chips, 1, LANES), f32),
            state, state, state, state, state, state,
            history, history, history,
            pltpu.VMEM((ITERS + 1, 1, LANES), f32),
            pltpu.VMEM((ITERS, 1, LANES), f32),
            pltpu.VMEM((2, blocks, half), bf16),
            pltpu.VMEM((2, half, padded), bf16),
            wide, wide, wide, wide,
            pltpu.VMEM((blocks // 2, 16, nodes), bf16),
            pltpu.VMEM((ITERS, parts, blocks * 8, LANES), f32),
            pltpu.VMEM((parts, padded, thin), bf16),
            pltpu.VMEM((parts, chips, shells, thin), f32),
            exchange, exchange, exchange, exchange,
            dma((6,)), dma,
            dma((blocks // LOAD,)),
            dma,
            dma((parts, far)), dma((parts, far)),
            dma((parts, far + 1)), dma((parts, far + 1)),
            dma((2, far + 1, 2)), dma((2, far + 1, 2)),
            dma((parts,)), dma((parts,)),
            dma((parts, far)), dma((parts, far)),
        ],
        compiler_params=pltpu.CompilerParams(
            collective_id=0, has_side_effects=True, vmem_limit_bytes=VMEM_BYTES
        ),
        name="coupling",
    )(
        shell_start, route.T, slot[None, :], fluid_traction, fluid_mass, robin_coef, rbf_blocks,
        shell_inverse,
    )
    smem = pl.BlockSpec(memory_space=pltpu.SMEM)
    return pl.pallas_call(
        hand_over,
        out_shape=(
            jax.ShapeDtypeStruct(current.shape, f32),
            jax.ShapeDtypeStruct(load.shape, bf16),
            jax.ShapeDtypeStruct((ITERS,), f32),
        ),
        in_specs=[vmem, vmem, smem],
        out_specs=(vmem, vmem, smem),
        name="results",
    )(current, load, norms)


def choose(nf, nz):
    def body(rbf_blocks, *others):
        if nf * nz > 32:
            return per_device(rbf_blocks, *others)
        return fused(nf, nz, rbf_blocks, *others)

    return body


def solution(mesh):
    in_specs = (
        P(("fluid", "solid"), None, None),
        P(("fluid", "solid"), None),
        P(("fluid", "solid"), None),
        P(("fluid", "solid"), None),
        P(("fluid", "solid")),
        P(("fluid", "solid"), None, None),
        P(("fluid", "solid"), None),
        P(("fluid", "solid"), None),
    )
    out_specs = (P(("fluid", "solid"), None), P(("fluid", "solid"), None), P())
    return jax.shard_map(
        choose(mesh.shape["fluid"], mesh.shape["solid"]), mesh=mesh, in_specs=in_specs, out_specs=out_specs, check_vma=False
    )
```

```python
import functools

import jax
import jax.numpy as jnp
from jax import lax
from jax.experimental import pallas as pl
from jax.experimental.pallas import tpu as pltpu
from jax.sharding import PartitionSpec as P

ITERS = 6


RELAX = 0.3
EPSILON = 1e-06


def transport(buffer, devices, capacity):
    breadth = buffer.shape[1]
    moved = lax.all_to_all(
        buffer.reshape(devices, capacity, breadth),
        ("fluid", "solid"),
        split_axis=0,
        concat_axis=0,
        tiled=True,
    )
    return moved.reshape(devices * capacity, breadth)


def least_squares(gram, target_side):
    order = gram.shape[0]
    lower = [[None] * order for _ in range(order)]
    for row in range(order):
        for column in range(row + 1):
            total = gram[row, column]
            for inner in range(column):
                total = total - lower[row][inner] * lower[column][inner]
            if row == column:
                lower[row][row] = jnp.sqrt(total)
            else:
                lower[row][column] = total / lower[column][column]
    middle = []
    for row in range(order):
        total = target_side[row]
        for inner in range(row):
            total = total - lower[row][inner] * middle[inner]
        middle.append(total / lower[row][row])
    result = [None] * order
    for row in reversed(range(order)):
        total = middle[row]
        for inner in range(row + 1, order):
            total = total - lower[inner][row] * result[inner]
        result[row] = total / lower[row][row]
    return jnp.stack(result)


def per_device(
    rbf_blocks, fluid_traction, fluid_mass, route, slot, shell_inverse, robin_coef, shell_start
):
    devices = lax.axis_size("fluid") * lax.axis_size("solid")
    blocks = rbf_blocks.shape[0]
    nodes = rbf_blocks.shape[1]
    breadth = 3 * nodes
    shells = shell_inverse.shape[0]
    capacity = max(2, 2 * blocks // devices)
    slots_all = devices * capacity
    destination = route[:, 0]
    block_order = jnp.arange(blocks, dtype=jnp.int32)
    earlier = (destination[:, None] == destination[None, :]) & (
        block_order[None, :] < block_order[:, None]
    )
    slot_rank = jnp.sum(earlier.astype(jnp.int32), axis=1)
    position = destination * capacity + slot_rank
    positions = jnp.arange(slots_all, dtype=jnp.int32)
    placing = positions[:, None] == position[None, :]
    place_out = placing.astype(jnp.bfloat16)
    place_in = (position[:, None] == positions[None, :]).astype(jnp.bfloat16)
    wanted = jnp.max(jnp.where(placing, slot[None, :] + 1, 0), axis=1) - 1
    asked = lax.all_to_all(
        wanted.reshape(devices, capacity),
        ("fluid", "solid"),
        split_axis=0,
        concat_axis=0,
        tiled=True,
    ).reshape(slots_all)
    shell_ids = jnp.arange(shells, dtype=jnp.int32)
    picking = (asked[:, None] == shell_ids[None, :]).astype(jnp.bfloat16)
    collecting = (shell_ids[:, None] == asked[None, :]).astype(jnp.bfloat16)
    traction = fluid_traction.astype(jnp.float32)
    massive = fluid_mass.astype(jnp.float32)
    count = shells * devices * breadth
    current = shell_start
    residuals = []
    images = []
    norms = []
    last_load = None
    for iteration in range(ITERS):
        current_half = current.astype(jnp.bfloat16)
        outgoing = jnp.dot(picking, current_half, preferred_element_type=jnp.float32).astype(
            jnp.bfloat16
        )
        incoming = transport(outgoing, devices, capacity)
        displaced = jnp.dot(place_in, incoming, preferred_element_type=jnp.float32).astype(
            jnp.bfloat16
        )
        moved = jnp.einsum(
            "bcj,bij->bci",
            displaced.reshape(blocks, 3, nodes),
            rbf_blocks,
            preferred_element_type=jnp.float32,
        ).reshape(blocks, breadth)
        load = (traction - massive * moved).astype(jnp.bfloat16)
        last_load = load
        mapped = (
            jnp.einsum(
                "bci,bij->bcj",
                load.reshape(blocks, 3, nodes),
                rbf_blocks,
                preferred_element_type=jnp.float32,
            )
            .reshape(blocks, breadth)
            .astype(jnp.bfloat16)
        )
        sending = jnp.dot(place_out, mapped, preferred_element_type=jnp.float32).astype(
            jnp.bfloat16
        )
        arrived = transport(sending, devices, capacity)
        shell_load = jnp.dot(collecting, arrived, preferred_element_type=jnp.float32)
        forcing = (shell_load + robin_coef * current).astype(jnp.bfloat16)
        image = jnp.einsum("bi,bij->bj", forcing, shell_inverse, preferred_element_type=jnp.float32)
        residual = image - current
        residuals.append(residual)
        images.append(image)
        squares_local = jnp.sum(residual * residual)
        if iteration == 0:
            gram_local = jnp.zeros((1, 1), jnp.float32)
            rhs_local = jnp.zeros((1,), jnp.float32)
        else:
            changes = jnp.stack(
                [(residuals[i + 1] - residuals[i]).reshape(-1) for i in range(iteration)]
            )
            gram_local = jnp.dot(changes, changes.T, precision=lax.Precision.HIGHEST)
            rhs_local = jnp.dot(changes, residual.reshape(-1), precision=lax.Precision.HIGHEST)
        gram, rhs, squares = lax.psum((gram_local, rhs_local, squares_local), ("fluid", "solid"))
        norms.append(jnp.sqrt(squares / count + EPSILON))
        if iteration == 0:
            current = current + RELAX * residual
        else:
            image_changes = jnp.stack([images[i + 1] - images[i] for i in range(iteration)])
            coefs = least_squares(gram, -rhs)
            current = image + jnp.tensordot(
                coefs, image_changes, axes=1, precision=lax.Precision.HIGHEST
            )
    return (current, last_load, jnp.stack(norms))


LOAD = 8
LAST = 52
LANES = 128
VMEM_BYTES = 67043328
MESH = pl.DeviceIdType.MESH


def kernel(
    nf, nz, blocks, nodes, shells, count,
    start_hbm, route_hbm, slot_hbm, tr_hbm, ms_hbm, robin_hbm, rbf_hbm, inv_hbm,
    cur_out, load_out, norm_out,
    start_ref, route_ref, slot_ref, tr_ref, ms_ref, robin_ref, load_buf,
    rbf, flip, inv, gath, scal, xcur, xprev, pprev, cur, rprev, robin, wx, wp, vhist, sc, cb,
    place, collect, tr8, ms8, disp8, map8, load8, moved, mapn, part,
    send_a, recv_a, send_b, recv_b,
    in_sem, out_sem, rbf_sem, inv_sem, ag_s, ag_r, pr_s, pr_r, sl_s, sl_r, ra_s, ra_r, rb_s, rb_r,
):
    f32, bf16 = jnp.float32, jnp.bfloat16
    parts = nodes // LANES
    thin = 3 * LANES
    breadth = 3 * nodes
    nxy = nf // 2
    nx = 2 if nxy % 2 == 0 else 1
    ny = nxy // nx
    chips = nxy * nz
    half = chips * shells
    group = nz * shells
    f = lax.axis_index("fluid")
    z = lax.axis_index("solid")
    core = lax.rem(f, 2)
    other = 1 - core
    xy = f // 2
    x, y = lax.rem(xy, nx), xy // nx
    nload = blocks // LOAD
    ngroup = blocks // 8

    nb = 2 if nz % 2 == 0 else 1
    na = nz // nb

    def hops(step):
        ey, ex, ea, eb = step
        return ey + ex + ea * nb + eb

    steps = sorted(
        [
            (ey, ex, ea, eb)
            for ey in range(ny) for ex in range(nx) for ea in range(na) for eb in range(nb)
            if ey + ex + ea + eb
        ],
        key=hops, reverse=True,
    )
    far = len(steps)

    def away(step, sign=1):
        ey, ex, ea, eb = step
        plane = lax.rem(y + sign * ey + ny, ny) * nx + lax.rem(x + sign * ex + nx, nx)
        depth = lax.rem(z // nb + sign * ea + na, na) * nb + lax.rem(lax.rem(z, nb) + sign * eb + nb, nb)
        return plane, depth

    targets = [away(s) for s in steps]
    sources = [away(s, -1) for s in steps]

    def chip(plane, depth):
        return plane * nz + depth

    me = chip(xy, z)

    def remote(src, dst, send_sem, recv_sem, plane, unit, depth):
        return pltpu.make_async_remote_copy(
            src_ref=src, dst_ref=dst, send_sem=send_sem, recv_sem=recv_sem,
            device_id=(plane * 2 + unit, depth), device_id_type=MESH,
        )

    first = pltpu.make_async_copy(start_hbm, start_ref, in_sem.at[0])
    first.start()
    barrier = pltpu.get_barrier_semaphore()
    for plane, depth in targets + [(xy, z)]:
        for unit in (core, other):
            if plane is xy and unit is core:
                continue
            pl.semaphore_signal(
                barrier, inc=1, device_id=(plane * 2 + unit, depth), device_id_type=MESH
            )

    def rbf_copy(i):
        at = pl.ds(i * LOAD, LOAD)
        return pltpu.make_async_copy(rbf_hbm.at[at], rbf.at[at], rbf_sem.at[i])

    def inv_copy():
        return pltpu.make_async_copy(inv_hbm, inv, inv_sem)

    smalls = [
        pltpu.make_async_copy(src, dst, in_sem.at[i + 1])
        for i, (src, dst) in enumerate((
            (route_hbm, route_ref), (slot_hbm, slot_ref), (tr_hbm, tr_ref),
            (ms_hbm, ms_ref), (robin_hbm, robin_ref),
        ))
    ]
    for copy in smalls:
        copy.start()
    for i in range(nload):
        rbf_copy(i).start()
    inv_copy().start()

    def lanes_of(c, h):
        return slice(c * nodes + h * LANES, c * nodes + (h + 1) * LANES)

    def thin_of(c):
        return slice(c * LANES, (c + 1) * LANES)

    def halved(ref, h):
        return jnp.concatenate([ref[:, lanes_of(c, h)] for c in range(3)], axis=1)

    def ag(j, h, k, incoming=False):
        at = chip(*sources[k]) if incoming else me
        block = gath.at[j, h, core, at]
        return remote(
            block, block, ag_s.at[h, k], ag_r.at[h, k], targets[k][0], core, targets[k][1]
        )

    def ag_pair(j, h, k, incoming=False):
        at = me if k == far else chip(*sources[k])
        block = gath.at[j, h, other if incoming else core, at]
        return remote(block, block, pr_s.at[h, k], pr_r.at[h, k], xy, other, z)

    def share(j, h):
        gath[j, h, core, me] = xcur[h].astype(bf16)
        for k in range(far):
            ag(j, h, k).start()
        ag_pair(j, h, far).start()

    def relay(j, h):
        for k in reversed(range(far)):
            ag(j, h, k, True).wait_recv()
            ag_pair(j, h, k).start()

    first.wait()
    for h in range(parts):
        xcur[h] = halved(start_ref, h)
    pl.semaphore_wait(barrier, 2 * far + 1)
    for h in range(parts):
        share(0, h)

    xprev[...] = xcur[...]
    for ref in (pprev, cur, rprev, wx, wp, vhist, sc, cb):
        ref[...] = jnp.zeros(ref.shape, ref.dtype)
    mapn[...] = jnp.zeros(mapn.shape, bf16)

    def clear(i, c):
        at = pl.ds(pl.multiple_of(i * 64, 64), 64)
        for ref in (tr8, ms8, disp8):
            ref[:, at, :] = jnp.zeros((parts, 64, LANES), f32)
        return c

    lax.fori_loop(0, ngroup, clear, 0)
    for copy in smalls:
        copy.wait()
    for h in range(parts):
        robin[h] = halved(robin_ref, h)

    def strided(q, c):
        return pl.ds(q * 64 + c, 8, stride=8)

    def rows_of(ref, at):
        return jnp.concatenate([ref[p, at, :] for p in range(parts)], axis=1)

    def set_rows(ref, at, value):
        for p in range(parts):
            ref[p, at, :] = value[:, p * LANES:(p + 1) * LANES]

    for src, dst in ((tr_ref, tr8), (ms_ref, ms8)):
        for row in range(0, blocks, 16):
            size = min(16, blocks - row)
            wide = src[row:row + size, :].astype(f32)
            for k in range(size // 8):
                for c in range(3):
                    for h in range(parts):
                        dst[h, strided(row // 8 + k, c), :] = wide[k * 8:(k + 1) * 8, lanes_of(c, h)]

    diagonal = lax.broadcasted_iota(jnp.int32, (blocks, blocks), 0) == lax.broadcasted_iota(
        jnp.int32, (blocks, blocks), 1
    )
    target = (route_ref[...] * shells + slot_ref[...]).astype(f32)
    column = jnp.sum(jnp.where(diagonal, target, 0.0), axis=1, keepdims=True)
    for side in range(2):
        unit = core if side == 0 else other
        line = lax.broadcasted_iota(jnp.int32, (half, 1), 0)
        ids = (line // group * 2 + unit) * group + lax.rem(line, group)
        collect[side] = jnp.zeros(collect.shape[1:], bf16)
        collect[side, :, 0:blocks] = jnp.where(ids.astype(f32) == target, 1.0, 0.0).astype(bf16)
        lane = lax.broadcasted_iota(jnp.int32, (1, half), 1)
        ids = (lane // group * 2 + unit) * group + lax.rem(lane, group)
        place[side] = jnp.where(ids.astype(f32) == column, 1.0, 0.0).astype(bf16)

    def turn(i, c):
        rbf_copy(i).wait()
        for u in range(LOAD):
            flip[i * LOAD + u] = rbf[i * LOAD + u].T
        return c

    lax.fori_loop(0, nload, turn, 0)
    lane = lax.broadcasted_iota(jnp.int32, (1, LANES), 1)

    def pick(vector, q):
        return jnp.sum(jnp.where(lane == q, vector, 0.0), axis=1, keepdims=True)

    def dot(a, b):
        return jnp.dot(a, b, preferred_element_type=f32)

    def scalar_copies(j, incoming=False):
        copies = []
        turn = lax.rem(j, 2)
        for k in range(far + 1):
            for unit in range(2):
                if k == far and unit == 0:
                    continue
                at = (me if k == far else chip(*sources[k])) if incoming else me
                mine = (core if unit == 0 else other) if incoming else core
                plane, depth = (xy, z) if k == far else targets[k]
                block = scal.at[j, mine, at]
                copies.append(remote(
                    block, block, sl_s.at[turn, k, unit], sl_r.at[turn, k, unit],
                    plane, core if unit == 0 else other, depth,
                ))
        return copies

    def scalars(j):
        residual = xcur[...] - cur[...]
        newest = residual - rprev[...]
        rprev[...] = residual
        vhist[lax.rem(j + ITERS - 2, ITERS)] = newest

        def total(product):
            rows = jnp.sum(jnp.sum(product, axis=0), axis=0, keepdims=True)
            return jnp.sum(rows, axis=1, keepdims=True)

        vector = jnp.where(lane == 0, total(residual * residual), 0.0)
        for i in range(ITERS - 1):
            vector = jnp.where(lane == 1 + i, total(vhist[i] * residual), vector)
            vector = jnp.where(lane == 8 + i, total(vhist[i] * newest), vector)
        scal[j, core, me] = vector
        for copy in scalar_copies(j):
            copy.start()

    def coefficients(j):
        for copy in scalar_copies(j, True):
            copy.wait_recv()
        k = j - 1
        total = jnp.sum(jnp.sum(scal[j], axis=0), axis=0)
        sc[j] = total
        norm = jnp.sqrt(pick(total, 0) / count + EPSILON)
        norm_out[k] = jnp.broadcast_to(norm, (1, LANES))

        order = ITERS - 1
        gram = [[None] * order for _ in range(order)]
        for col in range(order):
            vector = sc[col + 2]
            for row in range(col + 1):
                value = pick(vector, 8 + row)
                if row == col:
                    value = jnp.where(col < k, value, 1.0)
                gram[col][row] = value
        side = [-pick(total, 1 + i) for i in range(order)]
        lower = [[None] * order for _ in range(order)]
        for row in range(order):
            for col in range(row + 1):
                value = gram[row][col]
                for inner in range(col):
                    value = value - lower[row][inner] * lower[col][inner]
                if row == col:
                    lower[row][row] = jnp.sqrt(value)
                else:
                    lower[row][col] = value / lower[col][col]
        middle = []
        for row in range(order):
            value = side[row]
            for inner in range(row):
                value = value - lower[row][inner] * middle[inner]
            middle.append(value / lower[row][row])
        result = [None] * order
        for row in reversed(range(order)):
            value = middle[row]
            for inner in range(row + 1, order):
                value = value - lower[inner][row] * result[inner]
            result[row] = value / lower[row][row]
        relax = jnp.where(j == 1, jnp.full((1, 1), RELAX - 1.0, f32), 0.0)
        for i, value in enumerate([relax] + result):
            cb[i] = jnp.broadcast_to(value, (1, LANES))

    def blend(newest, history, h):
        value = newest
        for i in range(ITERS):
            value = value + jnp.concatenate([cb[i]] * 3, axis=1) * history[i, h]
        return value

    def note(j):
        wx[lax.rem(j + ITERS - 1, ITERS)] = xcur[...] - xprev[...]
        xprev[...] = xcur[...]

    upper = lax.broadcasted_iota(jnp.int32, (16, LANES), 0) < 8

    def iteration(j, carry):
        def fetch(h):
            def side(unit):
                return gath[j, h, unit].reshape(half, thin)

            picked = dot(place[0], side(core))
            for k in range(far + 1):
                ag_pair(j, h, k, True).wait_recv()
            picked = picked + dot(place[1], side(other))
            for q in range(ngroup):
                for c in range(3):
                    disp8[h, strided(q, c), :] = picked[q * 8:(q + 1) * 8, thin_of(c)]

        def move(begin, end, h):
            cut = slice(h * LANES, (h + 1) * LANES)
            for b in range(begin, end, 2):
                at = pl.ds(b * 8, 16)
                both = disp8[h, at, :]
                left = jnp.concatenate(
                    [jnp.where(upper, both, 0.0), jnp.where(upper, 0.0, both)], axis=1
                ).astype(bf16)
                shift = dot(left, jnp.concatenate([flip[b, cut, :], flip[b + 1, cut, :]], axis=0))
                if h > 0:
                    shift = shift + rows_of(moved.at[j], at)
                set_rows(moved.at[j], at, shift)
                if h == parts - 1:
                    load = rows_of(tr8, at) - rows_of(ms8, at) * shift
                    load8[b // 2] = load.astype(bf16)

        def back(begin, end, h):
            cut = slice(h * LANES, (h + 1) * LANES)
            for b in range(begin, end, 2):
                right = jnp.concatenate([rbf[b, :, cut], rbf[b + 1, :, cut]], axis=1)
                both = dot(load8[b // 2], right)
                map8[h, pl.ds(b * 8, 8), :] = both[0:8, 0:LANES]
                map8[h, pl.ds(b * 8 + 8, 8), :] = both[8:16, LANES:2 * LANES]

        def copy_a(h):
            return remote(send_a.at[h], recv_a.at[h], ra_s.at[h], ra_r.at[h], xy, other, z)

        def copy_b(h, k):
            return remote(
                send_b.at[h, k], recv_b.at[h, k], rb_s.at[h, k], rb_r.at[h, k],
                targets[k][0], core, targets[k][1],
            )

        def gather_up(h):
            for q in range(0, ngroup, 2):
                size = min(2, ngroup - q)
                for c in range(3):
                    rows = [map8[h, strided(q + k, c), :] for k in range(size)]
                    value = jnp.concatenate(rows, axis=0) if size > 1 else rows[0]
                    mapn[h, q * 8:(q + size) * 8, thin_of(c)] = value.astype(bf16)
            send_a[h] = dot(collect[1], mapn[h]).reshape(chips, shells, thin).astype(bf16)
            copy_a(h).start()
            part[h] = dot(collect[0], mapn[h]).reshape(chips, shells, thin)

        def spread_out(h):
            copy_a(h).wait_recv()
            for k in range(far):
                at = chip(*targets[k])
                send_b[h, k] = (part[h, at] + recv_a[h, at].astype(f32)).astype(bf16)
                copy_b(h, k).start()

        relay(j, 0)
        fetch(0)
        relay(j, 1)
        move(0, blocks, 0)
        fetch(1)
        move(0, blocks, 1)
        back(0, blocks, 0)
        gather_up(0)
        back(0, LAST, 1)
        spread_out(0)
        back(LAST, blocks, 1)
        gather_up(1)
        spread_out(1)

        @pl.when(j > 0)
        def _():
            coefficients(j)
            for copy in scalar_copies(j):
                copy.wait_send()

        for h in range(parts):
            cur[h] = blend(xcur[h], wx, h)
        for h in range(parts):
            for k in range(far):
                ag(j, h, k).wait_send()
            for k in range(far + 1):
                ag_pair(j, h, k).wait_send()
            copy_a(h).wait_send()

        @pl.when(j == 0)
        def _():
            inv_copy().wait()

        def forcing(h):
            shell_load = part[h, me] + recv_a[h, me].astype(f32)
            for k in reversed(range(far)):
                copy_b(h, k).wait_recv()
                shell_load = shell_load + recv_b[h, k].astype(f32)
            return (shell_load + robin[h] * xcur[h]).astype(bf16)

        def table(s, c, h, lanes):
            return inv[s, lanes_of(c, h), lanes]

        row = lax.broadcasted_iota(jnp.int32, (shells, LANES), 0)

        def tail_left(force, s):
            last = force[:, thin_of(2)].astype(f32)
            return jnp.concatenate(
                [jnp.where(row == s, last, 0.0), jnp.where(row == s + 1, last, 0.0)], axis=1
            )

        def tail_right(s, h, lanes):
            return jnp.concatenate([table(s, 2, h, lanes), table(s + 1, 2, h, lanes)], axis=0)

        def lead_right(s, h, lanes):
            return jnp.concatenate([table(s, 0, h, lanes), table(s, 1, h, lanes)], axis=0)

        force = forcing(0)
        shell_row = lax.broadcasted_iota(jnp.int32, (shells, breadth), 0)
        whole = slice(0, breadth)
        early = jnp.zeros((shells, breadth), f32)
        for s in range(shells):
            lead = dot(force[:, 0:2 * LANES], lead_right(s, 0, whole))
            early = jnp.where(shell_row == s, lead, early)
        for s in range(0, shells, 2):
            early = early + dot(tail_left(force, s).astype(bf16), tail_right(s, 0, whole))
        force = forcing(1)
        shell_row = lax.broadcasted_iota(jnp.int32, (shells, thin), 0)
        for h in range(parts):
            def wide_right(pieces):
                return jnp.concatenate(
                    [make(lanes_of(c, h)) for make in pieces for c in range(3)], axis=1
                )

            image = jnp.zeros((shells, thin), f32)
            for s in range(0, shells, 2):
                both = dot(force[:, 0:2 * LANES], wide_right(
                    [functools.partial(lead_right, s, 1), functools.partial(lead_right, s + 1, 1)]
                ))
                image = jnp.where(shell_row == s, both[:, 0:thin], image)
                image = jnp.where(shell_row == s + 1, both[:, thin:2 * thin], image)
            for s in range(0, shells, 4):
                left = jnp.concatenate([tail_left(force, s), tail_left(force, s + 2)], axis=0)
                both = dot(left.astype(bf16), wide_right(
                    [functools.partial(tail_right, s, 1), functools.partial(tail_right, s + 2, 1)]
                ))
                image = image + both[0:shells, 0:thin] + both[shells:2 * shells, thin:2 * thin]
            image = image + jnp.concatenate([early[:, lanes_of(c, h)] for c in range(3)], axis=1)
            wp[lax.rem(j + ITERS - 1, ITERS), h] = image - pprev[h]
            pprev[h] = image
            xcur[h] = blend(image, wp, h)

            @pl.when(j < ITERS - 1)
            def _():
                share(j + 1, h)

        scalars(j + 1)
        note(j + 1)
        for h in range(parts):
            for k in range(far):
                copy_b(h, k).wait_send()
        return carry

    lax.fori_loop(0, ITERS, iteration, 0)
    weights = []
    for i in range(ITERS):
        value = 1.0 if i == ITERS - 1 else -cb[i]
        value = value + cb[i - 1] if i > 0 else value
        weights.append(value)
    for q in range(0, ngroup, 2):
        size = min(2, ngroup - q)
        rows = slice(q * 8, (q + size) * 8)
        for c in range(3):
            for h in range(parts):
                shift = None
                for i in range(ITERS):
                    term = [moved[i, h, strided(q + k, c), :] for k in range(size)]
                    term = weights[i] * (jnp.concatenate(term, axis=0) if size > 1 else term[0])
                    shift = term if shift is None else shift + term
                lanes = lanes_of(c, h)
                load = tr_ref[rows, lanes].astype(f32) - ms_ref[rows, lanes].astype(f32) * shift
                load_buf[rows, lanes] = load.astype(bf16)
    write = pltpu.make_async_copy(load_buf, load_out, out_sem)
    write.start()
    coefficients(ITERS)
    for h in range(parts):
        last = blend(xcur[h], wx, h)
        for c in range(3):
            cur_out[:, lanes_of(c, h)] = last[:, thin_of(c)]
    for copy in scalar_copies(ITERS):
        copy.wait_send()
    write.wait()


def hand_over(current, load, norms, current_out, load_out, norm_out):
    current_out[...] = current[...]
    load_out[...] = load[...]
    for i in range(norm_out.shape[0]):
        norm_out[i] = norms[i, 0, 0]


def fused(nf, nz, rbf_blocks, fluid_traction, fluid_mass, route, slot, shell_inverse, robin_coef, shell_start):
    f32, bf16 = jnp.float32, jnp.bfloat16
    blocks, nodes, _ = rbf_blocks.shape
    shells, breadth = shell_start.shape
    chips = nf // 2 * nz
    half = chips * shells
    far = chips - 1
    padded = -(-blocks // LANES) * LANES
    dma = pltpu.SemaphoreType.DMA
    vmem = pl.BlockSpec(memory_space=pltpu.VMEM)
    anywhere = pl.BlockSpec(memory_space=pl.ANY)
    parts = nodes // LANES
    thin = 3 * LANES
    plain = pltpu.VMEM((shells, breadth), f32)
    state = pltpu.VMEM((parts, shells, thin), f32)
    history = pltpu.VMEM((ITERS, parts, shells, thin), f32)
    lines = blocks * 8 + 8
    wide = pltpu.VMEM((parts, lines, LANES), f32)
    exchange = pltpu.VMEM((parts, chips, shells, thin), bf16)
    current, load, norms = pl.pallas_call(
        functools.partial(kernel, nf, nz, blocks, nodes, shells, 2 * half * breadth),
        out_shape=(
            jax.ShapeDtypeStruct((shells, breadth), f32),
            jax.ShapeDtypeStruct((blocks, breadth), bf16),
            jax.ShapeDtypeStruct((ITERS, 1, LANES), f32),
        ),
        in_specs=[anywhere] * 8,
        out_specs=(vmem, anywhere, vmem),
        scratch_shapes=[
            plain,
            pltpu.VMEM((1, blocks), jnp.int32),
            pltpu.VMEM((1, blocks), jnp.int32),
            pltpu.VMEM((blocks, breadth), bf16),
            pltpu.VMEM((blocks, breadth), bf16),
            plain,
            pltpu.VMEM((blocks, breadth), bf16),
            pltpu.VMEM(rbf_blocks.shape, bf16),
            pltpu.VMEM(rbf_blocks.shape, bf16),
            pltpu.VMEM(shell_inverse.shape, bf16),
            pltpu.VMEM((ITERS, parts, 2, chips, shells, thin), bf16),
            pltpu.VMEM((ITERS + 1, 2, chips, 1, LANES), f32),
            state, state, state, state, state, state,
            history, history, history,
            pltpu.VMEM((ITERS + 1, 1, LANES), f32),
            pltpu.VMEM((ITERS, 1, LANES), f32),
            pltpu.VMEM((2, blocks, half), bf16),
            pltpu.VMEM((2, half, padded), bf16),
            wide, wide, wide, wide,
            pltpu.VMEM((blocks // 2, 16, nodes), bf16),
            pltpu.VMEM((ITERS, parts, lines, LANES), f32),
            pltpu.VMEM((parts, padded, thin), bf16),
            pltpu.VMEM((parts, chips, shells, thin), f32),
            exchange, exchange, exchange, exchange,
            dma((6,)), dma,
            dma((blocks // LOAD,)),
            dma,
            dma((parts, far)), dma((parts, far)),
            dma((parts, far + 1)), dma((parts, far + 1)),
            dma((2, far + 1, 2)), dma((2, far + 1, 2)),
            dma((parts,)), dma((parts,)),
            dma((parts, far)), dma((parts, far)),
        ],
        compiler_params=pltpu.CompilerParams(
            collective_id=0, has_side_effects=True, vmem_limit_bytes=VMEM_BYTES,
        ),
        name="coupling",
    )(
        shell_start, route.T, slot[None, :], fluid_traction, fluid_mass, robin_coef, rbf_blocks,
        shell_inverse,
    )
    smem = pl.BlockSpec(memory_space=pltpu.SMEM)
    return pl.pallas_call(
        hand_over,
        out_shape=(
            jax.ShapeDtypeStruct(current.shape, f32),
            jax.ShapeDtypeStruct(load.shape, bf16),
            jax.ShapeDtypeStruct((ITERS,), f32),
        ),
        in_specs=[vmem, vmem, smem],
        out_specs=(vmem, vmem, smem),
        name="results",
    )(current, load, norms)


def choose(nf, nz):
    def body(rbf_blocks, *others):
        if nf * nz > 32:
            return per_device(rbf_blocks, *others)
        return fused(nf, nz, rbf_blocks, *others)

    return body


def solution(mesh):
    in_specs = (
        P(("fluid", "solid"), None, None),
        P(("fluid", "solid"), None),
        P(("fluid", "solid"), None),
        P(("fluid", "solid"), None),
        P(("fluid", "solid")),
        P(("fluid", "solid"), None, None),
        P(("fluid", "solid"), None),
        P(("fluid", "solid"), None),
    )
    out_specs = (P(("fluid", "solid"), None), P(("fluid", "solid"), None), P())
    return jax.shard_map(
        choose(mesh.shape["fluid"], mesh.shape["solid"]), mesh=mesh, in_specs=in_specs, out_specs=out_specs, check_vma=False
    )
```

```python
import functools

import jax
import jax.numpy as jnp
from jax import lax
from jax.experimental import pallas as pl
from jax.experimental.pallas import tpu as pltpu
from jax.sharding import PartitionSpec as P

ITERS = 6


RELAX = 0.3
EPSILON = 1e-06


def transport(buffer, devices, capacity):
    breadth = buffer.shape[1]
    moved = lax.all_to_all(
        buffer.reshape(devices, capacity, breadth),
        ("fluid", "solid"),
        split_axis=0,
        concat_axis=0,
        tiled=True,
    )
    return moved.reshape(devices * capacity, breadth)


def least_squares(gram, target_side):
    order = gram.shape[0]
    lower = [[None] * order for _ in range(order)]
    for row in range(order):
        for column in range(row + 1):
            total = gram[row, column]
            for inner in range(column):
                total = total - lower[row][inner] * lower[column][inner]
            if row == column:
                lower[row][row] = jnp.sqrt(total)
            else:
                lower[row][column] = total / lower[column][column]
    middle = []
    for row in range(order):
        total = target_side[row]
        for inner in range(row):
            total = total - lower[row][inner] * middle[inner]
        middle.append(total / lower[row][row])
    result = [None] * order
    for row in reversed(range(order)):
        total = middle[row]
        for inner in range(row + 1, order):
            total = total - lower[inner][row] * result[inner]
        result[row] = total / lower[row][row]
    return jnp.stack(result)


def per_device(
    rbf_blocks, fluid_traction, fluid_mass, route, slot, shell_inverse, robin_coef, shell_start
):
    devices = lax.axis_size("fluid") * lax.axis_size("solid")
    blocks = rbf_blocks.shape[0]
    nodes = rbf_blocks.shape[1]
    breadth = 3 * nodes
    shells = shell_inverse.shape[0]
    capacity = max(2, 2 * blocks // devices)
    slots_all = devices * capacity
    destination = route[:, 0]
    block_order = jnp.arange(blocks, dtype=jnp.int32)
    earlier = (destination[:, None] == destination[None, :]) & (
        block_order[None, :] < block_order[:, None]
    )
    slot_rank = jnp.sum(earlier.astype(jnp.int32), axis=1)
    position = destination * capacity + slot_rank
    positions = jnp.arange(slots_all, dtype=jnp.int32)
    placing = positions[:, None] == position[None, :]
    place_out = placing.astype(jnp.bfloat16)
    place_in = (position[:, None] == positions[None, :]).astype(jnp.bfloat16)
    wanted = jnp.max(jnp.where(placing, slot[None, :] + 1, 0), axis=1) - 1
    asked = lax.all_to_all(
        wanted.reshape(devices, capacity),
        ("fluid", "solid"),
        split_axis=0,
        concat_axis=0,
        tiled=True,
    ).reshape(slots_all)
    shell_ids = jnp.arange(shells, dtype=jnp.int32)
    picking = (asked[:, None] == shell_ids[None, :]).astype(jnp.bfloat16)
    collecting = (shell_ids[:, None] == asked[None, :]).astype(jnp.bfloat16)
    traction = fluid_traction.astype(jnp.float32)
    massive = fluid_mass.astype(jnp.float32)
    count = shells * devices * breadth
    current = shell_start
    residuals = []
    images = []
    norms = []
    last_load = None
    for iteration in range(ITERS):
        current_half = current.astype(jnp.bfloat16)
        outgoing = jnp.dot(picking, current_half, preferred_element_type=jnp.float32).astype(
            jnp.bfloat16
        )
        incoming = transport(outgoing, devices, capacity)
        displaced = jnp.dot(place_in, incoming, preferred_element_type=jnp.float32).astype(
            jnp.bfloat16
        )
        moved = jnp.einsum(
            "bcj,bij->bci",
            displaced.reshape(blocks, 3, nodes),
            rbf_blocks,
            preferred_element_type=jnp.float32,
        ).reshape(blocks, breadth)
        load = (traction - massive * moved).astype(jnp.bfloat16)
        last_load = load
        mapped = (
            jnp.einsum(
                "bci,bij->bcj",
                load.reshape(blocks, 3, nodes),
                rbf_blocks,
                preferred_element_type=jnp.float32,
            )
            .reshape(blocks, breadth)
            .astype(jnp.bfloat16)
        )
        sending = jnp.dot(place_out, mapped, preferred_element_type=jnp.float32).astype(
            jnp.bfloat16
        )
        arrived = transport(sending, devices, capacity)
        shell_load = jnp.dot(collecting, arrived, preferred_element_type=jnp.float32)
        forcing = (shell_load + robin_coef * current).astype(jnp.bfloat16)
        image = jnp.einsum("bi,bij->bj", forcing, shell_inverse, preferred_element_type=jnp.float32)
        residual = image - current
        residuals.append(residual)
        images.append(image)
        squares_local = jnp.sum(residual * residual)
        if iteration == 0:
            gram_local = jnp.zeros((1, 1), jnp.float32)
            rhs_local = jnp.zeros((1,), jnp.float32)
        else:
            changes = jnp.stack(
                [(residuals[i + 1] - residuals[i]).reshape(-1) for i in range(iteration)]
            )
            gram_local = jnp.dot(changes, changes.T, precision=lax.Precision.HIGHEST)
            rhs_local = jnp.dot(changes, residual.reshape(-1), precision=lax.Precision.HIGHEST)
        gram, rhs, squares = lax.psum((gram_local, rhs_local, squares_local), ("fluid", "solid"))
        norms.append(jnp.sqrt(squares / count + EPSILON))
        if iteration == 0:
            current = current + RELAX * residual
        else:
            image_changes = jnp.stack([images[i + 1] - images[i] for i in range(iteration)])
            coefs = least_squares(gram, -rhs)
            current = image + jnp.tensordot(
                coefs, image_changes, axes=1, precision=lax.Precision.HIGHEST
            )
    return (current, last_load, jnp.stack(norms))


LOAD = 8
LAST = 52
LANES = 128
VMEM_BYTES = 67043328
MESH = pl.DeviceIdType.MESH


def kernel(
    nf, nz, blocks, nodes, shells, count,
    start_hbm, route_hbm, slot_hbm, tr_hbm, ms_hbm, robin_hbm, rbf_hbm, inv_hbm,
    cur_out, load_out, norm_out,
    start_ref, route_ref, slot_ref, tr_ref, ms_ref, robin_ref, load_buf,
    rbf, flip, inv, gath, scal, xcur, xprev, pprev, cur, rprev, robin, wx, wp, vhist, sc, cb,
    place, collect, tr8, ms8, disp8, map8, load8, moved, mapn, part, ahead,
    send_a, recv_a, send_b, recv_b,
    in_sem, out_sem, rbf_sem, inv_sem, ag_s, ag_r, pr_s, pr_r, sl_s, sl_r, ra_s, ra_r, rb_s, rb_r,
):
    f32, bf16 = jnp.float32, jnp.bfloat16
    parts = nodes // LANES
    thin = 3 * LANES
    breadth = 3 * nodes
    nxy = nf // 2
    nx = 2 if nxy % 2 == 0 else 1
    ny = nxy // nx
    chips = nxy * nz
    half = chips * shells
    group = nz * shells
    f = lax.axis_index("fluid")
    z = lax.axis_index("solid")
    core = lax.rem(f, 2)
    other = 1 - core
    xy = f // 2
    x, y = lax.rem(xy, nx), xy // nx
    nload = blocks // LOAD
    ngroup = blocks // 8

    nb = 2 if nz % 2 == 0 else 1
    na = nz // nb

    def hops(step):
        ey, ex, ea, eb = step
        return ey + ex + ea * nb + eb

    steps = sorted(
        [
            (ey, ex, ea, eb)
            for ey in range(ny) for ex in range(nx) for ea in range(na) for eb in range(nb)
            if ey + ex + ea + eb
        ],
        key=hops, reverse=True,
    )
    far = len(steps)

    def away(step, sign=1):
        ey, ex, ea, eb = step
        plane = lax.rem(y + sign * ey + ny, ny) * nx + lax.rem(x + sign * ex + nx, nx)
        depth = lax.rem(z // nb + sign * ea + na, na) * nb + lax.rem(lax.rem(z, nb) + sign * eb + nb, nb)
        return plane, depth

    targets = [away(s) for s in steps]
    sources = [away(s, -1) for s in steps]

    def chip(plane, depth):
        return plane * nz + depth

    me = chip(xy, z)

    def remote(src, dst, send_sem, recv_sem, plane, unit, depth):
        return pltpu.make_async_remote_copy(
            src_ref=src, dst_ref=dst, send_sem=send_sem, recv_sem=recv_sem,
            device_id=(plane * 2 + unit, depth), device_id_type=MESH,
        )

    first = pltpu.make_async_copy(start_hbm, start_ref, in_sem.at[0])
    first.start()
    barrier = pltpu.get_barrier_semaphore()
    for plane, depth in targets + [(xy, z)]:
        for unit in (core, other):
            if plane is xy and unit is core:
                continue
            pl.semaphore_signal(
                barrier, inc=1, device_id=(plane * 2 + unit, depth), device_id_type=MESH
            )

    def rbf_copy(i):
        at = pl.ds(i * LOAD, LOAD)
        return pltpu.make_async_copy(rbf_hbm.at[at], rbf.at[at], rbf_sem.at[i])

    def inv_copy():
        return pltpu.make_async_copy(inv_hbm, inv, inv_sem)

    smalls = [
        pltpu.make_async_copy(src, dst, in_sem.at[i + 1])
        for i, (src, dst) in enumerate((
            (route_hbm, route_ref), (slot_hbm, slot_ref), (tr_hbm, tr_ref),
            (ms_hbm, ms_ref), (robin_hbm, robin_ref),
        ))
    ]
    for copy in smalls:
        copy.start()
    for i in range(nload):
        rbf_copy(i).start()
    inv_copy().start()

    def lanes_of(c, h):
        return slice(c * nodes + h * LANES, c * nodes + (h + 1) * LANES)

    def thin_of(c):
        return slice(c * LANES, (c + 1) * LANES)

    def halved(ref, h):
        return jnp.concatenate([ref[:, lanes_of(c, h)] for c in range(3)], axis=1)

    def ag(j, h, k, incoming=False):
        at = chip(*sources[k]) if incoming else me
        block = gath.at[j, h, core, at]
        return remote(
            block, block, ag_s.at[h, k], ag_r.at[h, k], targets[k][0], core, targets[k][1]
        )

    def ag_pair(j, h, k, incoming=False):
        at = me if k == far else chip(*sources[k])
        block = gath.at[j, h, other if incoming else core, at]
        return remote(block, block, pr_s.at[h, k], pr_r.at[h, k], xy, other, z)

    def share(j, h):
        gath[j, h, core, me] = xcur[h].astype(bf16)
        for k in range(far):
            ag(j, h, k).start()
        ag_pair(j, h, far).start()

    def relay(j, h):
        for k in reversed(range(far)):
            ag(j, h, k, True).wait_recv()
            ag_pair(j, h, k).start()

    first.wait()
    for h in range(parts):
        xcur[h] = halved(start_ref, h)
    pl.semaphore_wait(barrier, 2 * far + 1)
    for h in range(parts):
        share(0, h)

    xprev[...] = xcur[...]
    for ref in (pprev, cur, rprev, wx, wp, vhist, sc, cb):
        ref[...] = jnp.zeros(ref.shape, ref.dtype)
    mapn[...] = jnp.zeros(mapn.shape, bf16)

    def clear(i, c):
        at = pl.ds(pl.multiple_of(i * 64, 64), 64)
        for ref in (tr8, ms8, disp8):
            ref[:, at, :] = jnp.zeros((parts, 64, LANES), f32)
        return c

    lax.fori_loop(0, ngroup, clear, 0)
    for copy in smalls:
        copy.wait()
    for h in range(parts):
        robin[h] = halved(robin_ref, h)

    def strided(q, c):
        return pl.ds(q * 64 + c, 8, stride=8)

    def rows_of(ref, at):
        return jnp.concatenate([ref[p, at, :] for p in range(parts)], axis=1)

    def set_rows(ref, at, value):
        for p in range(parts):
            ref[p, at, :] = value[:, p * LANES:(p + 1) * LANES]

    for src, dst in ((tr_ref, tr8), (ms_ref, ms8)):
        for row in range(0, blocks, 16):
            size = min(16, blocks - row)
            wide = src[row:row + size, :].astype(f32)
            for k in range(size // 8):
                for c in range(3):
                    for h in range(parts):
                        dst[h, strided(row // 8 + k, c), :] = wide[k * 8:(k + 1) * 8, lanes_of(c, h)]

    diagonal = lax.broadcasted_iota(jnp.int32, (blocks, blocks), 0) == lax.broadcasted_iota(
        jnp.int32, (blocks, blocks), 1
    )
    target = (route_ref[...] * shells + slot_ref[...]).astype(f32)
    column = jnp.sum(jnp.where(diagonal, target, 0.0), axis=1, keepdims=True)
    for side in range(2):
        unit = core if side == 0 else other
        line = lax.broadcasted_iota(jnp.int32, (half, 1), 0)
        ids = (line // group * 2 + unit) * group + lax.rem(line, group)
        collect[side] = jnp.zeros(collect.shape[1:], bf16)
        collect[side, :, 0:blocks] = jnp.where(ids.astype(f32) == target, 1.0, 0.0).astype(bf16)
        lane = lax.broadcasted_iota(jnp.int32, (1, half), 1)
        ids = (lane // group * 2 + unit) * group + lax.rem(lane, group)
        place[side] = jnp.where(ids.astype(f32) == column, 1.0, 0.0).astype(bf16)

    def turn(i, c):
        rbf_copy(i).wait()
        for u in range(LOAD):
            flip[i * LOAD + u] = rbf[i * LOAD + u].T
        return c

    lax.fori_loop(0, nload, turn, 0)
    lane = lax.broadcasted_iota(jnp.int32, (1, LANES), 1)

    def pick(vector, q):
        return jnp.sum(jnp.where(lane == q, vector, 0.0), axis=1, keepdims=True)

    def dot(a, b):
        return jnp.dot(a, b, preferred_element_type=f32)

    def scalar_copies(j, incoming=False):
        copies = []
        turn = lax.rem(j, 2)
        for k in range(far + 1):
            for unit in range(2):
                if k == far and unit == 0:
                    continue
                at = (me if k == far else chip(*sources[k])) if incoming else me
                mine = (core if unit == 0 else other) if incoming else core
                plane, depth = (xy, z) if k == far else targets[k]
                block = scal.at[j, mine, at]
                copies.append(remote(
                    block, block, sl_s.at[turn, k, unit], sl_r.at[turn, k, unit],
                    plane, core if unit == 0 else other, depth,
                ))
        return copies

    def scalars(j):
        residual = xcur[...] - cur[...]
        newest = residual - rprev[...]
        rprev[...] = residual
        vhist[lax.rem(j + ITERS - 2, ITERS)] = newest

        def total(product):
            rows = jnp.sum(jnp.sum(product, axis=0), axis=0, keepdims=True)
            return jnp.sum(rows, axis=1, keepdims=True)

        vector = jnp.where(lane == 0, total(residual * residual), 0.0)
        for i in range(ITERS - 1):
            vector = jnp.where(lane == 1 + i, total(vhist[i] * residual), vector)
            vector = jnp.where(lane == 8 + i, total(vhist[i] * newest), vector)
        scal[j, core, me] = vector
        for copy in scalar_copies(j):
            copy.start()

    def coefficients(j):
        for copy in scalar_copies(j, True):
            copy.wait_recv()
        k = j - 1
        total = jnp.sum(jnp.sum(scal[j], axis=0), axis=0)
        sc[j] = total
        norm = jnp.sqrt(pick(total, 0) / count + EPSILON)
        norm_out[k] = jnp.broadcast_to(norm, (1, LANES))

        order = ITERS - 1
        gram = [[None] * order for _ in range(order)]
        for col in range(order):
            vector = sc[col + 2]
            for row in range(col + 1):
                value = pick(vector, 8 + row)
                if row == col:
                    value = jnp.where(col < k, value, 1.0)
                gram[col][row] = value
        side = [-pick(total, 1 + i) for i in range(order)]
        lower = [[None] * order for _ in range(order)]
        for row in range(order):
            for col in range(row + 1):
                value = gram[row][col]
                for inner in range(col):
                    value = value - lower[row][inner] * lower[col][inner]
                if row == col:
                    lower[row][row] = jnp.sqrt(value)
                else:
                    lower[row][col] = value / lower[col][col]
        middle = []
        for row in range(order):
            value = side[row]
            for inner in range(row):
                value = value - lower[row][inner] * middle[inner]
            middle.append(value / lower[row][row])
        result = [None] * order
        for row in reversed(range(order)):
            value = middle[row]
            for inner in range(row + 1, order):
                value = value - lower[inner][row] * result[inner]
            result[row] = value / lower[row][row]
        relax = jnp.where(j == 1, jnp.full((1, 1), RELAX - 1.0, f32), 0.0)
        for i, value in enumerate([relax] + result):
            cb[i] = jnp.broadcast_to(value, (1, LANES))

    def blend(newest, history, h):
        value = newest
        for i in range(ITERS):
            value = value + jnp.concatenate([cb[i]] * 3, axis=1) * history[i, h]
        return value

    def note(j):
        wx[lax.rem(j + ITERS - 1, ITERS)] = xcur[...] - xprev[...]
        xprev[...] = xcur[...]

    upper = lax.broadcasted_iota(jnp.int32, (16, LANES), 0) < 8

    def iteration(j, carry):
        def side(h, unit):
            return gath[j, h, unit].reshape(half, thin)

        def fetch(h, picked):
            for k in range(far + 1):
                ag_pair(j, h, k, True).wait_recv()
            picked = picked + dot(place[1], side(h, other))
            for q in range(ngroup):
                for c in range(3):
                    disp8[h, strided(q, c), :] = picked[q * 8:(q + 1) * 8, thin_of(c)]

        def move(begin, end, h):
            cut = slice(h * LANES, (h + 1) * LANES)
            for b in range(begin, end, 2):
                at = pl.ds(b * 8, 16)
                both = disp8[h, at, :]
                left = jnp.concatenate(
                    [jnp.where(upper, both, 0.0), jnp.where(upper, 0.0, both)], axis=1
                ).astype(bf16)
                shift = dot(left, jnp.concatenate([flip[b, cut, :], flip[b + 1, cut, :]], axis=0))
                if h > 0:
                    shift = shift + rows_of(moved.at[j], at)
                set_rows(moved.at[j], at, shift)
                if h == parts - 1:
                    load = rows_of(tr8, at) - rows_of(ms8, at) * shift
                    load8[b // 2] = load.astype(bf16)

        def back(begin, end, h):
            cut = slice(h * LANES, (h + 1) * LANES)
            for b in range(begin, end, 2):
                right = jnp.concatenate([rbf[b, :, cut], rbf[b + 1, :, cut]], axis=1)
                both = dot(load8[b // 2], right)
                map8[h, pl.ds(b * 8, 8), :] = both[0:8, 0:LANES]
                map8[h, pl.ds(b * 8 + 8, 8), :] = both[8:16, LANES:2 * LANES]

        def copy_a(h):
            return remote(send_a.at[h], recv_a.at[h], ra_s.at[h], ra_r.at[h], xy, other, z)

        def copy_b(h, k):
            return remote(
                send_b.at[h, k], recv_b.at[h, k], rb_s.at[h, k], rb_r.at[h, k],
                targets[k][0], core, targets[k][1],
            )

        def gather_up(h):
            for q in range(0, ngroup, 2):
                size = min(2, ngroup - q)
                for c in range(3):
                    rows = [map8[h, strided(q + k, c), :] for k in range(size)]
                    value = jnp.concatenate(rows, axis=0) if size > 1 else rows[0]
                    mapn[h, q * 8:(q + size) * 8, thin_of(c)] = value.astype(bf16)
            send_a[h] = dot(collect[1], mapn[h]).reshape(chips, shells, thin).astype(bf16)
            copy_a(h).start()
            part[h] = dot(collect[0], mapn[h]).reshape(chips, shells, thin)

        def spread_out(h):
            copy_a(h).wait_recv()
            for k in range(far):
                at = chip(*targets[k])
                send_b[h, k] = (part[h, at] + recv_a[h, at].astype(f32)).astype(bf16)
                copy_b(h, k).start()

        relay(j, 0)
        fetch(0, dot(place[0], side(0, core)))
        relay(j, 1)
        ahead[...] = dot(place[0], side(1, core))
        move(0, blocks, 0)
        fetch(1, ahead[...])
        move(0, blocks, 1)
        back(0, blocks, 0)
        gather_up(0)
        back(0, LAST, 1)
        spread_out(0)
        back(LAST, blocks, 1)
        gather_up(1)
        spread_out(1)

        @pl.when(j > 0)
        def _():
            coefficients(j)
            for copy in scalar_copies(j):
                copy.wait_send()

        for h in range(parts):
            cur[h] = blend(xcur[h], wx, h)
        for h in range(parts):
            for k in range(far):
                ag(j, h, k).wait_send()
            for k in range(far + 1):
                ag_pair(j, h, k).wait_send()
            copy_a(h).wait_send()

        @pl.when(j == 0)
        def _():
            inv_copy().wait()

        def forcing(h):
            shell_load = part[h, me] + recv_a[h, me].astype(f32)
            for k in reversed(range(far)):
                copy_b(h, k).wait_recv()
                shell_load = shell_load + recv_b[h, k].astype(f32)
            return (shell_load + robin[h] * xcur[h]).astype(bf16)

        def table(s, c, h, lanes):
            return inv[s, lanes_of(c, h), lanes]

        row = lax.broadcasted_iota(jnp.int32, (shells, LANES), 0)

        def tail_left(force, s):
            last = force[:, thin_of(2)].astype(f32)
            return jnp.concatenate(
                [jnp.where(row == s, last, 0.0), jnp.where(row == s + 1, last, 0.0)], axis=1
            )

        def tail_right(s, h, lanes):
            return jnp.concatenate([table(s, 2, h, lanes), table(s + 1, 2, h, lanes)], axis=0)

        def lead_right(s, h, lanes):
            return jnp.concatenate([table(s, 0, h, lanes), table(s, 1, h, lanes)], axis=0)

        force = forcing(0)
        shell_row = lax.broadcasted_iota(jnp.int32, (shells, breadth), 0)
        whole = slice(0, breadth)
        early = jnp.zeros((shells, breadth), f32)
        for s in range(shells):
            lead = dot(force[:, 0:2 * LANES], lead_right(s, 0, whole))
            early = jnp.where(shell_row == s, lead, early)
        for s in range(0, shells, 2):
            early = early + dot(tail_left(force, s).astype(bf16), tail_right(s, 0, whole))
        force = forcing(1)
        shell_row = lax.broadcasted_iota(jnp.int32, (shells, thin), 0)
        for h in range(parts):
            def wide_right(pieces):
                return jnp.concatenate(
                    [make(lanes_of(c, h)) for make in pieces for c in range(3)], axis=1
                )

            image = jnp.zeros((shells, thin), f32)
            for s in range(0, shells, 2):
                both = dot(force[:, 0:2 * LANES], wide_right(
                    [functools.partial(lead_right, s, 1), functools.partial(lead_right, s + 1, 1)]
                ))
                image = jnp.where(shell_row == s, both[:, 0:thin], image)
                image = jnp.where(shell_row == s + 1, both[:, thin:2 * thin], image)
            for s in range(0, shells, 4):
                left = jnp.concatenate([tail_left(force, s), tail_left(force, s + 2)], axis=0)
                both = dot(left.astype(bf16), wide_right(
                    [functools.partial(tail_right, s, 1), functools.partial(tail_right, s + 2, 1)]
                ))
                image = image + both[0:shells, 0:thin] + both[shells:2 * shells, thin:2 * thin]
            image = image + jnp.concatenate([early[:, lanes_of(c, h)] for c in range(3)], axis=1)
            wp[lax.rem(j + ITERS - 1, ITERS), h] = image - pprev[h]
            pprev[h] = image
            xcur[h] = blend(image, wp, h)

            @pl.when(j < ITERS - 1)
            def _():
                share(j + 1, h)

        scalars(j + 1)
        note(j + 1)
        for h in range(parts):
            for k in range(far):
                copy_b(h, k).wait_send()
        return carry

    lax.fori_loop(0, ITERS, iteration, 0)
    weights = []
    for i in range(ITERS):
        value = 1.0 if i == ITERS - 1 else -cb[i]
        value = value + cb[i - 1] if i > 0 else value
        weights.append(value)
    for q in range(0, ngroup, 2):
        size = min(2, ngroup - q)
        rows = slice(q * 8, (q + size) * 8)
        for c in range(3):
            for h in range(parts):
                shift = None
                for i in range(ITERS):
                    term = [moved[i, h, strided(q + k, c), :] for k in range(size)]
                    term = weights[i] * (jnp.concatenate(term, axis=0) if size > 1 else term[0])
                    shift = term if shift is None else shift + term
                lanes = lanes_of(c, h)
                load = tr_ref[rows, lanes].astype(f32) - ms_ref[rows, lanes].astype(f32) * shift
                load_buf[rows, lanes] = load.astype(bf16)
    write = pltpu.make_async_copy(load_buf, load_out, out_sem)
    write.start()
    coefficients(ITERS)
    for h in range(parts):
        last = blend(xcur[h], wx, h)
        for c in range(3):
            cur_out[:, lanes_of(c, h)] = last[:, thin_of(c)]
    for copy in scalar_copies(ITERS):
        copy.wait_send()
    write.wait()


def hand_over(current, load, norms, current_out, load_out, norm_out):
    current_out[...] = current[...]
    load_out[...] = load[...]
    for i in range(norm_out.shape[0]):
        norm_out[i] = norms[i, 0, 0]


def fused(nf, nz, rbf_blocks, fluid_traction, fluid_mass, route, slot, shell_inverse, robin_coef, shell_start):
    f32, bf16 = jnp.float32, jnp.bfloat16
    blocks, nodes, _ = rbf_blocks.shape
    shells, breadth = shell_start.shape
    chips = nf // 2 * nz
    half = chips * shells
    far = chips - 1
    padded = -(-blocks // LANES) * LANES
    dma = pltpu.SemaphoreType.DMA
    vmem = pl.BlockSpec(memory_space=pltpu.VMEM)
    anywhere = pl.BlockSpec(memory_space=pl.ANY)
    parts = nodes // LANES
    thin = 3 * LANES
    plain = pltpu.VMEM((shells, breadth), f32)
    state = pltpu.VMEM((parts, shells, thin), f32)
    history = pltpu.VMEM((ITERS, parts, shells, thin), f32)
    lines = blocks * 8 + 8
    wide = pltpu.VMEM((parts, lines, LANES), f32)
    exchange = pltpu.VMEM((parts, chips, shells, thin), bf16)
    current, load, norms = pl.pallas_call(
        functools.partial(kernel, nf, nz, blocks, nodes, shells, 2 * half * breadth),
        out_shape=(
            jax.ShapeDtypeStruct((shells, breadth), f32),
            jax.ShapeDtypeStruct((blocks, breadth), bf16),
            jax.ShapeDtypeStruct((ITERS, 1, LANES), f32),
        ),
        in_specs=[anywhere] * 8,
        out_specs=(vmem, anywhere, vmem),
        scratch_shapes=[
            plain,
            pltpu.VMEM((1, blocks), jnp.int32),
            pltpu.VMEM((1, blocks), jnp.int32),
            pltpu.VMEM((blocks, breadth), bf16),
            pltpu.VMEM((blocks, breadth), bf16),
            plain,
            pltpu.VMEM((blocks, breadth), bf16),
            pltpu.VMEM(rbf_blocks.shape, bf16),
            pltpu.VMEM(rbf_blocks.shape, bf16),
            pltpu.VMEM(shell_inverse.shape, bf16),
            pltpu.VMEM((ITERS, parts, 2, chips, shells, thin), bf16),
            pltpu.VMEM((ITERS + 1, 2, chips, 1, LANES), f32),
            state, state, state, state, state, state,
            history, history, history,
            pltpu.VMEM((ITERS + 1, 1, LANES), f32),
            pltpu.VMEM((ITERS, 1, LANES), f32),
            pltpu.VMEM((2, blocks, half), bf16),
            pltpu.VMEM((2, half, padded), bf16),
            wide, wide, wide, wide,
            pltpu.VMEM((blocks // 2, 16, nodes), bf16),
            pltpu.VMEM((ITERS, parts, lines, LANES), f32),
            pltpu.VMEM((parts, padded, thin), bf16),
            pltpu.VMEM((parts, chips, shells, thin), f32),
            pltpu.VMEM((blocks, thin), f32),
            exchange, exchange, exchange, exchange,
            dma((6,)), dma,
            dma((blocks // LOAD,)),
            dma,
            dma((parts, far)), dma((parts, far)),
            dma((parts, far + 1)), dma((parts, far + 1)),
            dma((2, far + 1, 2)), dma((2, far + 1, 2)),
            dma((parts,)), dma((parts,)),
            dma((parts, far)), dma((parts, far)),
        ],
        compiler_params=pltpu.CompilerParams(
            collective_id=0, has_side_effects=True, vmem_limit_bytes=VMEM_BYTES,
        ),
        name="coupling",
    )(
        shell_start, route.T, slot[None, :], fluid_traction, fluid_mass, robin_coef, rbf_blocks,
        shell_inverse,
    )
    smem = pl.BlockSpec(memory_space=pltpu.SMEM)
    return pl.pallas_call(
        hand_over,
        out_shape=(
            jax.ShapeDtypeStruct(current.shape, f32),
            jax.ShapeDtypeStruct(load.shape, bf16),
            jax.ShapeDtypeStruct((ITERS,), f32),
        ),
        in_specs=[vmem, vmem, smem],
        out_specs=(vmem, vmem, smem),
        name="results",
    )(current, load, norms)


def choose(nf, nz):
    def body(rbf_blocks, *others):
        if nf * nz > 32:
            return per_device(rbf_blocks, *others)
        return fused(nf, nz, rbf_blocks, *others)

    return body


def solution(mesh):
    in_specs = (
        P(("fluid", "solid"), None, None),
        P(("fluid", "solid"), None),
        P(("fluid", "solid"), None),
        P(("fluid", "solid"), None),
        P(("fluid", "solid")),
        P(("fluid", "solid"), None, None),
        P(("fluid", "solid"), None),
        P(("fluid", "solid"), None),
    )
    out_specs = (P(("fluid", "solid"), None), P(("fluid", "solid"), None), P())
    return jax.shard_map(
        choose(mesh.shape["fluid"], mesh.shape["solid"]), mesh=mesh, in_specs=in_specs, out_specs=out_specs, check_vma=False
    )
```
